32 devices in a mesh: wide: 8 (over z, core), narrow: 4 (over y, x).
Axes of the slice: x: 2, y: 2, z: 4, core: 2. Of those that a mesh axis runs over, the one named last changes fastest.
Arguments:
- tokens: bfloat16 [8192, 2048], P(('wide', 'narrow')), may hold values from -6 to 6
- doc_ids: int32 [8, 1024], P('wide'), may hold values from 0 to 3, never falling along the last dimension, each value on 1 to 512 neighbouring positions
- cotangent: bfloat16 [8192, 2048], P(('wide', 'narrow')), may hold values from -6 to 6
- attn_gain: bfloat16 [2048], P('wide'), may hold values from 0.5 to 1.5
- w_query: bfloat16 [2048, 2048], P('wide', 'narrow'), may hold values from -0.125 to 0.125
- w_key: bfloat16 [2048, 1024], P('wide', 'narrow'), may hold values from -0.125 to 0.125
- w_value: bfloat16 [2048, 1024], P('wide', 'narrow'), may hold values from -0.125 to 0.125
- query_gain: bfloat16 [128], P('wide'), may hold values from 0.5 to 1.5
- key_gain: bfloat16 [128], P('wide'), may hold values from 0.5 to 1.5
- w_out: bfloat16 [2048, 2048], P('narrow', 'wide'), may hold values from -1 to 1
- mlp_gain: bfloat16 [2048], P('wide'), may hold values from 0.5 to 1.5
- w_gate: bfloat16 [2048, 6144], P('wide', 'narrow'), may hold values from -0.125 to 0.125
- w_up: bfloat16 [2048, 6144], P('wide', 'narrow'), may hold values from -0.125 to 0.125
- w_down: bfloat16 [6144, 2048], P('narrow', 'wide'), may hold values from -0.15625 to 0.15625
Outputs:
- output: bfloat16 [8192, 2048], P(('wide', 'narrow'))
- d_tokens: float32 [8192, 2048], P(('wide', 'narrow'))
- grad_attn_gain: float32 [2048], P('wide')
- grad_w_query: float32 [2048, 2048], P('wide', 'narrow')
- grad_w_key: float32 [2048, 1024], P('wide', 'narrow')
- grad_w_value: float32 [2048, 1024], P('wide', 'narrow')
- grad_query_gain: float32 [128], P('wide')
- grad_key_gain: float32 [128], P('wide')
- grad_w_out: float32 [2048, 2048], P('narrow', 'wide')
- grad_mlp_gain: float32 [2048], P('wide')
- grad_w_gate: float32 [2048, 6144], P('wide', 'narrow')
- grad_w_up: float32 [2048, 6144], P('wide', 'narrow')
- grad_w_down: float32 [6144, 2048], P('narrow', 'wide')
The draws below stay inside these ranges and needn't reach their ends.
Inputs may be any that keep to these rules, and one draw needn't show every extreme that they name: `doc_ids`: document numbers never fall along a sequence, each of 0 to 3 appears in every sequence, every document has 1 to 512 tokens and one has exactly 512.
All inputs are finite; a program needn't handle non-finite values.
Results may differ from the reference program's by a relative error of at most 0.025.
Values may be sent and summed in bfloat16 or wider, within the bound.
A program may use at most 192 MiB of HBM per device.

```python
import math
import jax
import jax.numpy as jnp
import numpy as np
from jax import lax

D = 2048
H = 16
KV = 8
HD = 128
FF = 6144
LEN = 1024
SEQS = 8
TOKENS = 8192


def steps_of(own_key, dims, cuts, low, high):
    def one(axis_at, blocks):
        steps = jax.random.uniform(jax.random.fold_in(jax.random.fold_in(own_key, 6), axis_at), (blocks,), jnp.float32, low / len(cuts), high / len(cuts))
        return jnp.repeat(jnp.exp(steps), dims[axis_at] // blocks).reshape((-1,) + (1,) * (len(dims) - axis_at - 1))

    level = one(*cuts[0])
    for cut in cuts[1:]:
        level = level * one(*cut)
    return level


def profile(amount, total, most, slope):
    portions = [(1 << 20) // math.isqrt(rank ** slope) + 1 for rank in range(2, amount + 1)]
    spare, given = total - most - (amount - 1), [1] * (amount - 1)
    while spare > 0:
        movable = [i for i in range(amount - 1) if given[i] < most]
        mass, remaining = sum([portions[i] for i in movable]), spare
        for i in movable:
            addition = min(most - given[i], max(1, remaining * portions[i] // mass), spare)
            given[i] = given[i] + addition
            spare = spare - addition
    return np.array([most] + given)


def ragged_sizes(rng, count, total, bound, slope):
    if count == 2:
        one = jax.random.randint(rng, (), max(1, total - bound), min(bound, total - 1) + 1)
        return jnp.stack([one, total - one])
    tallies = jnp.asarray(profile(count, total, bound, slope), jnp.int32)
    couples = (count - 1) // 2
    giver, sink = tallies[1:1 + 2 * couples:2], tallies[2:2 + 2 * couples:2]
    margin = jnp.minimum(giver - 1, bound - sink)
    passed = jax.random.randint(jax.random.fold_in(rng, 1), (couples,), 0, 1 << 20) % (margin + 1)
    tallies = tallies.at[1:1 + 2 * couples:2].set(giver - passed).at[2:2 + 2 * couples:2].set(sink + passed)
    return tallies[jax.random.permutation(jax.random.fold_in(rng, 2), count)]


def centred(rng, dims, spread, bound, pieces=(), kind=jnp.bfloat16):
    level = steps_of(rng, dims, pieces, -0.22, 0.18) if pieces else 1.0
    drawn = jax.random.normal(rng, dims, jnp.float32) * spread * level
    return jnp.minimum(jnp.maximum(drawn, -bound), bound).astype(kind)


def setup_inputs(seed: int = 0) -> dict:
    arg_keys = jax.random.split(jax.random.key(seed), 15)
    return {
        "tokens": centred(arg_keys[0], (TOKENS, D), 1.0, 6.0, ((0, 32),)),
        "doc_ids": jax.vmap(lambda own: jnp.searchsorted(jnp.cumsum(ragged_sizes(own, 4, LEN, LEN // 2, 2)), jnp.arange(LEN), side="right"))(jax.random.split(arg_keys[1], SEQS)).reshape((SEQS, LEN)).astype(jnp.int32),
        "cotangent": centred(arg_keys[2], (TOKENS, D), 1.0, 6.0, ((0, 32),)),
        "attn_gain": jnp.clip(1.0 + 0.1 * jax.random.normal(arg_keys[3], (D,), jnp.float32), 0.5, 1.5).astype(jnp.bfloat16),
        "w_query": centred(arg_keys[4], (D, H * HD), D ** -0.5, 0.125, ((0, 8), (1, 4))),
        "w_key": centred(arg_keys[5], (D, KV * HD), D ** -0.5, 0.125, ((0, 8), (1, 4))),
        "w_value": centred(arg_keys[6], (D, KV * HD), D ** -0.5, 0.125, ((0, 8), (1, 4))),
        "query_gain": jnp.clip(1.0 + 0.1 * jax.random.normal(arg_keys[7], (HD,), jnp.float32), 0.5, 1.5).astype(jnp.bfloat16),
        "key_gain": jnp.clip(1.0 + 0.1 * jax.random.normal(arg_keys[8], (HD,), jnp.float32), 0.5, 1.5).astype(jnp.bfloat16),
        "w_out": centred(arg_keys[9], (H * HD, D), (H * HD // 64) ** -0.5, 1.0, ((0, 4), (1, 8))),
        "mlp_gain": jnp.clip(1.0 + 0.1 * jax.random.normal(arg_keys[10], (D,), jnp.float32), 0.5, 1.5).astype(jnp.bfloat16),
        "w_gate": centred(arg_keys[11], (D, FF), D ** -0.5, 0.125, ((0, 8), (1, 4))),
        "w_up": centred(arg_keys[12], (D, FF), D ** -0.5, 0.125, ((0, 8), (1, 4))),
        "w_down": centred(arg_keys[13], (FF, D), (FF // 4) ** -0.5, 0.15625, ((0, 4), (1, 8))),
    }


EPS = 1e-06
ROPE_BASE = 1000000.0
NEG_FILL = -1e+30
HIGH = lax.Precision.HIGHEST

@jax.custom_vjp
def low(v):
    return lax.optimization_barrier(v.astype(jnp.bfloat16)).astype(jnp.float32)

@jax.custom_vjp
def low_back(v):
    return v

def low_keep(v):
    return (low(v), None)

def low_pass(kept, grad):
    return (grad,)

def back_keep(v):
    return (v, None)

def back_low(kept, grad):
    return (low(grad),)
low.defvjp(low_keep, low_pass)
low_back.defvjp(back_keep, back_low)

def rms_apply(values, gain):
    return values * lax.rsqrt(lax.optimization_barrier(jnp.mean(values * values, axis=-1, keepdims=True)) + EPS) * gain

def rotate(values):
    half = values.shape[-1] // 2
    return jnp.concatenate([-values[..., half:], values[..., :half]], axis=-1)

def rope_tables(doc_rows):
    index = lax.broadcasted_iota(jnp.int32, doc_rows.shape, 1)
    change = jnp.concatenate([jnp.ones((doc_rows.shape[0], 1), jnp.bool_), doc_rows[:, 1:] != doc_rows[:, :-1]], axis=1)
    begin = lax.cummax(jnp.where(change, index, 0), axis=1)
    position = (index - begin).astype(jnp.float32)
    freqs = ROPE_BASE ** (-(jnp.arange(HD // 2, dtype=jnp.float32) * (2.0 / HD)))
    angle = position[..., None] * freqs
    cosine = jnp.cos(angle)
    sine = jnp.sin(angle)
    return (jnp.concatenate([cosine, cosine], axis=-1), jnp.concatenate([sine, sine], axis=-1))

def layer(inputs, weights, doc_ids, cosine, sine):
    attn_gain, w_query, w_key, w_value, query_gain, key_gain, w_out, mlp_gain, w_gate, w_up, w_down = weights
    seq_count = doc_ids.shape[0]
    normed = low(rms_apply(inputs, attn_gain))
    q_pre = low_back(jnp.dot(normed, w_query, precision=HIGH))
    k_pre = low_back(jnp.dot(normed, w_key, precision=HIGH))
    v_all = low(low_back(jnp.dot(normed, w_value, precision=HIGH)))
    queries = q_pre.reshape(seq_count, LEN, H, HD)
    keys = k_pre.reshape(seq_count, LEN, KV, HD)
    values = v_all.reshape(seq_count, LEN, KV, HD)
    index = jnp.arange(LEN)
    causal = index[None, :] <= index[:, None]

    def one_sequence(items):
        q_seq, k_seq, v_seq, doc_row, cos_seq, sin_seq = items
        cos_heads = cos_seq[:, None, :]
        sin_heads = sin_seq[:, None, :]
        q_norm = rms_apply(q_seq, query_gain)
        k_norm = rms_apply(k_seq, key_gain)
        q_use = low(q_norm * cos_heads + rotate(q_norm) * sin_heads)
        k_use = low(k_norm * cos_heads + rotate(k_norm) * sin_heads)
        k_rep = jnp.repeat(k_use, H // KV, axis=1)
        v_rep = jnp.repeat(v_seq, H // KV, axis=1)
        scores = low_back(jnp.einsum('qhd,khd->hqk', q_use, k_rep, precision=HIGH) * HD ** (-0.5))
        allowed = causal & (doc_row[None, :] == doc_row[:, None])
        scores = jnp.where(allowed[None], scores, NEG_FILL)
        probs = jax.nn.softmax(scores, axis=-1)
        mixed = jnp.einsum('hqk,khd->qhd', low(probs), v_rep, precision=HIGH)
        return low(low_back(mixed)).reshape(LEN, H * HD)
    attended = lax.map(jax.checkpoint(one_sequence), (queries, keys, values, doc_ids, cosine, sine))
    attended = attended.reshape(seq_count * LEN, H * HD)
    resid = inputs + low_back(jnp.dot(attended, w_out, precision=HIGH))
    mlp_in = low(rms_apply(resid, mlp_gain))
    gate = low_back(jnp.dot(mlp_in, w_gate, precision=HIGH))
    up = low_back(jnp.dot(mlp_in, w_up, precision=HIGH))
    hidden = low(jax.nn.silu(gate) * up)
    return resid + low_back(jnp.dot(hidden, w_down, precision=HIGH))

def reference(tokens, doc_ids, cotangent, attn_gain, w_query, w_key, w_value, query_gain, key_gain, w_out, mlp_gain, w_gate, w_up, w_down):
    params = tuple((item.astype(jnp.float32) for item in (attn_gain, w_query, w_key, w_value, query_gain, key_gain, w_out, mlp_gain, w_gate, w_up, w_down)))
    cosine, sine = rope_tables(doc_ids)

    def forward(inputs, *weights):
        return layer(inputs, weights, doc_ids, cosine, sine)
    output, pullback = jax.vjp(forward, tokens.astype(jnp.float32), *params)
    grads = pullback(cotangent.astype(jnp.float32))
    return (output.astype(jnp.bfloat16), grads[0], grads[1], grads[2], grads[3], grads[4], grads[5], grads[6], grads[7], grads[8], grads[9], grads[10], grads[11])
```

```python
import jax
import jax.numpy as jnp
from jax import lax
from jax.sharding import PartitionSpec as P

H = 16
KV = 8
HD = 128


EPS = 1e-06
ROPE_BASE = 1000000.0
NEG_FILL = -1e30

XPERM = [(0, 1), (1, 0), (2, 3), (3, 2)]
YPERM = [(0, 2), (2, 0), (1, 3), (3, 1)]


def rms_apply(values, gain):
    return values * lax.rsqrt(jnp.mean(values * values, axis=-1, keepdims=True) + EPS) * gain


def rms_back(values, gain, grad):
    scale = lax.rsqrt(jnp.mean(values * values, axis=-1, keepdims=True) + EPS)
    weighted = grad * gain
    inner = jnp.mean(weighted * values, axis=-1, keepdims=True)
    d_values = scale * weighted - values * (scale * scale * scale) * inner
    return (d_values, grad * values * scale)


def rotate(values):
    half = values.shape[-1] // 2
    return jnp.concatenate([-values[..., half:], values[..., :half]], axis=-1)


def rotate_back(values):
    half = values.shape[-1] // 2
    return jnp.concatenate([values[..., half:], -values[..., :half]], axis=-1)


def rope_tables(doc_rows):
    index = lax.broadcasted_iota(jnp.int32, doc_rows.shape, 1)
    change = jnp.concatenate(
        [jnp.ones((doc_rows.shape[0], 1), jnp.bool_), doc_rows[:, 1:] != doc_rows[:, :-1]], axis=1
    )
    begin = lax.cummax(jnp.where(change, index, 0), axis=1)
    position = (index - begin).astype(jnp.float32)
    freqs = ROPE_BASE ** (-(jnp.arange(HD // 2, dtype=jnp.float32) * (2.0 / HD)))
    angle = position[..., None] * freqs
    cosine = jnp.cos(angle)
    sine = jnp.sin(angle)
    return (jnp.concatenate([cosine, cosine], axis=-1), jnp.concatenate([sine, sine], axis=-1))


def contract_rows(left, right):
    return lax.dot_general(
        left, right, (((0,), (0,)), ((), ())), preferred_element_type=jnp.float32
    )


def times_transposed(left, right):
    return lax.dot_general(
        left, right, (((1,), (1,)), ((), ())), preferred_element_type=jnp.float32
    )


def place(pieces, index, axis):
    first = jnp.stack([pieces[0], pieces[1]], axis=axis)
    second = jnp.stack([pieces[1], pieces[0]], axis=axis)
    return lax.select(jnp.broadcast_to(index == 0, first.shape), first, second)


def narrow_gather(x):
    if lax.axis_size("narrow") != 4:
        return lax.all_gather(x, "narrow", axis=0, tiled=True)
    n = lax.axis_index("narrow")
    xb = n % 2
    yb = n // 2
    r, c = x.shape
    h = c // 2
    a, b = x[:, :h], x[:, h:]
    a_x = lax.ppermute(a, "narrow", XPERM)
    b_y = lax.ppermute(b, "narrow", YPERM)
    a_pair = place((a, a_x), xb, 0)
    b_pair = place((b, b_y), yb, 0)
    a_pair_y = lax.ppermute(a_pair, "narrow", YPERM)
    b_pair_x = lax.ppermute(b_pair, "narrow", XPERM)
    a_full = place((a_pair, a_pair_y), yb, 0)
    b_full = place((b_pair, b_pair_x), xb, 1)
    return jnp.concatenate([a_full, b_full], axis=-1).reshape(4 * r, c)


def narrow_scatter(x):
    if lax.axis_size("narrow") != 4:
        return lax.psum_scatter(
            x.astype(jnp.bfloat16), "narrow", scatter_dimension=0, tiled=True
        ).astype(jnp.float32)
    n = lax.axis_index("narrow")
    xb = n % 2
    yb = n // 2
    rows, c = x.shape
    r = rows // 4
    h = c // 2
    quarters = x.reshape(2, 2, r, c)
    a = quarters[..., :h]
    b = quarters[..., h:]
    a_keep = lax.dynamic_index_in_dim(a, yb, 0, keepdims=False)
    a_send = lax.dynamic_index_in_dim(a, 1 - yb, 0, keepdims=False)
    b_keep = lax.dynamic_index_in_dim(b, xb, 1, keepdims=False)
    b_send = lax.dynamic_index_in_dim(b, 1 - xb, 1, keepdims=False)
    a_got = lax.ppermute(a_send.astype(jnp.bfloat16), "narrow", YPERM)
    b_got = lax.ppermute(b_send.astype(jnp.bfloat16), "narrow", XPERM)
    a_sum = a_keep + a_got.astype(jnp.float32)
    b_sum = b_keep + b_got.astype(jnp.float32)
    a_mine = lax.dynamic_index_in_dim(a_sum, xb, 0, keepdims=False)
    a_other = lax.dynamic_index_in_dim(a_sum, 1 - xb, 0, keepdims=False)
    b_mine = lax.dynamic_index_in_dim(b_sum, yb, 0, keepdims=False)
    b_other = lax.dynamic_index_in_dim(b_sum, 1 - yb, 0, keepdims=False)
    a_got2 = lax.ppermute(a_other.astype(jnp.bfloat16), "narrow", XPERM)
    b_got2 = lax.ppermute(b_other.astype(jnp.bfloat16), "narrow", YPERM)
    a_fin = a_mine + a_got2.astype(jnp.float32)
    b_fin = b_mine + b_got2.astype(jnp.float32)
    return jnp.concatenate([a_fin, b_fin], axis=-1)


def wide_gather(blocks):
    widths = [blk.shape[1] for blk in blocks]
    joined = lax.all_gather(jnp.concatenate(blocks, axis=1), "wide", axis=0, tiled=True)
    out = []
    start = 0
    for w in widths:
        out.append(joined[:, start : start + w])
        start += w
    return out


def wide_scatter(blocks):
    widths = [blk.shape[1] for blk in blocks]
    joined = jnp.concatenate([blk.astype(jnp.bfloat16) for blk in blocks], axis=1)
    summed = lax.psum_scatter(joined, "wide", scatter_dimension=0, tiled=True).astype(jnp.float32)
    out = []
    start = 0
    for w in widths:
        out.append(summed[:, start : start + w])
        start += w
    return out


def shards(
    tokens,
    doc_ids,
    cotangent,
    attn_gain,
    w_query,
    w_key,
    w_value,
    query_gain,
    key_gain,
    w_out,
    mlp_gain,
    w_gate,
    w_up,
    w_down,
):
    narrow_size = lax.axis_size("narrow")
    wide_size = lax.axis_size("wide")
    heads_here = H // narrow_size
    groups_here = KV // narrow_size
    repeat = H // KV
    seq_count, length = doc_ids.shape
    rows_group = seq_count * length
    scale = HD ** (-0.5)
    d_local = attn_gain.shape[0]
    hd_local = query_gain.shape[0]
    q_cols = w_query.shape[1]
    kv_cols = w_key.shape[1]
    ff_cols = w_gate.shape[1]

    gain_block = jnp.zeros((d_local, 128), jnp.bfloat16)
    gain_block = gain_block.at[:, 0].set(attn_gain)
    gain_block = gain_block.at[:, 1].set(mlp_gain)
    gain_block = gain_block.at[:hd_local, 2].set(query_gain)
    gain_block = gain_block.at[:hd_local, 3].set(key_gain)

    query_w, key_w, value_w, out_wt, gains_all = wide_gather(
        [w_query, w_key, w_value, w_out.T, gain_block]
    )
    gain_attn = gains_all[:, 0].astype(jnp.float32)
    gain_mlp = gains_all[:, 1].astype(jnp.float32)
    gain_query = gains_all.reshape(wide_size, d_local, 128)[:, :hd_local, 2].reshape(-1).astype(jnp.float32)
    gain_key = gains_all.reshape(wide_size, d_local, 128)[:, :hd_local, 3].reshape(-1).astype(jnp.float32)
    gate_w, up_w, down_wt = wide_gather([w_gate, w_up, w_down.T])

    cosine, sine = rope_tables(doc_ids)
    cos_heads = cosine[:, :, None, :]
    sin_heads = sine[:, :, None, :]
    position = jnp.arange(length)
    causal = position[None, :] <= position[:, None]

    def mask_for(doc_row):
        return causal & (doc_row[None, :] == doc_row[:, None])

    inputs = tokens.astype(jnp.float32)
    normed = rms_apply(inputs, gain_attn).astype(jnp.bfloat16)
    normed_all = narrow_gather(normed)
    grad_rows = narrow_gather(cotangent)
    q_pre = jnp.dot(normed_all, query_w, preferred_element_type=jnp.float32).reshape(
        seq_count, length, heads_here, HD
    )
    k_pre = jnp.dot(normed_all, key_w, preferred_element_type=jnp.float32).reshape(
        seq_count, length, groups_here, HD
    )
    v_use = (
        jnp.dot(normed_all, value_w, preferred_element_type=jnp.float32)
        .astype(jnp.bfloat16)
        .reshape(seq_count, length, groups_here, HD)
    )
    q_norm = rms_apply(q_pre, gain_query)
    k_norm = rms_apply(k_pre, gain_key)
    q_use = (q_norm * cos_heads + rotate(q_norm) * sin_heads).astype(jnp.bfloat16)
    k_use = (k_norm * cos_heads + rotate(k_norm) * sin_heads).astype(jnp.bfloat16)
    q_grouped = q_use.reshape(seq_count, length, groups_here, repeat, HD)

    def attend(carry, items):
        q_seq, k_seq, v_seq, doc_row = items
        allowed = mask_for(doc_row)
        scores = (
            jnp.einsum("qgrd,kgd->grqk", q_seq, k_seq, preferred_element_type=jnp.float32) * scale
        )
        scores = jnp.where(allowed, scores, NEG_FILL)
        top = jnp.max(scores, axis=-1, keepdims=True)
        weights = jnp.exp(scores - top)
        total = jnp.sum(weights, axis=-1, keepdims=True)
        probs = weights / total
        mixed = jnp.einsum(
            "grqk,kgd->qgrd", probs.astype(jnp.bfloat16), v_seq, preferred_element_type=jnp.float32
        )
        log_total = (top + jnp.log(total))[..., 0]
        return (carry, (mixed.astype(jnp.bfloat16).reshape(length, heads_here * HD), log_total))

    unused, (attended, log_totals) = lax.scan(attend, 0, (q_grouped, k_use, v_use, doc_ids))
    attended = attended.reshape(rows_group, heads_here * HD)
    resid = inputs + narrow_scatter(times_transposed(attended, out_wt))
    mlp_in = rms_apply(resid, gain_mlp).astype(jnp.bfloat16)
    mlp_all = narrow_gather(mlp_in)
    gate = jnp.dot(mlp_all, gate_w, preferred_element_type=jnp.float32)
    up = jnp.dot(mlp_all, up_w, preferred_element_type=jnp.float32)
    sigmoid = jax.nn.sigmoid(gate)
    hidden = (gate * sigmoid * up).astype(jnp.bfloat16)
    output = (resid + narrow_scatter(times_transposed(hidden, down_wt))).astype(jnp.bfloat16)
    grad_w_down_t = contract_rows(grad_rows, hidden)
    d_hidden = jnp.dot(grad_rows, down_wt, preferred_element_type=jnp.float32)
    d_up = (d_hidden * gate * sigmoid).astype(jnp.bfloat16)
    d_gate = (d_hidden * up * sigmoid * (1.0 + gate * (1.0 - sigmoid))).astype(jnp.bfloat16)
    grad_w_gate = contract_rows(mlp_all, d_gate)
    grad_w_up = contract_rows(mlp_all, d_up)
    mlp_shards = wide_scatter([grad_w_gate, grad_w_up, grad_w_down_t])
    d_mlp_in = narrow_scatter(times_transposed(d_gate, gate_w) + times_transposed(d_up, up_w))
    d_part, mlp_gain_terms = rms_back(resid, gain_mlp, d_mlp_in)
    grad_mlp_gain = jnp.sum(mlp_gain_terms, axis=0)
    d_resid = cotangent.astype(jnp.float32) + d_part
    branch_rows = narrow_gather(d_resid.astype(jnp.bfloat16))
    grad_w_out_t = contract_rows(branch_rows, attended)
    d_attended = jnp.dot(branch_rows, out_wt, preferred_element_type=jnp.float32).astype(jnp.bfloat16)
    d_grouped = d_attended.reshape(seq_count, length, groups_here, repeat, HD)

    def attend_back(carry, items):
        q_seq, k_seq, v_seq, doc_row, log_total, d_mixed = items
        allowed = mask_for(doc_row)
        scores = (
            jnp.einsum("qgrd,kgd->grqk", q_seq, k_seq, preferred_element_type=jnp.float32) * scale
        )
        probs = jnp.where(allowed, jnp.exp(scores - log_total[..., None]), 0.0)
        d_probs = jnp.einsum("qgrd,kgd->grqk", d_mixed, v_seq, preferred_element_type=jnp.float32)
        inner = jnp.sum(probs * d_probs, axis=-1, keepdims=True)
        d_scores = (probs * (d_probs - inner)).astype(jnp.bfloat16)
        d_query = (
            jnp.einsum("grqk,kgd->qgrd", d_scores, k_seq, preferred_element_type=jnp.float32)
            * scale
        )
        d_key = (
            jnp.einsum("grqk,qgrd->kgd", d_scores, q_seq, preferred_element_type=jnp.float32)
            * scale
        )
        d_value = jnp.einsum(
            "grqk,qgrd->kgd",
            probs.astype(jnp.bfloat16),
            d_mixed,
            preferred_element_type=jnp.float32,
        )
        return (carry, (d_query, d_key, d_value.astype(jnp.bfloat16)))

    unused, (d_query, d_key, d_value) = lax.scan(
        attend_back, 0, (q_grouped, k_use, v_use, doc_ids, log_totals, d_grouped)
    )
    d_query = d_query.reshape(seq_count, length, heads_here, HD)
    d_q_norm = d_query * cos_heads + rotate_back(d_query * sin_heads)
    d_k_norm = d_key * cos_heads + rotate_back(d_key * sin_heads)
    d_q_pre, query_terms = rms_back(q_pre, gain_query, d_q_norm)
    d_k_pre, key_terms = rms_back(k_pre, gain_key, d_k_norm)
    grad_query_gain = jnp.sum(query_terms, axis=(0, 1, 2))
    grad_key_gain = jnp.sum(key_terms, axis=(0, 1, 2))
    d_q_pre = d_q_pre.astype(jnp.bfloat16).reshape(rows_group, heads_here * HD)
    d_k_pre = d_k_pre.astype(jnp.bfloat16).reshape(rows_group, groups_here * HD)
    d_value = d_value.reshape(rows_group, groups_here * HD)
    grad_w_query = contract_rows(normed_all, d_q_pre)
    grad_w_key = contract_rows(normed_all, d_k_pre)
    grad_w_value = contract_rows(normed_all, d_value)
    total = times_transposed(d_q_pre, query_w)
    total = total + times_transposed(d_k_pre, key_w)
    d_normed = narrow_scatter(total + times_transposed(d_value, value_w))
    d_input_part, attn_gain_terms = rms_back(inputs, gain_attn, d_normed)
    grad_attn_gain = jnp.sum(attn_gain_terms, axis=0)
    d_tokens = d_resid + d_input_part

    d_full = d_local * wide_size
    gain_grads = jnp.zeros((d_full, 128), jnp.float32)
    gain_grads = gain_grads.at[:, 0].set(grad_attn_gain)
    gain_grads = gain_grads.at[:, 1].set(grad_mlp_gain)
    gain_grads = gain_grads.reshape(wide_size, d_local, 128)
    gain_grads = gain_grads.at[:, :hd_local, 2].set(grad_query_gain.reshape(wide_size, hd_local))
    gain_grads = gain_grads.at[:, :hd_local, 3].set(grad_key_gain.reshape(wide_size, hd_local))
    gain_grads = gain_grads.reshape(d_full, 128)
    g_query, g_key, g_value, g_out_t, g_gains = wide_scatter(
        [grad_w_query, grad_w_key, grad_w_value, grad_w_out_t, gain_grads]
    )
    gain_totals = lax.psum(g_gains[:, :4], "narrow")
    return (
        output,
        d_tokens,
        gain_totals[:, 0],
        g_query,
        g_key,
        g_value,
        gain_totals[:hd_local, 2],
        gain_totals[:hd_local, 3],
        g_out_t.T,
        gain_totals[:, 1],
        mlp_shards[0],
        mlp_shards[1],
        mlp_shards[2].T,
    )


def solution(mesh):
    in_specs = (
        P(("wide", "narrow"), None),
        P("wide", None),
        P(("wide", "narrow"), None),
        P("wide"),
        P("wide", "narrow"),
        P("wide", "narrow"),
        P("wide", "narrow"),
        P("wide"),
        P("wide"),
        P("narrow", "wide"),
        P("wide"),
        P("wide", "narrow"),
        P("wide", "narrow"),
        P("narrow", "wide"),
    )
    out_specs = (
        P(("wide", "narrow"), None),
        P(("wide", "narrow"), None),
        P("wide"),
        P("wide", "narrow"),
        P("wide", "narrow"),
        P("wide", "narrow"),
        P("wide"),
        P("wide"),
        P("narrow", "wide"),
        P("wide"),
        P("wide", "narrow"),
        P("wide", "narrow"),
        P("narrow", "wide"),
    )
    return jax.shard_map(shards, mesh=mesh, in_specs=in_specs, out_specs=out_specs, check_vma=False)
```

```python
import jax
import jax.numpy as jnp
from jax import lax
from jax.sharding import PartitionSpec as P

H = 16
KV = 8
HD = 128


EPS = 1e-06
ROPE_BASE = 1000000.0
NEG_FILL = -1e30

XPERM = [(0, 1), (1, 0), (2, 3), (3, 2)]
YPERM = [(0, 2), (2, 0), (1, 3), (3, 1)]
BLOCK_XOR = (0, 1, 2, 3, 0, 2, 1, 3)


def rms_apply(values, gain):
    return values * lax.rsqrt(jnp.mean(values * values, axis=-1, keepdims=True) + EPS) * gain


def rms_back(values, gain, grad):
    scale = lax.rsqrt(jnp.mean(values * values, axis=-1, keepdims=True) + EPS)
    weighted = grad * gain
    inner = jnp.mean(weighted * values, axis=-1, keepdims=True)
    d_values = scale * weighted - values * (scale * scale * scale) * inner
    return (d_values, grad * values * scale)


def rotate(values):
    half = values.shape[-1] // 2
    return jnp.concatenate([-values[..., half:], values[..., :half]], axis=-1)


def rotate_back(values):
    half = values.shape[-1] // 2
    return jnp.concatenate([values[..., half:], -values[..., :half]], axis=-1)


def doc_positions(doc_rows):
    index = lax.broadcasted_iota(jnp.int32, doc_rows.shape, 1)
    change = jnp.concatenate(
        [jnp.ones((doc_rows.shape[0], 1), jnp.bool_), doc_rows[:, 1:] != doc_rows[:, :-1]], axis=1
    )
    begin = lax.cummax(jnp.where(change, index, 0), axis=1)
    return index - begin


def rope_from_positions(position):
    freqs = ROPE_BASE ** (-(jnp.arange(HD // 2, dtype=jnp.float32) * (2.0 / HD)))
    angle = position.astype(jnp.float32)[..., None] * freqs
    cosine = jnp.cos(angle)
    sine = jnp.sin(angle)
    return (jnp.concatenate([cosine, cosine], axis=-1), jnp.concatenate([sine, sine], axis=-1))


def contract_rows(left, right):
    return lax.dot_general(
        left, right, (((0,), (0,)), ((), ())), preferred_element_type=jnp.float32
    )


def times_transposed(left, right):
    return lax.dot_general(
        left, right, (((1,), (1,)), ((), ())), preferred_element_type=jnp.float32
    )


def relative_ok(seq_count):
    return lax.axis_size("narrow") == 4 and seq_count == 1


def gather_order(shard_rows):
    n = lax.axis_index("narrow")
    half = shard_rows // 2
    index = jnp.arange(4 * shard_rows, dtype=jnp.int32)
    block = index // half
    offset = index % half
    block_xor = jnp.asarray(BLOCK_XOR, jnp.int32)[block]
    shard = jnp.bitwise_xor(n, block_xor)
    return shard * shard_rows + offset + half * (block >= 4).astype(jnp.int32)


def narrow_gather(x, relative):
    if not relative:
        return lax.all_gather(x, "narrow", axis=0, tiled=True)
    half = x.shape[0] // 2
    a, b = x[:half], x[half:]
    a_x = lax.ppermute(a, "narrow", XPERM)
    b_y = lax.ppermute(b, "narrow", YPERM)
    a_pair = jnp.concatenate([a, a_x], axis=0)
    b_pair = jnp.concatenate([b, b_y], axis=0)
    a_pair_y = lax.ppermute(a_pair, "narrow", YPERM)
    b_pair_x = lax.ppermute(b_pair, "narrow", XPERM)
    return jnp.concatenate([a_pair, a_pair_y, b_pair, b_pair_x], axis=0)


def narrow_scatter(x, relative):
    if not relative:
        return lax.psum_scatter(
            x.astype(jnp.bfloat16), "narrow", scatter_dimension=0, tiled=True
        ).astype(jnp.float32)
    rows, c = x.shape
    half = rows // 8
    blocks = x.reshape(8, half, c)
    a_got = lax.ppermute(blocks[2:4].astype(jnp.bfloat16), "narrow", YPERM)
    b_got = lax.ppermute(blocks[6:8].astype(jnp.bfloat16), "narrow", XPERM)
    a_sum = blocks[0:2] + a_got.astype(jnp.float32)
    b_sum = blocks[4:6] + b_got.astype(jnp.float32)
    a_got2 = lax.ppermute(a_sum[1].astype(jnp.bfloat16), "narrow", XPERM)
    b_got2 = lax.ppermute(b_sum[1].astype(jnp.bfloat16), "narrow", YPERM)
    return jnp.concatenate(
        [a_sum[0] + a_got2.astype(jnp.float32), b_sum[0] + b_got2.astype(jnp.float32)], axis=0
    )


def split_cols(joined, widths):
    out = []
    start = 0
    for w in widths:
        out.append(joined[:, start : start + w])
        start += w
    return out


def wide_gather(blocks):
    joined = lax.all_gather(jnp.concatenate(blocks, axis=1), "wide", axis=0, tiled=True)
    return split_cols(joined, [blk.shape[1] for blk in blocks])


def wide_scatter(blocks):
    joined = jnp.concatenate([blk.astype(jnp.bfloat16) for blk in blocks], axis=1)
    summed = lax.psum_scatter(joined, "wide", scatter_dimension=0, tiled=True).astype(jnp.float32)
    return split_cols(summed, [blk.shape[1] for blk in blocks])


def shards(
    tokens,
    doc_ids,
    cotangent,
    attn_gain,
    w_query,
    w_key,
    w_value,
    query_gain,
    key_gain,
    w_out,
    mlp_gain,
    w_gate,
    w_up,
    w_down,
):
    narrow_size = lax.axis_size("narrow")
    wide_size = lax.axis_size("wide")
    heads_here = H // narrow_size
    groups_here = KV // narrow_size
    repeat = H // KV
    seq_count, length = doc_ids.shape
    rows_group = seq_count * length
    shard_rows = tokens.shape[0]
    scale = HD ** (-0.5)
    d_local = attn_gain.shape[0]
    hd_local = query_gain.shape[0]
    q_cols = w_query.shape[1]
    kv_cols = w_key.shape[1]
    ff_cols = w_gate.shape[1]
    ff_half = ff_cols // 2
    relative = relative_ok(seq_count)

    tokens_all = narrow_gather(tokens, relative)
    grad_rows = narrow_gather(cotangent, relative)

    gain_block = jnp.zeros((d_local, 128), jnp.bfloat16)
    gain_block = gain_block.at[:, 0].set(attn_gain)
    gain_block = gain_block.at[:, 1].set(mlp_gain)
    gain_block = gain_block.at[:hd_local, 2].set(query_gain)
    gain_block = gain_block.at[:hd_local, 3].set(key_gain)
    qkv_w, out_wt, gains_all = wide_gather(
        [jnp.concatenate([w_query, w_key, w_value], axis=1), w_out.T, gain_block]
    )
    gain_attn = gains_all[:, 0].astype(jnp.float32)
    gain_mlp = gains_all[:, 1].astype(jnp.float32)
    gains_split = gains_all.reshape(wide_size, d_local, 128)
    gain_query = gains_split[:, :hd_local, 2].reshape(-1).astype(jnp.float32)
    gain_key = gains_split[:, :hd_local, 3].reshape(-1).astype(jnp.float32)
    down_t = w_down.T
    mlp_sets = []
    for h in range(2):
        cols = slice(h * ff_half, (h + 1) * ff_half)
        mlp_sets.append(wide_gather([w_gate[:, cols], w_up[:, cols], down_t[:, cols]]))

    if relative:
        order = gather_order(shard_rows)
        doc_row = jnp.take(doc_ids[0], order)
        position = jnp.take(doc_positions(doc_ids)[0], order)
    else:
        order = jnp.arange(rows_group, dtype=jnp.int32)
        doc_row = doc_ids.reshape(-1)
        position = doc_positions(doc_ids).reshape(-1)
    cosine, sine = rope_from_positions(position)
    cos_heads = cosine[:, None, :]
    sin_heads = sine[:, None, :]
    allowed = (order[None, :] <= order[:, None]) & (doc_row[None, :] == doc_row[:, None])
    if not relative:
        seq_of = jnp.arange(rows_group, dtype=jnp.int32) // length
        allowed = allowed & (seq_of[None, :] == seq_of[:, None])

    inputs = tokens.astype(jnp.float32)
    normed_all = rms_apply(tokens_all.astype(jnp.float32), gain_attn).astype(jnp.bfloat16)
    qkv = jnp.dot(normed_all, qkv_w, preferred_element_type=jnp.float32)
    q_pre = qkv[:, :q_cols].reshape(rows_group, heads_here, HD)
    k_pre = qkv[:, q_cols : q_cols + kv_cols].reshape(rows_group, groups_here, HD)
    v_use = qkv[:, q_cols + kv_cols :].astype(jnp.bfloat16).reshape(rows_group, groups_here, HD)
    q_norm = rms_apply(q_pre, gain_query)
    k_norm = rms_apply(k_pre, gain_key)
    q_use = (q_norm * cos_heads + rotate(q_norm) * sin_heads).astype(jnp.bfloat16)
    k_use = (k_norm * cos_heads + rotate(k_norm) * sin_heads).astype(jnp.bfloat16)
    q_grouped = q_use.reshape(rows_group, groups_here, repeat, HD)

    scores = jnp.einsum("qgrd,kgd->grqk", q_grouped, k_use, preferred_element_type=jnp.float32) * scale
    scores = jnp.where(allowed, scores, NEG_FILL)
    top = jnp.max(scores, axis=-1, keepdims=True)
    weights = jnp.exp(scores - top)
    total = jnp.sum(weights, axis=-1, keepdims=True)
    probs = weights / total
    mixed = jnp.einsum(
        "grqk,kgd->qgrd", probs.astype(jnp.bfloat16), v_use, preferred_element_type=jnp.float32
    )
    log_totals = (top + jnp.log(total))[..., 0]
    attended = mixed.astype(jnp.bfloat16).reshape(rows_group, heads_here * HD)

    resid = inputs + narrow_scatter(times_transposed(attended, out_wt), relative)
    mlp_in = rms_apply(resid, gain_mlp).astype(jnp.bfloat16)
    mlp_all = narrow_gather(mlp_in, relative)

    down_partial = None
    d_mlp_partial = None
    mlp_grads = []
    for h in range(2):
        gate_w, up_w, down_wt = mlp_sets[h]
        gate = jnp.dot(mlp_all, gate_w, preferred_element_type=jnp.float32)
        up = jnp.dot(mlp_all, up_w, preferred_element_type=jnp.float32)
        sigmoid = jax.nn.sigmoid(gate)
        hidden = (gate * sigmoid * up).astype(jnp.bfloat16)
        part = times_transposed(hidden, down_wt)
        down_partial = part if down_partial is None else down_partial + part
        g_down_t = contract_rows(grad_rows, hidden)
        d_hidden = jnp.dot(grad_rows, down_wt, preferred_element_type=jnp.float32)
        d_up = (d_hidden * gate * sigmoid).astype(jnp.bfloat16)
        d_gate = (d_hidden * up * sigmoid * (1.0 + gate * (1.0 - sigmoid))).astype(jnp.bfloat16)
        g_gate_up = contract_rows(mlp_all, jnp.concatenate([d_gate, d_up], axis=1))
        mlp_grads.append(wide_scatter([g_gate_up, g_down_t]))
        part = times_transposed(d_gate, gate_w) + times_transposed(d_up, up_w)
        d_mlp_partial = part if d_mlp_partial is None else d_mlp_partial + part

    d_mlp_in = narrow_scatter(d_mlp_partial, relative)
    d_part, mlp_gain_terms = rms_back(resid, gain_mlp, d_mlp_in)
    grad_mlp_gain = jnp.sum(mlp_gain_terms, axis=0)
    d_resid = cotangent.astype(jnp.float32) + d_part
    branch_rows = narrow_gather(d_resid.astype(jnp.bfloat16), relative)
    (g_out_t,) = wide_scatter([contract_rows(branch_rows, attended)])
    d_attended = jnp.dot(branch_rows, out_wt, preferred_element_type=jnp.float32).astype(jnp.bfloat16)
    d_mixed = d_attended.reshape(rows_group, groups_here, repeat, HD)

    p_scores = jnp.einsum("qgrd,kgd->grqk", q_grouped, k_use, preferred_element_type=jnp.float32) * scale
    p_probs = jnp.where(allowed, jnp.exp(p_scores - log_totals[..., None]), 0.0)
    d_probs = jnp.einsum("qgrd,kgd->grqk", d_mixed, v_use, preferred_element_type=jnp.float32)
    inner = jnp.sum(p_probs * d_probs, axis=-1, keepdims=True)
    d_scores = (p_probs * (d_probs - inner)).astype(jnp.bfloat16)
    d_query = jnp.einsum("grqk,kgd->qgrd", d_scores, k_use, preferred_element_type=jnp.float32) * scale
    d_key = jnp.einsum("grqk,qgrd->kgd", d_scores, q_grouped, preferred_element_type=jnp.float32) * scale
    d_value = jnp.einsum(
        "grqk,qgrd->kgd", p_probs.astype(jnp.bfloat16), d_mixed, preferred_element_type=jnp.float32
    ).astype(jnp.bfloat16)

    d_query = d_query.reshape(rows_group, heads_here, HD)
    d_q_norm = d_query * cos_heads + rotate_back(d_query * sin_heads)
    d_k_norm = d_key * cos_heads + rotate_back(d_key * sin_heads)
    d_q_pre, query_terms = rms_back(q_pre, gain_query, d_q_norm)
    d_k_pre, key_terms = rms_back(k_pre, gain_key, d_k_norm)
    grad_query_gain = jnp.sum(query_terms, axis=(0, 1))
    grad_key_gain = jnp.sum(key_terms, axis=(0, 1))
    d_qkv = jnp.concatenate(
        [
            d_q_pre.astype(jnp.bfloat16).reshape(rows_group, heads_here * HD),
            d_k_pre.astype(jnp.bfloat16).reshape(rows_group, groups_here * HD),
            d_value.reshape(rows_group, groups_here * HD),
        ],
        axis=1,
    )
    (g_qkv,) = wide_scatter([contract_rows(normed_all, d_qkv)])
    d_normed = narrow_scatter(times_transposed(d_qkv, qkv_w), relative)
    d_input_part, attn_gain_terms = rms_back(inputs, gain_attn, d_normed)
    grad_attn_gain = jnp.sum(attn_gain_terms, axis=0)
    d_tokens = d_resid + d_input_part

    gain_grads = lax.psum(
        jnp.concatenate([grad_attn_gain, grad_mlp_gain, grad_query_gain, grad_key_gain]),
        ("wide", "narrow"),
    )
    w = lax.axis_index("wide")
    d_full = d_local * wide_size
    hd_full = hd_local * wide_size
    attn_gain_grad = lax.dynamic_slice_in_dim(gain_grads, w * d_local, d_local)
    mlp_gain_grad = lax.dynamic_slice_in_dim(gain_grads, d_full + w * d_local, d_local)
    query_gain_grad = lax.dynamic_slice_in_dim(gain_grads, 2 * d_full + w * hd_local, hd_local)
    key_gain_grad = lax.dynamic_slice_in_dim(gain_grads, 2 * d_full + hd_full + w * hd_local, hd_local)

    g_query = g_qkv[:, :q_cols]
    g_key = g_qkv[:, q_cols : q_cols + kv_cols]
    g_value = g_qkv[:, q_cols + kv_cols :]
    g_gate = jnp.concatenate([mlp_grads[h][0][:, :ff_half] for h in range(2)], axis=1)
    g_up = jnp.concatenate([mlp_grads[h][0][:, ff_half:] for h in range(2)], axis=1)
    g_down = jnp.concatenate([mlp_grads[h][1] for h in range(2)], axis=1).T
    output = (resid + narrow_scatter(down_partial, relative)).astype(jnp.bfloat16)
    return (
        output,
        d_tokens,
        attn_gain_grad,
        g_query,
        g_key,
        g_value,
        query_gain_grad,
        key_gain_grad,
        g_out_t.T,
        mlp_gain_grad,
        g_gate,
        g_up,
        g_down,
    )


def solution(mesh):
    in_specs = (
        P(("wide", "narrow"), None),
        P("wide", None),
        P(("wide", "narrow"), None),
        P("wide"),
        P("wide", "narrow"),
        P("wide", "narrow"),
        P("wide", "narrow"),
        P("wide"),
        P("wide"),
        P("narrow", "wide"),
        P("wide"),
        P("wide", "narrow"),
        P("wide", "narrow"),
        P("narrow", "wide"),
    )
    out_specs = (
        P(("wide", "narrow"), None),
        P(("wide", "narrow"), None),
        P("wide"),
        P("wide", "narrow"),
        P("wide", "narrow"),
        P("wide", "narrow"),
        P("wide"),
        P("wide"),
        P("narrow", "wide"),
        P("wide"),
        P("wide", "narrow"),
        P("wide", "narrow"),
        P("narrow", "wide"),
    )
    return jax.shard_map(shards, mesh=mesh, in_specs=in_specs, out_specs=out_specs, check_vma=False)
```

```python
import jax
import jax.numpy as jnp
from jax import lax
from jax.sharding import PartitionSpec as P

H = 16
KV = 8
HD = 128


EPS = 1e-06
ROPE_BASE = 1000000.0
NEG_FILL = -1e30

XPERM = [(0, 1), (1, 0), (2, 3), (3, 2)]
YPERM = [(0, 2), (2, 0), (1, 3), (3, 1)]
BLOCK_XOR = (0, 1, 2, 3, 0, 2, 1, 3)


def rms_apply(values, gain):
    return values * lax.rsqrt(jnp.mean(values * values, axis=-1, keepdims=True) + EPS) * gain


def rms_back(values, gain, grad):
    scale = lax.rsqrt(jnp.mean(values * values, axis=-1, keepdims=True) + EPS)
    weighted = grad * gain
    inner = jnp.mean(weighted * values, axis=-1, keepdims=True)
    d_values = scale * weighted - values * (scale * scale * scale) * inner
    return (d_values, grad * values * scale)


def rotate(values):
    half = values.shape[-1] // 2
    return jnp.concatenate([-values[..., half:], values[..., :half]], axis=-1)


def rotate_back(values):
    half = values.shape[-1] // 2
    return jnp.concatenate([values[..., half:], -values[..., :half]], axis=-1)


def doc_positions(doc_rows):
    index = lax.broadcasted_iota(jnp.int32, doc_rows.shape, 1)
    change = jnp.concatenate(
        [jnp.ones((doc_rows.shape[0], 1), jnp.bool_), doc_rows[:, 1:] != doc_rows[:, :-1]], axis=1
    )
    begin = lax.cummax(jnp.where(change, index, 0), axis=1)
    return index - begin


def rope_from_positions(position):
    freqs = ROPE_BASE ** (-(jnp.arange(HD // 2, dtype=jnp.float32) * (2.0 / HD)))
    angle = position.astype(jnp.float32)[..., None] * freqs
    cosine = jnp.cos(angle)
    sine = jnp.sin(angle)
    return (jnp.concatenate([cosine, cosine], axis=-1), jnp.concatenate([sine, sine], axis=-1))


def contract_rows(left, right):
    return lax.dot_general(
        left, right, (((0,), (0,)), ((), ())), preferred_element_type=jnp.float32
    )


def times_transposed(left, right):
    return lax.dot_general(
        left, right, (((1,), (1,)), ((), ())), preferred_element_type=jnp.float32
    )


def relative_ok(seq_count):
    return lax.axis_size("narrow") == 4 and seq_count == 1


def relative_rows(vec):
    n = lax.axis_index("narrow")
    half = vec.shape[0] // 8
    split = vec.reshape(4, 2, half)
    pieces = []
    for blk, flip in enumerate(BLOCK_XOR):
        source = split[:, 1 if blk >= 4 else 0]
        pieces.append(lax.dynamic_index_in_dim(source, jnp.bitwise_xor(n, flip), 0, keepdims=False))
    return jnp.concatenate(pieces)


def narrow_allreduce(v):
    if lax.axis_size("narrow") != 4:
        return lax.psum(v, "narrow")
    v = v + lax.ppermute(v, "narrow", XPERM)
    return v + lax.ppermute(v, "narrow", YPERM)


def narrow_gather(x, relative):
    if not relative:
        return lax.all_gather(x, "narrow", axis=0, tiled=True)
    half = x.shape[0] // 2
    a, b = x[:half], x[half:]
    a_x = lax.ppermute(a, "narrow", XPERM)
    b_y = lax.ppermute(b, "narrow", YPERM)
    a_pair = jnp.concatenate([a, a_x], axis=0)
    b_pair = jnp.concatenate([b, b_y], axis=0)
    a_pair_y = lax.ppermute(a_pair, "narrow", YPERM)
    b_pair_x = lax.ppermute(b_pair, "narrow", XPERM)
    return jnp.concatenate([a_pair, a_pair_y, b_pair, b_pair_x], axis=0)


def narrow_scatter(x, relative):
    if not relative:
        return lax.psum_scatter(
            x.astype(jnp.bfloat16), "narrow", scatter_dimension=0, tiled=True
        ).astype(jnp.float32)
    rows, c = x.shape
    half = rows // 8
    blocks = x.reshape(8, half, c)
    a_got = lax.ppermute(blocks[2:4].astype(jnp.bfloat16), "narrow", YPERM)
    b_got = lax.ppermute(blocks[6:8].astype(jnp.bfloat16), "narrow", XPERM)
    a_sum = blocks[0:2] + a_got.astype(jnp.float32)
    b_sum = blocks[4:6] + b_got.astype(jnp.float32)
    a_got2 = lax.ppermute(a_sum[1].astype(jnp.bfloat16), "narrow", XPERM)
    b_got2 = lax.ppermute(b_sum[1].astype(jnp.bfloat16), "narrow", YPERM)
    return jnp.concatenate(
        [a_sum[0] + a_got2.astype(jnp.float32), b_sum[0] + b_got2.astype(jnp.float32)], axis=0
    )


def split_cols(joined, widths):
    out = []
    start = 0
    for w in widths:
        out.append(joined[:, start : start + w])
        start += w
    return out


def wide_gather(blocks):
    joined = lax.all_gather(jnp.concatenate(blocks, axis=1), "wide", axis=0, tiled=True)
    return split_cols(joined, [blk.shape[1] for blk in blocks])


def wide_scatter(blocks):
    joined = jnp.concatenate([blk.astype(jnp.bfloat16) for blk in blocks], axis=1)
    summed = lax.psum_scatter(joined, "wide", scatter_dimension=0, tiled=True).astype(jnp.float32)
    return split_cols(summed, [blk.shape[1] for blk in blocks])


def shards(
    tokens,
    doc_ids,
    cotangent,
    attn_gain,
    w_query,
    w_key,
    w_value,
    query_gain,
    key_gain,
    w_out,
    mlp_gain,
    w_gate,
    w_up,
    w_down,
):
    narrow_size = lax.axis_size("narrow")
    wide_size = lax.axis_size("wide")
    heads_here = H // narrow_size
    groups_here = KV // narrow_size
    repeat = H // KV
    seq_count, length = doc_ids.shape
    rows_group = seq_count * length
    shard_rows = tokens.shape[0]
    scale = HD ** (-0.5)
    d_local = attn_gain.shape[0]
    hd_local = query_gain.shape[0]
    q_cols = w_query.shape[1]
    kv_cols = w_key.shape[1]
    ff_cols = w_gate.shape[1]
    ff_half = ff_cols // 2
    relative = relative_ok(seq_count)

    tokens_all = narrow_gather(tokens, relative)
    grad_rows = narrow_gather(cotangent, relative)

    gain_block = jnp.zeros((d_local, 128), jnp.bfloat16)
    gain_block = gain_block.at[:, 0].set(attn_gain)
    gain_block = gain_block.at[:, 1].set(mlp_gain)
    gain_block = gain_block.at[:hd_local, 2].set(query_gain)
    gain_block = gain_block.at[:hd_local, 3].set(key_gain)
    qkv_w, out_wt, gains_all = wide_gather(
        [jnp.concatenate([w_query, w_key, w_value], axis=1), w_out.T, gain_block]
    )
    gain_attn = gains_all[:, 0].astype(jnp.float32)
    gain_mlp = gains_all[:, 1].astype(jnp.float32)
    gains_split = gains_all.reshape(wide_size, d_local, 128)
    gain_query = gains_split[:, :hd_local, 2].reshape(-1).astype(jnp.float32)
    gain_key = gains_split[:, :hd_local, 3].reshape(-1).astype(jnp.float32)
    down_t = w_down.T
    mlp_sets = []
    for h in range(2):
        cols = slice(h * ff_half, (h + 1) * ff_half)
        mlp_sets.append(wide_gather([w_gate[:, cols], w_up[:, cols], down_t[:, cols]]))

    if relative:
        order = relative_rows(jnp.arange(rows_group, dtype=jnp.int32))
        doc_row = relative_rows(doc_ids[0])
        position = relative_rows(doc_positions(doc_ids)[0])
    else:
        order = jnp.arange(rows_group, dtype=jnp.int32)
        doc_row = doc_ids.reshape(-1)
        position = doc_positions(doc_ids).reshape(-1)
    cosine, sine = rope_from_positions(position)
    cos_heads = cosine[:, None, :]
    sin_heads = sine[:, None, :]
    allowed = (order[None, :] <= order[:, None]) & (doc_row[None, :] == doc_row[:, None])
    if not relative:
        seq_of = jnp.arange(rows_group, dtype=jnp.int32) // length
        allowed = allowed & (seq_of[None, :] == seq_of[:, None])

    inputs = tokens.astype(jnp.float32)
    normed_all = rms_apply(tokens_all.astype(jnp.float32), gain_attn).astype(jnp.bfloat16)
    qkv = jnp.dot(normed_all, qkv_w, preferred_element_type=jnp.float32)
    q_pre = qkv[:, :q_cols].reshape(rows_group, heads_here, HD)
    k_pre = qkv[:, q_cols : q_cols + kv_cols].reshape(rows_group, groups_here, HD)
    v_use = qkv[:, q_cols + kv_cols :].astype(jnp.bfloat16).reshape(rows_group, groups_here, HD)
    q_norm = rms_apply(q_pre, gain_query)
    k_norm = rms_apply(k_pre, gain_key)
    q_use = (q_norm * cos_heads + rotate(q_norm) * sin_heads).astype(jnp.bfloat16)
    k_use = (k_norm * cos_heads + rotate(k_norm) * sin_heads).astype(jnp.bfloat16)
    q_grouped = q_use.reshape(rows_group, groups_here, repeat, HD)

    scores = jnp.einsum("qgrd,kgd->grqk", q_grouped, k_use, preferred_element_type=jnp.float32) * scale
    scores = jnp.where(allowed, scores, NEG_FILL)
    top = jnp.max(scores, axis=-1, keepdims=True)
    weights = jnp.exp(scores - top)
    total = jnp.sum(weights, axis=-1, keepdims=True)
    probs = weights / total
    mixed = jnp.einsum(
        "grqk,kgd->qgrd", probs.astype(jnp.bfloat16), v_use, preferred_element_type=jnp.float32
    )
    log_totals = (top + jnp.log(total))[..., 0]
    attended = mixed.astype(jnp.bfloat16).reshape(rows_group, heads_here * HD)

    resid = inputs + narrow_scatter(times_transposed(attended, out_wt), relative)
    mlp_in = rms_apply(resid, gain_mlp).astype(jnp.bfloat16)
    mlp_all = narrow_gather(mlp_in, relative)

    down_partial = None
    d_mlp_partial = None
    mlp_grads = []
    for h in range(2):
        gate_w, up_w, down_wt = mlp_sets[h]
        gate = jnp.dot(mlp_all, gate_w, preferred_element_type=jnp.float32)
        up = jnp.dot(mlp_all, up_w, preferred_element_type=jnp.float32)
        sigmoid = jax.nn.sigmoid(gate)
        hidden = (gate * sigmoid * up).astype(jnp.bfloat16)
        part = times_transposed(hidden, down_wt)
        down_partial = part if down_partial is None else down_partial + part
        g_down_t = contract_rows(grad_rows, hidden)
        d_hidden = jnp.dot(grad_rows, down_wt, preferred_element_type=jnp.float32)
        d_up = (d_hidden * gate * sigmoid).astype(jnp.bfloat16)
        d_gate = (d_hidden * up * sigmoid * (1.0 + gate * (1.0 - sigmoid))).astype(jnp.bfloat16)
        g_gate_up = contract_rows(mlp_all, jnp.concatenate([d_gate, d_up], axis=1))
        part = times_transposed(d_gate, gate_w) + times_transposed(d_up, up_w)
        d_mlp_partial = part if d_mlp_partial is None else d_mlp_partial + part
        joined = jnp.concatenate([g_gate_up.astype(jnp.bfloat16), g_down_t.astype(jnp.bfloat16)], axis=1)
        if h == 0:
            joined, mlp_sets[1] = lax.optimization_barrier((joined, mlp_sets[1]))
        else:
            joined, d_mlp_partial = lax.optimization_barrier((joined, d_mlp_partial))
        summed = lax.psum_scatter(joined, "wide", scatter_dimension=0, tiled=True).astype(jnp.float32)
        mlp_grads.append(split_cols(summed, [2 * ff_half, ff_half]))

    d_mlp_in = narrow_scatter(d_mlp_partial, relative)
    d_part, mlp_gain_terms = rms_back(resid, gain_mlp, d_mlp_in)
    grad_mlp_gain = jnp.sum(mlp_gain_terms, axis=0)
    d_resid = cotangent.astype(jnp.float32) + d_part
    branch_rows = narrow_gather(d_resid.astype(jnp.bfloat16), relative)
    (g_out_t,) = wide_scatter([contract_rows(branch_rows, attended)])
    d_attended = jnp.dot(branch_rows, out_wt, preferred_element_type=jnp.float32).astype(jnp.bfloat16)
    d_mixed = d_attended.reshape(rows_group, groups_here, repeat, HD)

    p_scores = jnp.einsum("qgrd,kgd->grqk", q_grouped, k_use, preferred_element_type=jnp.float32) * scale
    p_probs = jnp.where(allowed, jnp.exp(p_scores - log_totals[..., None]), 0.0)
    d_probs = jnp.einsum("qgrd,kgd->grqk", d_mixed, v_use, preferred_element_type=jnp.float32)
    inner = jnp.sum(p_probs * d_probs, axis=-1, keepdims=True)
    d_scores = (p_probs * (d_probs - inner)).astype(jnp.bfloat16)
    d_query = jnp.einsum("grqk,kgd->qgrd", d_scores, k_use, preferred_element_type=jnp.float32) * scale
    d_key = jnp.einsum("grqk,qgrd->kgd", d_scores, q_grouped, preferred_element_type=jnp.float32) * scale
    d_value = jnp.einsum(
        "grqk,qgrd->kgd", p_probs.astype(jnp.bfloat16), d_mixed, preferred_element_type=jnp.float32
    ).astype(jnp.bfloat16)

    d_query = d_query.reshape(rows_group, heads_here, HD)
    d_q_norm = d_query * cos_heads + rotate_back(d_query * sin_heads)
    d_k_norm = d_key * cos_heads + rotate_back(d_key * sin_heads)
    d_q_pre, query_terms = rms_back(q_pre, gain_query, d_q_norm)
    d_k_pre, key_terms = rms_back(k_pre, gain_key, d_k_norm)
    grad_query_gain = jnp.sum(query_terms, axis=(0, 1))
    grad_key_gain = jnp.sum(key_terms, axis=(0, 1))
    d_qkv = jnp.concatenate(
        [
            d_q_pre.astype(jnp.bfloat16).reshape(rows_group, heads_here * HD),
            d_k_pre.astype(jnp.bfloat16).reshape(rows_group, groups_here * HD),
            d_value.reshape(rows_group, groups_here * HD),
        ],
        axis=1,
    )
    d_normed_partial = times_transposed(d_qkv, qkv_w)
    tokens_all_f = tokens_all.astype(jnp.float32)
    scale_all = lax.rsqrt(jnp.mean(tokens_all_f * tokens_all_f, axis=-1, keepdims=True) + EPS)
    attn_gain_part = jnp.sum(d_normed_partial * tokens_all_f * scale_all, axis=0)
    gain_parts = narrow_allreduce(
        jnp.concatenate([attn_gain_part, grad_mlp_gain, grad_query_gain, grad_key_gain])
    )
    d_full = d_local * wide_size
    hd_full = hd_local * wide_size

    def by_chunk(vec, size):
        return jnp.pad(vec.reshape(wide_size, size), ((0, 0), (0, d_local - size)))

    gain_block = jnp.stack(
        [
            by_chunk(gain_parts[:d_full], d_local),
            by_chunk(gain_parts[d_full : 2 * d_full], d_local),
            by_chunk(gain_parts[2 * d_full : 2 * d_full + hd_full], hd_local),
            by_chunk(gain_parts[2 * d_full + hd_full :], hd_local),
        ],
        axis=-1,
    ).reshape(d_full, 4)
    gain_block = jnp.pad(gain_block, ((0, 0), (0, 124)))
    g_qkv, g_gains = wide_scatter([contract_rows(normed_all, d_qkv), gain_block])
    d_normed = narrow_scatter(d_normed_partial, relative)
    d_input_part, unused_terms = rms_back(inputs, gain_attn, d_normed)
    d_tokens = d_resid + d_input_part
    attn_gain_grad = g_gains[:, 0]
    mlp_gain_grad = g_gains[:, 1]
    query_gain_grad = g_gains[:hd_local, 2]
    key_gain_grad = g_gains[:hd_local, 3]

    g_query = g_qkv[:, :q_cols]
    g_key = g_qkv[:, q_cols : q_cols + kv_cols]
    g_value = g_qkv[:, q_cols + kv_cols :]
    g_gate = jnp.concatenate([mlp_grads[h][0][:, :ff_half] for h in range(2)], axis=1)
    g_up = jnp.concatenate([mlp_grads[h][0][:, ff_half:] for h in range(2)], axis=1)
    g_down = jnp.concatenate([mlp_grads[h][1] for h in range(2)], axis=1).T
    output = (resid + narrow_scatter(down_partial, relative)).astype(jnp.bfloat16)
    return (
        output,
        d_tokens,
        attn_gain_grad,
        g_query,
        g_key,
        g_value,
        query_gain_grad,
        key_gain_grad,
        g_out_t.T,
        mlp_gain_grad,
        g_gate,
        g_up,
        g_down,
    )


def solution(mesh):
    in_specs = (
        P(("wide", "narrow"), None),
        P("wide", None),
        P(("wide", "narrow"), None),
        P("wide"),
        P("wide", "narrow"),
        P("wide", "narrow"),
        P("wide", "narrow"),
        P("wide"),
        P("wide"),
        P("narrow", "wide"),
        P("wide"),
        P("wide", "narrow"),
        P("wide", "narrow"),
        P("narrow", "wide"),
    )
    out_specs = (
        P(("wide", "narrow"), None),
        P(("wide", "narrow"), None),
        P("wide"),
        P("wide", "narrow"),
        P("wide", "narrow"),
        P("wide", "narrow"),
        P("wide"),
        P("wide"),
        P("narrow", "wide"),
        P("wide"),
        P("wide", "narrow"),
        P("wide", "narrow"),
        P("narrow", "wide"),
    )
    return jax.shard_map(shards, mesh=mesh, in_specs=in_specs, out_specs=out_specs, check_vma=False)
```

```python
import jax
import jax.numpy as jnp
from jax import lax
from jax.sharding import PartitionSpec as P

H = 16
KV = 8
HD = 128


EPS = 1e-06
ROPE_BASE = 1000000.0
NEG_FILL = -1e30

XPERM = [(0, 1), (1, 0), (2, 3), (3, 2)]
YPERM = [(0, 2), (2, 0), (1, 3), (3, 1)]
BLOCK_XOR = (0, 1, 2, 3, 0, 2, 1, 3)


def rms_apply(values, gain):
    return values * lax.rsqrt(jnp.mean(values * values, axis=-1, keepdims=True) + EPS) * gain


def rms_back(values, gain, grad):
    scale = lax.rsqrt(jnp.mean(values * values, axis=-1, keepdims=True) + EPS)
    weighted = grad * gain
    inner = jnp.mean(weighted * values, axis=-1, keepdims=True)
    d_values = scale * weighted - values * (scale * scale * scale) * inner
    return (d_values, grad * values * scale)


def rotate(values):
    half = values.shape[-1] // 2
    return jnp.concatenate([-values[..., half:], values[..., :half]], axis=-1)


def rotate_back(values):
    half = values.shape[-1] // 2
    return jnp.concatenate([values[..., half:], -values[..., :half]], axis=-1)


def doc_positions(doc_rows):
    index = lax.broadcasted_iota(jnp.int32, doc_rows.shape, 1)
    change = jnp.concatenate(
        [jnp.ones((doc_rows.shape[0], 1), jnp.bool_), doc_rows[:, 1:] != doc_rows[:, :-1]], axis=1
    )
    begin = lax.cummax(jnp.where(change, index, 0), axis=1)
    return index - begin


def rope_from_positions(position):
    freqs = ROPE_BASE ** (-(jnp.arange(HD // 2, dtype=jnp.float32) * (2.0 / HD)))
    angle = position.astype(jnp.float32)[..., None] * freqs
    cosine = jnp.cos(angle)
    sine = jnp.sin(angle)
    return (jnp.concatenate([cosine, cosine], axis=-1), jnp.concatenate([sine, sine], axis=-1))


def contract_rows(left, right):
    return lax.dot_general(
        left, right, (((0,), (0,)), ((), ())), preferred_element_type=jnp.float32
    )


def times_transposed(left, right):
    return lax.dot_general(
        left, right, (((1,), (1,)), ((), ())), preferred_element_type=jnp.float32
    )


def relative_ok(seq_count):
    return lax.axis_size("narrow") == 4 and seq_count == 1


def relative_rows(vec):
    n = lax.axis_index("narrow")
    half = vec.shape[0] // 8
    split = vec.reshape(4, 2, half)
    pieces = []
    for blk, flip in enumerate(BLOCK_XOR):
        source = split[:, 1 if blk >= 4 else 0]
        pieces.append(lax.dynamic_index_in_dim(source, jnp.bitwise_xor(n, flip), 0, keepdims=False))
    return jnp.concatenate(pieces)


def narrow_allreduce(v):
    if lax.axis_size("narrow") != 4:
        return lax.psum(v, "narrow")
    v = v + lax.ppermute(v, "narrow", XPERM)
    return v + lax.ppermute(v, "narrow", YPERM)


def narrow_gather(x, relative):
    if not relative:
        return lax.all_gather(x, "narrow", axis=0, tiled=True)
    half = x.shape[0] // 2
    a, b = x[:half], x[half:]
    a_x = lax.ppermute(a, "narrow", XPERM)
    b_y = lax.ppermute(b, "narrow", YPERM)
    a_pair = jnp.concatenate([a, a_x], axis=0)
    b_pair = jnp.concatenate([b, b_y], axis=0)
    a_pair_y = lax.ppermute(a_pair, "narrow", YPERM)
    b_pair_x = lax.ppermute(b_pair, "narrow", XPERM)
    return jnp.concatenate([a_pair, a_pair_y, b_pair, b_pair_x], axis=0)


def narrow_scatter(x, relative):
    if not relative:
        return lax.psum_scatter(
            x.astype(jnp.bfloat16), "narrow", scatter_dimension=0, tiled=True
        ).astype(jnp.float32)
    rows, c = x.shape
    half = rows // 8
    blocks = x.reshape(8, half, c)
    a_got = lax.ppermute(blocks[2:4].astype(jnp.bfloat16), "narrow", YPERM)
    b_got = lax.ppermute(blocks[6:8].astype(jnp.bfloat16), "narrow", XPERM)
    a_sum = blocks[0:2] + a_got.astype(jnp.float32)
    b_sum = blocks[4:6] + b_got.astype(jnp.float32)
    a_got2 = lax.ppermute(a_sum[1].astype(jnp.bfloat16), "narrow", XPERM)
    b_got2 = lax.ppermute(b_sum[1].astype(jnp.bfloat16), "narrow", YPERM)
    return jnp.concatenate(
        [a_sum[0] + a_got2.astype(jnp.float32), b_sum[0] + b_got2.astype(jnp.float32)], axis=0
    )


def split_cols(joined, widths):
    out = []
    start = 0
    for w in widths:
        out.append(joined[:, start : start + w])
        start += w
    return out


def wide_gather(blocks):
    joined = lax.all_gather(jnp.concatenate(blocks, axis=1), "wide", axis=0, tiled=True)
    return split_cols(joined, [blk.shape[1] for blk in blocks])


def wide_scatter(blocks):
    joined = jnp.concatenate([blk.astype(jnp.bfloat16) for blk in blocks], axis=1)
    summed = lax.psum_scatter(joined, "wide", scatter_dimension=0, tiled=True).astype(jnp.float32)
    return split_cols(summed, [blk.shape[1] for blk in blocks])


def shards(
    tokens,
    doc_ids,
    cotangent,
    attn_gain,
    w_query,
    w_key,
    w_value,
    query_gain,
    key_gain,
    w_out,
    mlp_gain,
    w_gate,
    w_up,
    w_down,
):
    narrow_size = lax.axis_size("narrow")
    wide_size = lax.axis_size("wide")
    heads_here = H // narrow_size
    groups_here = KV // narrow_size
    repeat = H // KV
    seq_count, length = doc_ids.shape
    rows_group = seq_count * length
    shard_rows = tokens.shape[0]
    scale = HD ** (-0.5)
    d_local = attn_gain.shape[0]
    hd_local = query_gain.shape[0]
    q_cols = w_query.shape[1]
    kv_cols = w_key.shape[1]
    ff_cols = w_gate.shape[1]
    ff_half = ff_cols // 2
    relative = relative_ok(seq_count)

    tokens_all = narrow_gather(tokens, relative)
    grad_rows = narrow_gather(cotangent, relative)

    gain_block = jnp.zeros((d_local, 128), jnp.bfloat16)
    gain_block = gain_block.at[:, 0].set(attn_gain)
    gain_block = gain_block.at[:, 1].set(mlp_gain)
    gain_block = gain_block.at[:hd_local, 2].set(query_gain)
    gain_block = gain_block.at[:hd_local, 3].set(key_gain)
    qkv_w, out_wt, gains_all = wide_gather(
        [jnp.concatenate([w_query, w_key, w_value], axis=1), w_out.T, gain_block]
    )
    gain_attn = gains_all[:, 0].astype(jnp.float32)
    gain_mlp = gains_all[:, 1].astype(jnp.float32)
    gains_split = gains_all.reshape(wide_size, d_local, 128)
    gain_query = gains_split[:, :hd_local, 2].reshape(-1).astype(jnp.float32)
    gain_key = gains_split[:, :hd_local, 3].reshape(-1).astype(jnp.float32)
    down_t = w_down.T
    mlp_sets = []
    for h in range(2):
        cols = slice(h * ff_half, (h + 1) * ff_half)
        mlp_sets.append(wide_gather([w_gate[:, cols], w_up[:, cols], down_t[:, cols]]))

    if relative:
        order = relative_rows(jnp.arange(rows_group, dtype=jnp.int32))
        doc_row = relative_rows(doc_ids[0])
        position = relative_rows(doc_positions(doc_ids)[0])
    else:
        order = jnp.arange(rows_group, dtype=jnp.int32)
        doc_row = doc_ids.reshape(-1)
        position = doc_positions(doc_ids).reshape(-1)
    cosine, sine = rope_from_positions(position)
    cos_heads = cosine[:, None, :]
    sin_heads = sine[:, None, :]
    allowed = (order[None, :] <= order[:, None]) & (doc_row[None, :] == doc_row[:, None])
    if not relative:
        seq_of = jnp.arange(rows_group, dtype=jnp.int32) // length
        allowed = allowed & (seq_of[None, :] == seq_of[:, None])

    inputs = tokens.astype(jnp.float32)
    normed_all = rms_apply(tokens_all.astype(jnp.float32), gain_attn).astype(jnp.bfloat16)
    qkv = jnp.dot(normed_all, qkv_w, preferred_element_type=jnp.float32)
    q_pre = qkv[:, :q_cols].reshape(rows_group, heads_here, HD)
    k_pre = qkv[:, q_cols : q_cols + kv_cols].reshape(rows_group, groups_here, HD)
    v_use = qkv[:, q_cols + kv_cols :].astype(jnp.bfloat16).reshape(rows_group, groups_here, HD)
    q_norm = rms_apply(q_pre, gain_query)
    k_norm = rms_apply(k_pre, gain_key)
    q_use = (q_norm * cos_heads + rotate(q_norm) * sin_heads).astype(jnp.bfloat16)
    k_use = (k_norm * cos_heads + rotate(k_norm) * sin_heads).astype(jnp.bfloat16)
    q_grouped = q_use.reshape(rows_group, groups_here, repeat, HD)

    scores = jnp.einsum("qgrd,kgd->grqk", q_grouped, k_use, preferred_element_type=jnp.float32) * scale
    scores = jnp.where(allowed, scores, NEG_FILL)
    top = jnp.max(scores, axis=-1, keepdims=True)
    weights = jnp.exp(scores - top)
    total = jnp.sum(weights, axis=-1, keepdims=True)
    probs = weights / total
    mixed = jnp.einsum(
        "grqk,kgd->qgrd", probs.astype(jnp.bfloat16), v_use, preferred_element_type=jnp.float32
    )
    log_totals = (top + jnp.log(total))[..., 0]
    attended = mixed.astype(jnp.bfloat16).reshape(rows_group, heads_here * HD)

    resid = inputs + narrow_scatter(times_transposed(attended, out_wt), relative)
    mlp_in = rms_apply(resid, gain_mlp).astype(jnp.bfloat16)
    mlp_all = narrow_gather(mlp_in, relative)

    down_partial = None
    d_mlp_partial = None
    mlp_grads = []
    for h in range(2):
        gate_w, up_w, down_wt = mlp_sets[h]
        gate = jnp.dot(mlp_all, gate_w, preferred_element_type=jnp.float32)
        up = jnp.dot(mlp_all, up_w, preferred_element_type=jnp.float32)
        sigmoid = jax.nn.sigmoid(gate)
        hidden = (gate * sigmoid * up).astype(jnp.bfloat16)
        part = times_transposed(hidden, down_wt)
        down_partial = part if down_partial is None else down_partial + part
        g_down_t = contract_rows(grad_rows, hidden)
        d_hidden = jnp.dot(grad_rows, down_wt, preferred_element_type=jnp.float32)
        d_up = (d_hidden * gate * sigmoid).astype(jnp.bfloat16)
        d_gate = (d_hidden * up * sigmoid * (1.0 + gate * (1.0 - sigmoid))).astype(jnp.bfloat16)
        g_gate_up = contract_rows(mlp_all, jnp.concatenate([d_gate, d_up], axis=1))
        part = times_transposed(d_gate, gate_w) + times_transposed(d_up, up_w)
        d_mlp_partial = part if d_mlp_partial is None else d_mlp_partial + part
        joined = jnp.concatenate([g_gate_up.astype(jnp.bfloat16), g_down_t.astype(jnp.bfloat16)], axis=1)
        if h == 0:
            joined, mlp_sets[1] = lax.optimization_barrier((joined, mlp_sets[1]))
        else:
            joined, d_mlp_partial = lax.optimization_barrier((joined, d_mlp_partial))
        mlp_grads.append(lax.psum_scatter(joined, "wide", scatter_dimension=0, tiled=True))

    d_mlp_in = narrow_scatter(d_mlp_partial, relative)
    d_part, mlp_gain_terms = rms_back(resid, gain_mlp, d_mlp_in)
    grad_mlp_gain = jnp.sum(mlp_gain_terms, axis=0)
    d_resid = cotangent.astype(jnp.float32) + d_part
    branch_rows = narrow_gather(d_resid.astype(jnp.bfloat16), relative)
    out_grad = contract_rows(branch_rows, attended).astype(jnp.bfloat16)
    mlp_grads, out_grad = lax.optimization_barrier((mlp_grads, out_grad))
    mlp_grads = [split_cols(g.astype(jnp.float32), [2 * ff_half, ff_half]) for g in mlp_grads]
    g_out_t = lax.psum_scatter(out_grad, "wide", scatter_dimension=0, tiled=True).astype(jnp.float32)
    d_attended = jnp.dot(branch_rows, out_wt, preferred_element_type=jnp.float32).astype(jnp.bfloat16)
    d_mixed = d_attended.reshape(rows_group, groups_here, repeat, HD)

    p_scores = jnp.einsum("qgrd,kgd->grqk", q_grouped, k_use, preferred_element_type=jnp.float32) * scale
    p_probs = jnp.where(allowed, jnp.exp(p_scores - log_totals[..., None]), 0.0)
    d_probs = jnp.einsum("qgrd,kgd->grqk", d_mixed, v_use, preferred_element_type=jnp.float32)
    inner = jnp.sum(p_probs * d_probs, axis=-1, keepdims=True)
    d_scores = (p_probs * (d_probs - inner)).astype(jnp.bfloat16)
    d_query = jnp.einsum("grqk,kgd->qgrd", d_scores, k_use, preferred_element_type=jnp.float32) * scale
    d_key = jnp.einsum("grqk,qgrd->kgd", d_scores, q_grouped, preferred_element_type=jnp.float32) * scale
    d_value = jnp.einsum(
        "grqk,qgrd->kgd", p_probs.astype(jnp.bfloat16), d_mixed, preferred_element_type=jnp.float32
    ).astype(jnp.bfloat16)

    d_query = d_query.reshape(rows_group, heads_here, HD)
    d_q_norm = d_query * cos_heads + rotate_back(d_query * sin_heads)
    d_k_norm = d_key * cos_heads + rotate_back(d_key * sin_heads)
    d_q_pre, query_terms = rms_back(q_pre, gain_query, d_q_norm)
    d_k_pre, key_terms = rms_back(k_pre, gain_key, d_k_norm)
    grad_query_gain = jnp.sum(query_terms, axis=(0, 1))
    grad_key_gain = jnp.sum(key_terms, axis=(0, 1))
    d_qkv = jnp.concatenate(
        [
            d_q_pre.astype(jnp.bfloat16).reshape(rows_group, heads_here * HD),
            d_k_pre.astype(jnp.bfloat16).reshape(rows_group, groups_here * HD),
            d_value.reshape(rows_group, groups_here * HD),
        ],
        axis=1,
    )
    d_normed_partial = times_transposed(d_qkv, qkv_w)
    tokens_all_f = tokens_all.astype(jnp.float32)
    scale_all = lax.rsqrt(jnp.mean(tokens_all_f * tokens_all_f, axis=-1, keepdims=True) + EPS)
    attn_gain_part = jnp.sum(d_normed_partial * tokens_all_f * scale_all, axis=0)
    gain_parts = narrow_allreduce(
        jnp.concatenate([attn_gain_part, grad_mlp_gain, grad_query_gain, grad_key_gain])
    )
    d_full = d_local * wide_size
    hd_full = hd_local * wide_size

    def by_chunk(vec, size):
        return jnp.pad(vec.reshape(wide_size, size), ((0, 0), (0, d_local - size)))

    gain_block = jnp.stack(
        [
            by_chunk(gain_parts[:d_full], d_local),
            by_chunk(gain_parts[d_full : 2 * d_full], d_local),
            by_chunk(gain_parts[2 * d_full : 2 * d_full + hd_full], hd_local),
            by_chunk(gain_parts[2 * d_full + hd_full :], hd_local),
        ],
        axis=-1,
    ).reshape(d_full, 4)
    gain_block = jnp.pad(gain_block, ((0, 0), (0, 124)))
    qkv_grad = jnp.concatenate(
        [contract_rows(normed_all, d_qkv).astype(jnp.bfloat16), gain_block.astype(jnp.bfloat16)], axis=1
    )
    g_out_t, qkv_grad = lax.optimization_barrier((g_out_t, qkv_grad))
    g_qkv, g_gains = split_cols(
        lax.psum_scatter(qkv_grad, "wide", scatter_dimension=0, tiled=True).astype(jnp.float32),
        [q_cols + 2 * kv_cols, 128],
    )
    d_normed = narrow_scatter(d_normed_partial, relative)
    d_input_part, unused_terms = rms_back(inputs, gain_attn, d_normed)
    d_tokens = d_resid + d_input_part
    attn_gain_grad = g_gains[:, 0]
    mlp_gain_grad = g_gains[:, 1]
    query_gain_grad = g_gains[:hd_local, 2]
    key_gain_grad = g_gains[:hd_local, 3]

    g_query = g_qkv[:, :q_cols]
    g_key = g_qkv[:, q_cols : q_cols + kv_cols]
    g_value = g_qkv[:, q_cols + kv_cols :]
    g_gate = jnp.concatenate([mlp_grads[h][0][:, :ff_half] for h in range(2)], axis=1)
    g_up = jnp.concatenate([mlp_grads[h][0][:, ff_half:] for h in range(2)], axis=1)
    g_down = jnp.concatenate([mlp_grads[h][1] for h in range(2)], axis=1).T
    output = (resid + narrow_scatter(down_partial, relative)).astype(jnp.bfloat16)
    return (
        output,
        d_tokens,
        attn_gain_grad,
        g_query,
        g_key,
        g_value,
        query_gain_grad,
        key_gain_grad,
        g_out_t.T,
        mlp_gain_grad,
        g_gate,
        g_up,
        g_down,
    )


def solution(mesh):
    in_specs = (
        P(("wide", "narrow"), None),
        P("wide", None),
        P(("wide", "narrow"), None),
        P("wide"),
        P("wide", "narrow"),
        P("wide", "narrow"),
        P("wide", "narrow"),
        P("wide"),
        P("wide"),
        P("narrow", "wide"),
        P("wide"),
        P("wide", "narrow"),
        P("wide", "narrow"),
        P("narrow", "wide"),
    )
    out_specs = (
        P(("wide", "narrow"), None),
        P(("wide", "narrow"), None),
        P("wide"),
        P("wide", "narrow"),
        P("wide", "narrow"),
        P("wide", "narrow"),
        P("wide"),
        P("wide"),
        P("narrow", "wide"),
        P("wide"),
        P("wide", "narrow"),
        P("wide", "narrow"),
        P("narrow", "wide"),
    )
    return jax.shard_map(shards, mesh=mesh, in_specs=in_specs, out_specs=out_specs, check_vma=False)
```

```python
import jax
import jax.numpy as jnp
from jax import lax
from jax.sharding import PartitionSpec as P

H = 16
KV = 8
HD = 128


EPS = 1e-06
ROPE_BASE = 1000000.0
NEG_FILL = -1e30

XPERM = [(0, 1), (1, 0), (2, 3), (3, 2)]
YPERM = [(0, 2), (2, 0), (1, 3), (3, 1)]
BLOCK_XOR = (0, 1, 2, 3, 0, 2, 1, 3)


def rms_apply(values, gain):
    return values * lax.rsqrt(jnp.mean(values * values, axis=-1, keepdims=True) + EPS) * gain


def rms_back(values, gain, grad):
    scale = lax.rsqrt(jnp.mean(values * values, axis=-1, keepdims=True) + EPS)
    weighted = grad * gain
    inner = jnp.mean(weighted * values, axis=-1, keepdims=True)
    d_values = scale * weighted - values * (scale * scale * scale) * inner
    return (d_values, grad * values * scale)


def rotate(values):
    half = values.shape[-1] // 2
    return jnp.concatenate([-values[..., half:], values[..., :half]], axis=-1)


def rotate_back(values):
    half = values.shape[-1] // 2
    return jnp.concatenate([values[..., half:], -values[..., :half]], axis=-1)


def doc_positions(doc_rows):
    index = lax.broadcasted_iota(jnp.int32, doc_rows.shape, 1)
    change = jnp.concatenate(
        [jnp.ones((doc_rows.shape[0], 1), jnp.bool_), doc_rows[:, 1:] != doc_rows[:, :-1]], axis=1
    )
    begin = lax.cummax(jnp.where(change, index, 0), axis=1)
    return index - begin


def rope_from_positions(position):
    freqs = ROPE_BASE ** (-(jnp.arange(HD // 2, dtype=jnp.float32) * (2.0 / HD)))
    angle = position.astype(jnp.float32)[..., None] * freqs
    cosine = jnp.cos(angle)
    sine = jnp.sin(angle)
    return (jnp.concatenate([cosine, cosine], axis=-1), jnp.concatenate([sine, sine], axis=-1))


def contract_rows(left, right):
    return lax.dot_general(
        left, right, (((0,), (0,)), ((), ())), preferred_element_type=jnp.float32
    )


def times_transposed(left, right):
    return lax.dot_general(
        left, right, (((1,), (1,)), ((), ())), preferred_element_type=jnp.float32
    )


def relative_ok(seq_count):
    return lax.axis_size("narrow") == 4 and seq_count == 1


def relative_rows(vec):
    n = lax.axis_index("narrow")
    half = vec.shape[0] // 8
    split = vec.reshape(4, 2, half)
    pieces = []
    for blk, flip in enumerate(BLOCK_XOR):
        source = split[:, 1 if blk >= 4 else 0]
        pieces.append(lax.dynamic_index_in_dim(source, jnp.bitwise_xor(n, flip), 0, keepdims=False))
    return jnp.concatenate(pieces)


def narrow_allreduce(v):
    if lax.axis_size("narrow") != 4:
        return lax.psum(v, "narrow")
    v = v + lax.ppermute(v, "narrow", XPERM)
    return v + lax.ppermute(v, "narrow", YPERM)


def narrow_gather(x, relative):
    if not relative:
        return lax.all_gather(x, "narrow", axis=0, tiled=True)
    half = x.shape[0] // 2
    a, b = x[:half], x[half:]
    a_x = lax.ppermute(a, "narrow", XPERM)
    b_y = lax.ppermute(b, "narrow", YPERM)
    a_pair = jnp.concatenate([a, a_x], axis=0)
    b_pair = jnp.concatenate([b, b_y], axis=0)
    a_pair_y = lax.ppermute(a_pair, "narrow", YPERM)
    b_pair_x = lax.ppermute(b_pair, "narrow", XPERM)
    return jnp.concatenate([a_pair, a_pair_y, b_pair, b_pair_x], axis=0)


def narrow_scatter(x, relative):
    if not relative:
        return lax.psum_scatter(
            x.astype(jnp.bfloat16), "narrow", scatter_dimension=0, tiled=True
        ).astype(jnp.float32)
    rows, c = x.shape
    half = rows // 8
    blocks = x.reshape(8, half, c)
    a_got = lax.ppermute(blocks[2:4].astype(jnp.bfloat16), "narrow", YPERM)
    b_got = lax.ppermute(blocks[6:8].astype(jnp.bfloat16), "narrow", XPERM)
    a_sum = blocks[0:2] + a_got.astype(jnp.float32)
    b_sum = blocks[4:6] + b_got.astype(jnp.float32)
    a_got2 = lax.ppermute(a_sum[1].astype(jnp.bfloat16), "narrow", XPERM)
    b_got2 = lax.ppermute(b_sum[1].astype(jnp.bfloat16), "narrow", YPERM)
    return jnp.concatenate(
        [a_sum[0] + a_got2.astype(jnp.float32), b_sum[0] + b_got2.astype(jnp.float32)], axis=0
    )


def split_cols(joined, widths):
    out = []
    start = 0
    for w in widths:
        out.append(joined[:, start : start + w])
        start += w
    return out


def wide_gather(blocks):
    joined = lax.all_gather(jnp.concatenate(blocks, axis=1), "wide", axis=0, tiled=True)
    return split_cols(joined, [blk.shape[1] for blk in blocks])


def wide_scatter(blocks):
    joined = jnp.concatenate([blk.astype(jnp.bfloat16) for blk in blocks], axis=1)
    summed = lax.psum_scatter(joined, "wide", scatter_dimension=0, tiled=True).astype(jnp.float32)
    return split_cols(summed, [blk.shape[1] for blk in blocks])


def shards(
    tokens,
    doc_ids,
    cotangent,
    attn_gain,
    w_query,
    w_key,
    w_value,
    query_gain,
    key_gain,
    w_out,
    mlp_gain,
    w_gate,
    w_up,
    w_down,
):
    narrow_size = lax.axis_size("narrow")
    wide_size = lax.axis_size("wide")
    heads_here = H // narrow_size
    groups_here = KV // narrow_size
    repeat = H // KV
    seq_count, length = doc_ids.shape
    rows_group = seq_count * length
    shard_rows = tokens.shape[0]
    scale = HD ** (-0.5)
    d_local = attn_gain.shape[0]
    hd_local = query_gain.shape[0]
    q_cols = w_query.shape[1]
    kv_cols = w_key.shape[1]
    ff_cols = w_gate.shape[1]
    ff_half = ff_cols // 2
    relative = relative_ok(seq_count)

    tokens_all = narrow_gather(tokens, relative)
    grad_rows = narrow_gather(cotangent, relative)

    pad_hd = ((0, d_local - hd_local),)
    gain_block = jnp.pad(
        jnp.stack(
            [attn_gain, mlp_gain, jnp.pad(query_gain, pad_hd), jnp.pad(key_gain, pad_hd)], axis=1
        ),
        ((0, 0), (0, 124)),
    )
    qkv_w, out_wt, gains_all = wide_gather(
        [jnp.concatenate([w_query, w_key, w_value], axis=1), w_out.T, gain_block]
    )
    gain_attn = gains_all[:, 0].astype(jnp.float32)
    gain_mlp = gains_all[:, 1].astype(jnp.float32)
    gains_split = gains_all.reshape(wide_size, d_local, 128)
    gain_query = gains_split[:, :hd_local, 2].reshape(-1).astype(jnp.float32)
    gain_key = gains_split[:, :hd_local, 3].reshape(-1).astype(jnp.float32)
    down_t = w_down.T
    mlp_sets = []
    for h in range(2):
        cols = slice(h * ff_half, (h + 1) * ff_half)
        mlp_sets.append(wide_gather([w_gate[:, cols], w_up[:, cols], down_t[:, cols]]))

    if relative:
        order = relative_rows(jnp.arange(rows_group, dtype=jnp.int32))
        doc_row = relative_rows(doc_ids[0])
        position = relative_rows(doc_positions(doc_ids)[0])
    else:
        order = jnp.arange(rows_group, dtype=jnp.int32)
        doc_row = doc_ids.reshape(-1)
        position = doc_positions(doc_ids).reshape(-1)
    cosine, sine = rope_from_positions(position)
    cos_heads = cosine[:, None, :]
    sin_heads = sine[:, None, :]
    allowed = (order[None, :] <= order[:, None]) & (doc_row[None, :] == doc_row[:, None])
    if not relative:
        seq_of = jnp.arange(rows_group, dtype=jnp.int32) // length
        allowed = allowed & (seq_of[None, :] == seq_of[:, None])

    inputs = tokens.astype(jnp.float32)
    normed_all = rms_apply(tokens_all.astype(jnp.float32), gain_attn).astype(jnp.bfloat16)
    qkv = jnp.dot(normed_all, qkv_w, preferred_element_type=jnp.float32)
    q_pre = qkv[:, :q_cols].reshape(rows_group, heads_here, HD)
    k_pre = qkv[:, q_cols : q_cols + kv_cols].reshape(rows_group, groups_here, HD)
    v_use = qkv[:, q_cols + kv_cols :].astype(jnp.bfloat16).reshape(rows_group, groups_here, HD)
    q_norm = rms_apply(q_pre, gain_query)
    k_norm = rms_apply(k_pre, gain_key)
    q_use = (q_norm * cos_heads + rotate(q_norm) * sin_heads).astype(jnp.bfloat16)
    k_use = (k_norm * cos_heads + rotate(k_norm) * sin_heads).astype(jnp.bfloat16)
    q_grouped = q_use.reshape(rows_group, groups_here, repeat, HD)

    scores = jnp.einsum("qgrd,kgd->grqk", q_grouped, k_use, preferred_element_type=jnp.float32) * scale
    scores = jnp.where(allowed, scores, NEG_FILL)
    top = jnp.max(scores, axis=-1, keepdims=True)
    weights = jnp.exp(scores - top)
    total = jnp.sum(weights, axis=-1, keepdims=True)
    probs = weights / total
    mixed = jnp.einsum(
        "grqk,kgd->qgrd", probs.astype(jnp.bfloat16), v_use, preferred_element_type=jnp.float32
    )
    log_totals = (top + jnp.log(total))[..., 0]
    attended = mixed.astype(jnp.bfloat16).reshape(rows_group, heads_here * HD)

    resid = inputs + narrow_scatter(times_transposed(attended, out_wt), relative)
    mlp_in = rms_apply(resid, gain_mlp).astype(jnp.bfloat16)
    mlp_all = narrow_gather(mlp_in, relative)

    down_partial = None
    d_mlp_partial = None
    mlp_grads = []
    for h in range(2):
        gate_w, up_w, down_wt = mlp_sets[h]
        gate = jnp.dot(mlp_all, gate_w, preferred_element_type=jnp.float32)
        up = jnp.dot(mlp_all, up_w, preferred_element_type=jnp.float32)
        sigmoid = jax.nn.sigmoid(gate)
        hidden = (gate * sigmoid * up).astype(jnp.bfloat16)
        part = times_transposed(hidden, down_wt)
        down_partial = part if down_partial is None else down_partial + part
        g_down_t = contract_rows(grad_rows, hidden)
        d_hidden = jnp.dot(grad_rows, down_wt, preferred_element_type=jnp.float32)
        d_up = (d_hidden * gate * sigmoid).astype(jnp.bfloat16)
        d_gate = (d_hidden * up * sigmoid * (1.0 + gate * (1.0 - sigmoid))).astype(jnp.bfloat16)
        g_gate_up = contract_rows(mlp_all, jnp.concatenate([d_gate, d_up], axis=1))
        part = times_transposed(d_gate, gate_w) + times_transposed(d_up, up_w)
        d_mlp_partial = part if d_mlp_partial is None else d_mlp_partial + part
        joined = jnp.concatenate([g_gate_up.astype(jnp.bfloat16), g_down_t.astype(jnp.bfloat16)], axis=1)
        if h == 0:
            joined, mlp_sets[1] = lax.optimization_barrier((joined, mlp_sets[1]))
            mlp_grads.append(lax.psum_scatter(joined, "wide", scatter_dimension=0, tiled=True))
        else:
            last_joined = joined

    d_mlp_in = narrow_scatter(d_mlp_partial, relative)
    d_part, mlp_gain_terms = rms_back(resid, gain_mlp, d_mlp_in)
    grad_mlp_gain = jnp.sum(mlp_gain_terms, axis=0)
    d_resid = cotangent.astype(jnp.float32) + d_part
    p_scores = jnp.einsum("qgrd,kgd->grqk", q_grouped, k_use, preferred_element_type=jnp.float32) * scale
    p_probs = jnp.where(allowed, jnp.exp(p_scores - log_totals[..., None]), 0.0)
    d_resid_low, p_probs, last_joined = lax.optimization_barrier(
        (d_resid.astype(jnp.bfloat16), p_probs, last_joined)
    )
    mlp_grads.append(lax.psum_scatter(last_joined, "wide", scatter_dimension=0, tiled=True))
    branch_rows = narrow_gather(d_resid_low, relative)
    out_grad = contract_rows(branch_rows, attended).astype(jnp.bfloat16)
    mlp_grads, out_grad = lax.optimization_barrier((mlp_grads, out_grad))
    mlp_grads = [split_cols(g.astype(jnp.float32), [2 * ff_half, ff_half]) for g in mlp_grads]
    g_out_t = lax.psum_scatter(out_grad, "wide", scatter_dimension=0, tiled=True).astype(jnp.float32)
    d_attended = jnp.dot(branch_rows, out_wt, preferred_element_type=jnp.float32).astype(jnp.bfloat16)
    d_mixed = d_attended.reshape(rows_group, groups_here, repeat, HD)

    d_probs = jnp.einsum("qgrd,kgd->grqk", d_mixed, v_use, preferred_element_type=jnp.float32)
    inner = jnp.sum(p_probs * d_probs, axis=-1, keepdims=True)
    d_scores = (p_probs * (d_probs - inner)).astype(jnp.bfloat16)
    d_query = jnp.einsum("grqk,kgd->qgrd", d_scores, k_use, preferred_element_type=jnp.float32) * scale
    d_key = jnp.einsum("grqk,qgrd->kgd", d_scores, q_grouped, preferred_element_type=jnp.float32) * scale
    d_value = jnp.einsum(
        "grqk,qgrd->kgd", p_probs.astype(jnp.bfloat16), d_mixed, preferred_element_type=jnp.float32
    ).astype(jnp.bfloat16)

    d_query = d_query.reshape(rows_group, heads_here, HD)
    d_q_norm = d_query * cos_heads + rotate_back(d_query * sin_heads)
    d_k_norm = d_key * cos_heads + rotate_back(d_key * sin_heads)
    d_q_pre, query_terms = rms_back(q_pre, gain_query, d_q_norm)
    d_k_pre, key_terms = rms_back(k_pre, gain_key, d_k_norm)
    grad_query_gain = jnp.sum(query_terms, axis=(0, 1))
    grad_key_gain = jnp.sum(key_terms, axis=(0, 1))
    d_qkv = jnp.concatenate(
        [
            d_q_pre.astype(jnp.bfloat16).reshape(rows_group, heads_here * HD),
            d_k_pre.astype(jnp.bfloat16).reshape(rows_group, groups_here * HD),
            d_value.reshape(rows_group, groups_here * HD),
        ],
        axis=1,
    )
    d_normed_partial = times_transposed(d_qkv, qkv_w)
    tokens_all_f = tokens_all.astype(jnp.float32)
    scale_all = lax.rsqrt(jnp.mean(tokens_all_f * tokens_all_f, axis=-1, keepdims=True) + EPS)
    attn_gain_part = jnp.sum(d_normed_partial * tokens_all_f * scale_all, axis=0)
    gain_parts = narrow_allreduce(
        jnp.concatenate([attn_gain_part, grad_mlp_gain, grad_query_gain, grad_key_gain])
    )
    d_full = d_local * wide_size
    hd_full = hd_local * wide_size

    def by_chunk(vec, size):
        return jnp.pad(vec.reshape(wide_size, size), ((0, 0), (0, d_local - size)))

    gain_block = jnp.stack(
        [
            by_chunk(gain_parts[:d_full], d_local),
            by_chunk(gain_parts[d_full : 2 * d_full], d_local),
            by_chunk(gain_parts[2 * d_full : 2 * d_full + hd_full], hd_local),
            by_chunk(gain_parts[2 * d_full + hd_full :], hd_local),
        ],
        axis=-1,
    ).reshape(d_full, 4)
    gain_block = jnp.pad(gain_block, ((0, 0), (0, 124)))
    qkv_grad = jnp.concatenate(
        [contract_rows(normed_all, d_qkv).astype(jnp.bfloat16), gain_block.astype(jnp.bfloat16)], axis=1
    )
    g_out_t, qkv_grad = lax.optimization_barrier((g_out_t, qkv_grad))
    g_qkv, g_gains = split_cols(
        lax.psum_scatter(qkv_grad, "wide", scatter_dimension=0, tiled=True).astype(jnp.float32),
        [q_cols + 2 * kv_cols, 128],
    )
    d_normed = narrow_scatter(d_normed_partial, relative)
    d_input_part, unused_terms = rms_back(inputs, gain_attn, d_normed)
    d_tokens = d_resid + d_input_part
    attn_gain_grad = g_gains[:, 0]
    mlp_gain_grad = g_gains[:, 1]
    query_gain_grad = g_gains[:hd_local, 2]
    key_gain_grad = g_gains[:hd_local, 3]

    g_query = g_qkv[:, :q_cols]
    g_key = g_qkv[:, q_cols : q_cols + kv_cols]
    g_value = g_qkv[:, q_cols + kv_cols :]
    g_gate = jnp.concatenate([mlp_grads[h][0][:, :ff_half] for h in range(2)], axis=1)
    g_up = jnp.concatenate([mlp_grads[h][0][:, ff_half:] for h in range(2)], axis=1)
    g_down = jnp.concatenate([mlp_grads[h][1] for h in range(2)], axis=1).T
    output = (resid + narrow_scatter(down_partial, relative)).astype(jnp.bfloat16)
    return (
        output,
        d_tokens,
        attn_gain_grad,
        g_query,
        g_key,
        g_value,
        query_gain_grad,
        key_gain_grad,
        g_out_t.T,
        mlp_gain_grad,
        g_gate,
        g_up,
        g_down,
    )


def solution(mesh):
    in_specs = (
        P(("wide", "narrow"), None),
        P("wide", None),
        P(("wide", "narrow"), None),
        P("wide"),
        P("wide", "narrow"),
        P("wide", "narrow"),
        P("wide", "narrow"),
        P("wide"),
        P("wide"),
        P("narrow", "wide"),
        P("wide"),
        P("wide", "narrow"),
        P("wide", "narrow"),
        P("narrow", "wide"),
    )
    out_specs = (
        P(("wide", "narrow"), None),
        P(("wide", "narrow"), None),
        P("wide"),
        P("wide", "narrow"),
        P("wide", "narrow"),
        P("wide", "narrow"),
        P("wide"),
        P("wide"),
        P("narrow", "wide"),
        P("wide"),
        P("wide", "narrow"),
        P("wide", "narrow"),
        P("narrow", "wide"),
    )
    return jax.shard_map(shards, mesh=mesh, in_specs=in_specs, out_specs=out_specs, check_vma=False)
```

```python
import jax
import jax.numpy as jnp
from jax import lax
from jax.sharding import PartitionSpec as P


H = 16
KV = 8
HD = 128


EPS = 1e-06
ROPE_BASE = 1000000.0
NEG_FILL = -1e30

XPERM = [(0, 1), (1, 0), (2, 3), (3, 2)]
YPERM = [(0, 2), (2, 0), (1, 3), (3, 1)]
BLOCK_XOR = (0, 1, 2, 3, 0, 2, 1, 3)


def rms_apply(values, gain):
    return values * lax.rsqrt(jnp.mean(values * values, axis=-1, keepdims=True) + EPS) * gain


def rms_back(values, gain, grad):
    scale = lax.rsqrt(jnp.mean(values * values, axis=-1, keepdims=True) + EPS)
    weighted = grad * gain
    inner = jnp.mean(weighted * values, axis=-1, keepdims=True)
    d_values = scale * weighted - values * (scale * scale * scale) * inner
    return (d_values, grad * values * scale)


def rotate(values):
    half = values.shape[-1] // 2
    return jnp.concatenate([-values[..., half:], values[..., :half]], axis=-1)


def rotate_back(values):
    half = values.shape[-1] // 2
    return jnp.concatenate([values[..., half:], -values[..., :half]], axis=-1)


def doc_positions(doc_rows):
    index = lax.broadcasted_iota(jnp.int32, doc_rows.shape, 1)
    change = jnp.concatenate(
        [jnp.ones((doc_rows.shape[0], 1), jnp.bool_), doc_rows[:, 1:] != doc_rows[:, :-1]], axis=1
    )
    begin = lax.cummax(jnp.where(change, index, 0), axis=1)
    return index - begin


def rope_from_positions(position):
    freqs = ROPE_BASE ** (-(jnp.arange(HD // 2, dtype=jnp.float32) * (2.0 / HD)))
    angle = position.astype(jnp.float32)[..., None] * freqs
    cosine = jnp.cos(angle)
    sine = jnp.sin(angle)
    return (jnp.concatenate([cosine, cosine], axis=-1), jnp.concatenate([sine, sine], axis=-1))


def contract_rows(left, right):
    return lax.dot_general(
        left, right, (((0,), (0,)), ((), ())), preferred_element_type=jnp.float32
    )


def times_transposed(left, right):
    return lax.dot_general(
        left, right, (((1,), (1,)), ((), ())), preferred_element_type=jnp.float32
    )


def relative_ok(seq_count):
    return lax.axis_size("narrow") == 4 and seq_count == 1


def relative_rows(vec):
    n = lax.axis_index("narrow")
    half = vec.shape[0] // 8
    split = vec.reshape(4, 2, half)
    pieces = []
    for blk, flip in enumerate(BLOCK_XOR):
        source = split[:, 1 if blk >= 4 else 0]
        pieces.append(lax.dynamic_index_in_dim(source, jnp.bitwise_xor(n, flip), 0, keepdims=False))
    return jnp.concatenate(pieces)


def narrow_allreduce(v):
    if lax.axis_size("narrow") != 4:
        return lax.psum(v, "narrow")
    v = v + lax.ppermute(v, "narrow", XPERM)
    return v + lax.ppermute(v, "narrow", YPERM)


def narrow_gather(x, relative):
    if not relative:
        return lax.all_gather(x, "narrow", axis=0, tiled=True)
    half = x.shape[0] // 2
    a, b = x[:half], x[half:]
    a_x = lax.ppermute(a, "narrow", XPERM)
    b_y = lax.ppermute(b, "narrow", YPERM)
    a_pair = jnp.concatenate([a, a_x], axis=0)
    b_pair = jnp.concatenate([b, b_y], axis=0)
    a_pair_y = lax.ppermute(a_pair, "narrow", YPERM)
    b_pair_x = lax.ppermute(b_pair, "narrow", XPERM)
    return jnp.concatenate([a_pair, a_pair_y, b_pair, b_pair_x], axis=0)


def narrow_scatter(x, relative):
    if not relative:
        return lax.psum_scatter(
            x.astype(jnp.bfloat16), "narrow", scatter_dimension=0, tiled=True
        ).astype(jnp.float32)
    rows, c = x.shape
    half = rows // 8
    blocks = x.reshape(8, half, c)
    a_got = lax.ppermute(blocks[2:4].astype(jnp.bfloat16), "narrow", YPERM)
    b_got = lax.ppermute(blocks[6:8].astype(jnp.bfloat16), "narrow", XPERM)
    a_sum = blocks[0:2] + a_got.astype(jnp.float32)
    b_sum = blocks[4:6] + b_got.astype(jnp.float32)
    a_got2 = lax.ppermute(a_sum[1].astype(jnp.bfloat16), "narrow", XPERM)
    b_got2 = lax.ppermute(b_sum[1].astype(jnp.bfloat16), "narrow", YPERM)
    return jnp.concatenate(
        [a_sum[0] + a_got2.astype(jnp.float32), b_sum[0] + b_got2.astype(jnp.float32)], axis=0
    )


def split_cols(joined, widths):
    out = []
    start = 0
    for w in widths:
        out.append(joined[:, start : start + w])
        start += w
    return out


def wide_gather(blocks):
    joined = lax.all_gather(jnp.concatenate(blocks, axis=1), "wide", axis=0, tiled=True)
    return split_cols(joined, [blk.shape[1] for blk in blocks])


def qkv_scatter(grad):
    return lax.psum_scatter(grad, "wide", scatter_dimension=0, tiled=True)


def shards_body(
    tokens,
    doc_ids,
    cotangent,
    attn_gain,
    w_query,
    w_key,
    w_value,
    query_gain,
    key_gain,
    w_out,
    mlp_gain,
    w_gate,
    w_up,
    w_down,
):
    narrow_size = lax.axis_size("narrow")
    wide_size = lax.axis_size("wide")
    heads_here = H // narrow_size
    groups_here = KV // narrow_size
    repeat = H // KV
    seq_count, length = doc_ids.shape
    rows_group = seq_count * length
    scale = HD ** (-0.5)
    d_local = attn_gain.shape[0]
    hd_local = query_gain.shape[0]
    q_cols = w_query.shape[1]
    kv_cols = w_key.shape[1]
    ff_cols = w_gate.shape[1]
    ff_half = ff_cols // 2
    relative = relative_ok(seq_count)

    tokens_all = narrow_gather(tokens, relative)
    grad_rows = narrow_gather(cotangent, relative)

    pad_hd = ((0, d_local - hd_local),)
    gain_block = jnp.pad(
        jnp.stack(
            [attn_gain, mlp_gain, jnp.pad(query_gain, pad_hd), jnp.pad(key_gain, pad_hd)], axis=1
        ),
        ((0, 0), (0, 124)),
    )
    qkv_w, out_wt, gains_all = wide_gather(
        [jnp.concatenate([w_query, w_key, w_value], axis=1), w_out.T, gain_block]
    )
    gain_attn = gains_all[:, 0].astype(jnp.float32)
    gain_mlp = gains_all[:, 1].astype(jnp.float32)
    gains_split = gains_all.reshape(wide_size, d_local, 128)
    gain_query = gains_split[:, :hd_local, 2].reshape(-1).astype(jnp.float32)
    gain_key = gains_split[:, :hd_local, 3].reshape(-1).astype(jnp.float32)
    down_t = w_down.T
    mlp_sets = []
    for h in range(2):
        cols = slice(h * ff_half, (h + 1) * ff_half)
        mlp_sets.append(wide_gather([w_gate[:, cols], w_up[:, cols], down_t[:, cols]]))

    if relative:
        order = relative_rows(jnp.arange(rows_group, dtype=jnp.int32))
        doc_row = relative_rows(doc_ids[0])
        position = relative_rows(doc_positions(doc_ids)[0])
    else:
        order = jnp.arange(rows_group, dtype=jnp.int32)
        doc_row = doc_ids.reshape(-1)
        position = doc_positions(doc_ids).reshape(-1)
    cosine, sine = rope_from_positions(position)
    cos_heads = cosine[:, None, :]
    sin_heads = sine[:, None, :]
    allowed = (order[None, :] <= order[:, None]) & (doc_row[None, :] == doc_row[:, None])
    if not relative:
        seq_of = jnp.arange(rows_group, dtype=jnp.int32) // length
        allowed = allowed & (seq_of[None, :] == seq_of[:, None])

    inputs = tokens.astype(jnp.float32)
    normed_all = rms_apply(tokens_all.astype(jnp.float32), gain_attn).astype(jnp.bfloat16)
    qkv = jnp.dot(normed_all, qkv_w, preferred_element_type=jnp.float32)
    q_pre = qkv[:, :q_cols].reshape(rows_group, heads_here, HD)
    k_pre = qkv[:, q_cols : q_cols + kv_cols].reshape(rows_group, groups_here, HD)
    v_use = qkv[:, q_cols + kv_cols :].astype(jnp.bfloat16).reshape(rows_group, groups_here, HD)
    q_norm = rms_apply(q_pre, gain_query)
    k_norm = rms_apply(k_pre, gain_key)
    q_use = (q_norm * cos_heads + rotate(q_norm) * sin_heads).astype(jnp.bfloat16)
    k_use = (k_norm * cos_heads + rotate(k_norm) * sin_heads).astype(jnp.bfloat16)
    q_grouped = q_use.reshape(rows_group, groups_here, repeat, HD)

    scores = jnp.einsum("qgrd,kgd->grqk", q_grouped, k_use, preferred_element_type=jnp.float32) * scale
    scores = jnp.where(allowed, scores, NEG_FILL)
    top = jnp.max(scores, axis=-1, keepdims=True)
    weights = jnp.exp(scores - top)
    total = jnp.sum(weights, axis=-1, keepdims=True)
    probs = weights / total
    mixed = jnp.einsum(
        "grqk,kgd->qgrd", probs.astype(jnp.bfloat16), v_use, preferred_element_type=jnp.float32
    )
    log_totals = (top + jnp.log(total))[..., 0]
    attended = mixed.astype(jnp.bfloat16).reshape(rows_group, heads_here * HD)

    resid = inputs + narrow_scatter(times_transposed(attended, out_wt), relative)
    mlp_in = rms_apply(resid, gain_mlp).astype(jnp.bfloat16)
    mlp_all = narrow_gather(mlp_in, relative)

    down_partial = None
    d_mlp_partial = None
    mlp_grads = []
    for h in range(2):
      gate_w, up_w, down_wt = mlp_sets[h]
      gate = jnp.dot(mlp_all, gate_w, preferred_element_type=jnp.float32)
      up = jnp.dot(mlp_all, up_w, preferred_element_type=jnp.float32)
      sigmoid = jax.nn.sigmoid(gate)
      hidden = (gate * sigmoid * up).astype(jnp.bfloat16)
      part = times_transposed(hidden, down_wt)
      down_partial = part if down_partial is None else down_partial + part
      g_down_t = contract_rows(grad_rows, hidden)
      d_hidden = jnp.dot(grad_rows, down_wt, preferred_element_type=jnp.float32)
      d_up = (d_hidden * gate * sigmoid).astype(jnp.bfloat16)
      d_gate = (d_hidden * up * sigmoid * (1.0 + gate * (1.0 - sigmoid))).astype(jnp.bfloat16)
      g_gate_up = contract_rows(mlp_all, jnp.concatenate([d_gate, d_up], axis=1))
      part = times_transposed(d_gate, gate_w) + times_transposed(d_up, up_w)
      d_mlp_partial = part if d_mlp_partial is None else d_mlp_partial + part
      joined = jnp.concatenate([g_gate_up.astype(jnp.bfloat16), g_down_t.astype(jnp.bfloat16)], axis=1)
      if h == 0:
          joined, mlp_sets[1] = lax.optimization_barrier((joined, mlp_sets[1]))
          mlp_grads.append(lax.psum_scatter(joined, "wide", scatter_dimension=0, tiled=True))
      else:
          last_joined = joined

    d_mlp_in = narrow_scatter(d_mlp_partial, relative)
    d_part, mlp_gain_terms = rms_back(resid, gain_mlp, d_mlp_in)
    grad_mlp_gain = jnp.sum(mlp_gain_terms, axis=0)
    d_resid = cotangent.astype(jnp.float32) + d_part
    p_scores = jnp.einsum("qgrd,kgd->grqk", q_grouped, k_use, preferred_element_type=jnp.float32) * scale
    p_probs = jnp.where(allowed, jnp.exp(p_scores - log_totals[..., None]), 0.0)
    d_resid_low, p_probs, last_joined = lax.optimization_barrier(
        (d_resid.astype(jnp.bfloat16), p_probs, last_joined)
    )
    mlp_grads.append(lax.psum_scatter(last_joined, "wide", scatter_dimension=0, tiled=True))
    branch_rows = narrow_gather(d_resid_low, relative)
    out_grad = contract_rows(branch_rows, attended).astype(jnp.bfloat16)
    g_out_t = lax.psum_scatter(out_grad, "wide", scatter_dimension=0, tiled=True)
    d_attended = jnp.dot(branch_rows, out_wt, preferred_element_type=jnp.float32).astype(jnp.bfloat16)
    d_mixed = d_attended.reshape(rows_group, groups_here, repeat, HD)

    d_probs = jnp.einsum("qgrd,kgd->grqk", d_mixed, v_use, preferred_element_type=jnp.float32)
    inner = jnp.sum(p_probs * d_probs, axis=-1, keepdims=True)
    d_scores = (p_probs * (d_probs - inner)).astype(jnp.bfloat16)
    d_query = jnp.einsum("grqk,kgd->qgrd", d_scores, k_use, preferred_element_type=jnp.float32) * scale
    d_key = jnp.einsum("grqk,qgrd->kgd", d_scores, q_grouped, preferred_element_type=jnp.float32) * scale
    d_value = jnp.einsum(
        "grqk,qgrd->kgd", p_probs.astype(jnp.bfloat16), d_mixed, preferred_element_type=jnp.float32
    ).astype(jnp.bfloat16)

    d_query = d_query.reshape(rows_group, heads_here, HD)
    d_q_norm = d_query * cos_heads + rotate_back(d_query * sin_heads)
    d_k_norm = d_key * cos_heads + rotate_back(d_key * sin_heads)
    d_q_pre, query_terms = rms_back(q_pre, gain_query, d_q_norm)
    d_k_pre, key_terms = rms_back(k_pre, gain_key, d_k_norm)
    grad_query_gain = jnp.sum(query_terms, axis=(0, 1))
    grad_key_gain = jnp.sum(key_terms, axis=(0, 1))
    d_qkv = jnp.concatenate(
        [
            d_q_pre.astype(jnp.bfloat16).reshape(rows_group, heads_here * HD),
            d_k_pre.astype(jnp.bfloat16).reshape(rows_group, groups_here * HD),
            d_value.reshape(rows_group, groups_here * HD),
        ],
        axis=1,
    )
    d_normed_partial = times_transposed(d_qkv, qkv_w)
    tokens_all_f = tokens_all.astype(jnp.float32)
    scale_all = lax.rsqrt(jnp.mean(tokens_all_f * tokens_all_f, axis=-1, keepdims=True) + EPS)
    attn_gain_part = jnp.sum(d_normed_partial * tokens_all_f * scale_all, axis=0)
    gain_parts = narrow_allreduce(
        jnp.concatenate([attn_gain_part, grad_mlp_gain, grad_query_gain, grad_key_gain])
    )
    d_full = d_local * wide_size
    hd_full = hd_local * wide_size

    def by_chunk(vec, size):
        return jnp.pad(vec.reshape(wide_size, size), ((0, 0), (0, d_local - size)))

    gain_block = jnp.stack(
        [
            by_chunk(gain_parts[:d_full], d_local),
            by_chunk(gain_parts[d_full : 2 * d_full], d_local),
            by_chunk(gain_parts[2 * d_full : 2 * d_full + hd_full], hd_local),
            by_chunk(gain_parts[2 * d_full + hd_full :], hd_local),
        ],
        axis=-1,
    ).reshape(d_full, 4)
    gain_block = jnp.pad(gain_block, ((0, 0), (0, 124)))
    qkv_grad = jnp.concatenate(
        [contract_rows(normed_all, d_qkv).astype(jnp.bfloat16), gain_block.astype(jnp.bfloat16)], axis=1
    )
    g_out_t = g_out_t.astype(jnp.float32)
    mlp_grads = [split_cols(g.astype(jnp.float32), [2 * ff_half, ff_half]) for g in mlp_grads]
    g_qkv, g_gains = split_cols(
        qkv_scatter(qkv_grad).astype(jnp.float32),
        [q_cols + 2 * kv_cols, 128],
    )
    d_normed = narrow_scatter(d_normed_partial, relative)
    d_input_part, _ = rms_back(inputs, gain_attn, d_normed)
    d_tokens = d_resid + d_input_part
    attn_gain_grad = g_gains[:, 0]
    mlp_gain_grad = g_gains[:, 1]
    query_gain_grad = g_gains[:hd_local, 2]
    key_gain_grad = g_gains[:hd_local, 3]

    g_query = g_qkv[:, :q_cols]
    g_key = g_qkv[:, q_cols : q_cols + kv_cols]
    g_value = g_qkv[:, q_cols + kv_cols :]
    g_gate = jnp.concatenate([mlp_grads[h][0][:, :ff_half] for h in range(2)], axis=1)
    g_up = jnp.concatenate([mlp_grads[h][0][:, ff_half:] for h in range(2)], axis=1)
    g_down = jnp.concatenate([mlp_grads[h][1] for h in range(2)], axis=1).T
    output = (resid + narrow_scatter(down_partial, relative)).astype(jnp.bfloat16)
    return (
        output,
        d_tokens,
        attn_gain_grad,
        g_query,
        g_key,
        g_value,
        query_gain_grad,
        key_gain_grad,
        g_out_t.T,
        mlp_gain_grad,
        g_gate,
        g_up,
        g_down,
    )


def solution(mesh):
    in_specs = (
        P(("wide", "narrow"), None),
        P("wide", None),
        P(("wide", "narrow"), None),
        P("wide"),
        P("wide", "narrow"),
        P("wide", "narrow"),
        P("wide", "narrow"),
        P("wide"),
        P("wide"),
        P("narrow", "wide"),
        P("wide"),
        P("wide", "narrow"),
        P("wide", "narrow"),
        P("narrow", "wide"),
    )
    out_specs = (
        P(("wide", "narrow"), None),
        P(("wide", "narrow"), None),
        P("wide"),
        P("wide", "narrow"),
        P("wide", "narrow"),
        P("wide", "narrow"),
        P("wide"),
        P("wide"),
        P("narrow", "wide"),
        P("wide"),
        P("wide", "narrow"),
        P("wide", "narrow"),
        P("narrow", "wide"),
    )
    return jax.shard_map(shards_body, mesh=mesh, in_specs=in_specs, out_specs=out_specs, check_vma=False)
```

```python
import jax
import jax.numpy as jnp
from jax import lax
from jax.sharding import PartitionSpec as P


H = 16
KV = 8
HD = 128


EPS = 1e-06
ROPE_BASE = 1000000.0
NEG_FILL = -1e30

XPERM = [(0, 1), (1, 0), (2, 3), (3, 2)]
YPERM = [(0, 2), (2, 0), (1, 3), (3, 1)]
BLOCK_XOR = (0, 1, 2, 3, 0, 2, 1, 3)


def rms_apply(values, gain):
    return values * lax.rsqrt(jnp.mean(values * values, axis=-1, keepdims=True) + EPS) * gain


def rms_back(values, gain, grad):
    scale = lax.rsqrt(jnp.mean(values * values, axis=-1, keepdims=True) + EPS)
    weighted = grad * gain
    inner = jnp.mean(weighted * values, axis=-1, keepdims=True)
    d_values = scale * weighted - values * (scale * scale * scale) * inner
    return (d_values, grad * values * scale)


def rotate(values):
    half = values.shape[-1] // 2
    return jnp.concatenate([-values[..., half:], values[..., :half]], axis=-1)


def rotate_back(values):
    half = values.shape[-1] // 2
    return jnp.concatenate([values[..., half:], -values[..., :half]], axis=-1)


def doc_positions(doc_rows):
    index = lax.broadcasted_iota(jnp.int32, doc_rows.shape, 1)
    change = jnp.concatenate(
        [jnp.ones((doc_rows.shape[0], 1), jnp.bool_), doc_rows[:, 1:] != doc_rows[:, :-1]], axis=1
    )
    begin = lax.cummax(jnp.where(change, index, 0), axis=1)
    return index - begin


def rope_from_positions(position):
    freqs = ROPE_BASE ** (-(jnp.arange(HD // 2, dtype=jnp.float32) * (2.0 / HD)))
    angle = position.astype(jnp.float32)[..., None] * freqs
    cosine = jnp.cos(angle)
    sine = jnp.sin(angle)
    return (jnp.concatenate([cosine, cosine], axis=-1), jnp.concatenate([sine, sine], axis=-1))


def contract_rows(left, right):
    return lax.dot_general(
        left, right, (((0,), (0,)), ((), ())), preferred_element_type=jnp.float32
    )


def times_transposed(left, right):
    return lax.dot_general(
        left, right, (((1,), (1,)), ((), ())), preferred_element_type=jnp.float32
    )


def relative_ok(seq_count):
    return lax.axis_size("narrow") == 4 and seq_count == 1


def relative_rows(vec):
    n = lax.axis_index("narrow")
    half = vec.shape[0] // 8
    split = vec.reshape(4, 2, half)
    pieces = []
    for blk, flip in enumerate(BLOCK_XOR):
        source = split[:, 1 if blk >= 4 else 0]
        pieces.append(lax.dynamic_index_in_dim(source, jnp.bitwise_xor(n, flip), 0, keepdims=False))
    return jnp.concatenate(pieces)


def narrow_allreduce(v):
    if lax.axis_size("narrow") != 4:
        return lax.psum(v, "narrow")
    v = v + lax.ppermute(v, "narrow", XPERM)
    return v + lax.ppermute(v, "narrow", YPERM)


def narrow_gather(x, relative):
    if not relative:
        return lax.all_gather(x, "narrow", axis=0, tiled=True)
    half = x.shape[0] // 2
    a, b = x[:half], x[half:]
    a_x = lax.ppermute(a, "narrow", XPERM)
    b_y = lax.ppermute(b, "narrow", YPERM)
    a_pair = jnp.concatenate([a, a_x], axis=0)
    b_pair = jnp.concatenate([b, b_y], axis=0)
    a_pair_y = lax.ppermute(a_pair, "narrow", YPERM)
    b_pair_x = lax.ppermute(b_pair, "narrow", XPERM)
    return jnp.concatenate([a_pair, a_pair_y, b_pair, b_pair_x], axis=0)


def narrow_scatter(x, relative):
    if not relative:
        return lax.psum_scatter(
            x.astype(jnp.bfloat16), "narrow", scatter_dimension=0, tiled=True
        ).astype(jnp.float32)
    rows, c = x.shape
    half = rows // 8
    blocks = x.reshape(8, half, c)
    a_got = lax.ppermute(blocks[2:4].astype(jnp.bfloat16), "narrow", YPERM)
    b_got = lax.ppermute(blocks[6:8].astype(jnp.bfloat16), "narrow", XPERM)
    a_sum = blocks[0:2] + a_got.astype(jnp.float32)
    b_sum = blocks[4:6] + b_got.astype(jnp.float32)
    a_got2 = lax.ppermute(a_sum[1].astype(jnp.bfloat16), "narrow", XPERM)
    b_got2 = lax.ppermute(b_sum[1].astype(jnp.bfloat16), "narrow", YPERM)
    return jnp.concatenate(
        [a_sum[0] + a_got2.astype(jnp.float32), b_sum[0] + b_got2.astype(jnp.float32)], axis=0
    )


def split_cols(joined, widths):
    out = []
    start = 0
    for w in widths:
        out.append(joined[:, start : start + w])
        start += w
    return out


def wide_gather(blocks):
    joined = lax.all_gather(jnp.concatenate(blocks, axis=1), "wide", axis=0, tiled=True)
    return split_cols(joined, [blk.shape[1] for blk in blocks])


def shards_body(
    tokens,
    doc_ids,
    cotangent,
    attn_gain,
    w_query,
    w_key,
    w_value,
    query_gain,
    key_gain,
    w_out,
    mlp_gain,
    w_gate,
    w_up,
    w_down,
):
    narrow_size = lax.axis_size("narrow")
    wide_size = lax.axis_size("wide")
    heads_here = H // narrow_size
    groups_here = KV // narrow_size
    repeat = H // KV
    seq_count, length = doc_ids.shape
    rows_group = seq_count * length
    scale = HD ** (-0.5)
    d_local = attn_gain.shape[0]
    hd_local = query_gain.shape[0]
    q_cols = w_query.shape[1]
    kv_cols = w_key.shape[1]
    ff_cols = w_gate.shape[1]
    ff_half = ff_cols // 2
    relative = relative_ok(seq_count)

    tokens_all = narrow_gather(tokens, relative)
    grad_rows = narrow_gather(cotangent, relative)

    pad_hd = ((0, d_local - hd_local),)
    gain_block = jnp.pad(
        jnp.stack(
            [attn_gain, mlp_gain, jnp.pad(query_gain, pad_hd), jnp.pad(key_gain, pad_hd)], axis=1
        ),
        ((0, 0), (0, 124)),
    )
    qkv_w, out_wt, gains_all = wide_gather(
        [jnp.concatenate([w_query, w_key, w_value], axis=1), w_out.T, gain_block]
    )
    gain_attn = gains_all[:, 0].astype(jnp.float32)
    gain_mlp = gains_all[:, 1].astype(jnp.float32)
    gains_split = gains_all.reshape(wide_size, d_local, 128)
    gain_query = gains_split[:, :hd_local, 2].reshape(-1).astype(jnp.float32)
    gain_key = gains_split[:, :hd_local, 3].reshape(-1).astype(jnp.float32)
    down_t = w_down.T
    mlp_sets = []
    for h in range(2):
        cols = slice(h * ff_half, (h + 1) * ff_half)
        mlp_sets.append(wide_gather([w_gate[:, cols], w_up[:, cols], down_t[:, cols]]))

    if relative:
        order = relative_rows(jnp.arange(rows_group, dtype=jnp.int32))
        doc_row = relative_rows(doc_ids[0])
        position = relative_rows(doc_positions(doc_ids)[0])
    else:
        order = jnp.arange(rows_group, dtype=jnp.int32)
        doc_row = doc_ids.reshape(-1)
        position = doc_positions(doc_ids).reshape(-1)
    cosine, sine = rope_from_positions(position)
    cos_heads = cosine[:, None, :]
    sin_heads = sine[:, None, :]
    allowed = (order[None, :] <= order[:, None]) & (doc_row[None, :] == doc_row[:, None])
    if not relative:
        seq_of = jnp.arange(rows_group, dtype=jnp.int32) // length
        allowed = allowed & (seq_of[None, :] == seq_of[:, None])

    inputs = tokens.astype(jnp.float32)
    normed_all = rms_apply(tokens_all.astype(jnp.float32), gain_attn).astype(jnp.bfloat16)
    qkv = jnp.dot(normed_all, qkv_w, preferred_element_type=jnp.float32)
    q_pre = qkv[:, :q_cols].reshape(rows_group, heads_here, HD)
    k_pre = qkv[:, q_cols : q_cols + kv_cols].reshape(rows_group, groups_here, HD)
    v_use = qkv[:, q_cols + kv_cols :].astype(jnp.bfloat16).reshape(rows_group, groups_here, HD)
    q_norm = rms_apply(q_pre, gain_query)
    k_norm = rms_apply(k_pre, gain_key)
    q_use = (q_norm * cos_heads + rotate(q_norm) * sin_heads).astype(jnp.bfloat16)
    k_use = (k_norm * cos_heads + rotate(k_norm) * sin_heads).astype(jnp.bfloat16)
    q_grouped = q_use.reshape(rows_group, groups_here, repeat, HD)

    scores = jnp.einsum("qgrd,kgd->grqk", q_grouped, k_use, preferred_element_type=jnp.float32) * scale
    scores = jnp.where(allowed, scores, NEG_FILL)
    top = jnp.max(scores, axis=-1, keepdims=True)
    weights = jnp.exp(scores - top)
    total = jnp.sum(weights, axis=-1, keepdims=True)
    probs = weights / total
    mixed = jnp.einsum(
        "grqk,kgd->qgrd", probs.astype(jnp.bfloat16), v_use, preferred_element_type=jnp.float32
    )
    log_totals = (top + jnp.log(total))[..., 0]
    attended = mixed.astype(jnp.bfloat16).reshape(rows_group, heads_here * HD)

    resid = inputs + narrow_scatter(times_transposed(attended, out_wt), relative)
    mlp_in = rms_apply(resid, gain_mlp).astype(jnp.bfloat16)
    mlp_all = narrow_gather(mlp_in, relative)

    down_partial = None
    d_mlp_partial = None
    mlp_grads = []
    for h in range(2):
        gate_w, up_w, down_wt = mlp_sets[h]
        gate = jnp.dot(mlp_all, gate_w, preferred_element_type=jnp.float32)
        up = jnp.dot(mlp_all, up_w, preferred_element_type=jnp.float32)
        sigmoid = jax.nn.sigmoid(gate)
        hidden = (gate * sigmoid * up).astype(jnp.bfloat16)
        part = times_transposed(hidden, down_wt)
        down_partial = part if down_partial is None else down_partial + part
        d_hidden = jnp.dot(grad_rows, down_wt, preferred_element_type=jnp.float32)
        d_up = (d_hidden * gate * sigmoid).astype(jnp.bfloat16)
        d_gate = (d_hidden * up * sigmoid * (1.0 + gate * (1.0 - sigmoid))).astype(jnp.bfloat16)
        part = times_transposed(d_gate, gate_w) + times_transposed(d_up, up_w)
        d_mlp_partial = part if d_mlp_partial is None else d_mlp_partial + part
        g_down_t = contract_rows(grad_rows, hidden)
        g_gate_up = contract_rows(mlp_all, jnp.concatenate([d_gate, d_up], axis=1))
        joined = jnp.concatenate(
            [g_gate_up.astype(jnp.bfloat16), g_down_t.astype(jnp.bfloat16)], axis=1
        )
        if h == 0:
            joined, mlp_sets[1] = lax.optimization_barrier((joined, mlp_sets[1]))
            mlp_grads.append(lax.psum_scatter(joined, "wide", scatter_dimension=0, tiled=True))
        else:
            last_joined = joined

    d_mlp_in = narrow_scatter(d_mlp_partial, relative)
    d_part, mlp_gain_terms = rms_back(resid, gain_mlp, d_mlp_in)
    grad_mlp_gain = jnp.sum(mlp_gain_terms, axis=0)
    d_resid = cotangent.astype(jnp.float32) + d_part
    p_scores = (
        jnp.einsum("qgrd,kgd->grqk", q_grouped, k_use, preferred_element_type=jnp.float32) * scale
    )
    p_probs = jnp.where(allowed, jnp.exp(p_scores - log_totals[..., None]), 0.0)
    d_resid_low, last_joined = lax.optimization_barrier((d_resid.astype(jnp.bfloat16), last_joined))
    mlp_grads.append(lax.psum_scatter(last_joined, "wide", scatter_dimension=0, tiled=True))
    branch_rows = narrow_gather(d_resid_low, relative)
    out_grad = contract_rows(branch_rows, attended).astype(jnp.bfloat16)
    mlp_grads, out_grad = lax.optimization_barrier((mlp_grads, out_grad))
    mlp_grads = [split_cols(g.astype(jnp.float32), [2 * ff_half, ff_half]) for g in mlp_grads]
    g_out_t = lax.psum_scatter(out_grad, "wide", scatter_dimension=0, tiled=True).astype(jnp.float32)
    d_attended = jnp.dot(branch_rows, out_wt, preferred_element_type=jnp.float32).astype(jnp.bfloat16)
    d_mixed = d_attended.reshape(rows_group, groups_here, repeat, HD)

    d_probs = jnp.einsum("qgrd,kgd->grqk", d_mixed, v_use, preferred_element_type=jnp.float32)
    inner = jnp.sum(p_probs * d_probs, axis=-1, keepdims=True)
    d_scores = (p_probs * (d_probs - inner)).astype(jnp.bfloat16)
    d_query = jnp.einsum("grqk,kgd->qgrd", d_scores, k_use, preferred_element_type=jnp.float32) * scale
    d_key = jnp.einsum("grqk,qgrd->kgd", d_scores, q_grouped, preferred_element_type=jnp.float32) * scale
    d_value = jnp.einsum(
        "grqk,qgrd->kgd", p_probs.astype(jnp.bfloat16), d_mixed, preferred_element_type=jnp.float32
    ).astype(jnp.bfloat16)

    d_query = d_query.reshape(rows_group, heads_here, HD)
    d_q_norm = d_query * cos_heads + rotate_back(d_query * sin_heads)
    d_k_norm = d_key * cos_heads + rotate_back(d_key * sin_heads)
    d_q_pre, query_terms = rms_back(q_pre, gain_query, d_q_norm)
    d_k_pre, key_terms = rms_back(k_pre, gain_key, d_k_norm)
    grad_query_gain = jnp.sum(query_terms, axis=(0, 1))
    grad_key_gain = jnp.sum(key_terms, axis=(0, 1))
    d_qkv = jnp.concatenate(
        [
            d_q_pre.astype(jnp.bfloat16).reshape(rows_group, heads_here * HD),
            d_k_pre.astype(jnp.bfloat16).reshape(rows_group, groups_here * HD),
            d_value.reshape(rows_group, groups_here * HD),
        ],
        axis=1,
    )
    d_normed_partial = times_transposed(d_qkv, qkv_w)
    tokens_all_f = tokens_all.astype(jnp.float32)
    scale_all = lax.rsqrt(jnp.mean(tokens_all_f * tokens_all_f, axis=-1, keepdims=True) + EPS)
    attn_gain_part = jnp.sum(d_normed_partial * tokens_all_f * scale_all, axis=0)
    gain_parts = narrow_allreduce(
        jnp.concatenate([attn_gain_part, grad_mlp_gain, grad_query_gain, grad_key_gain])
    )
    d_full = d_local * wide_size
    hd_full = hd_local * wide_size

    def by_chunk(vec, size):
        return jnp.pad(vec.reshape(wide_size, size), ((0, 0), (0, d_local - size)))

    gain_block = jnp.stack(
        [
            by_chunk(gain_parts[:d_full], d_local),
            by_chunk(gain_parts[d_full : 2 * d_full], d_local),
            by_chunk(gain_parts[2 * d_full : 2 * d_full + hd_full], hd_local),
            by_chunk(gain_parts[2 * d_full + hd_full :], hd_local),
        ],
        axis=-1,
    ).reshape(d_full, 4)
    gain_block = jnp.pad(gain_block, ((0, 0), (0, 124)))
    qkv_grad = jnp.concatenate(
        [contract_rows(normed_all, d_qkv).astype(jnp.bfloat16), gain_block.astype(jnp.bfloat16)], axis=1
    )
    g_out_t, qkv_grad = lax.optimization_barrier((g_out_t, qkv_grad))
    g_qkv, g_gains = split_cols(
        lax.psum_scatter(qkv_grad, "wide", scatter_dimension=0, tiled=True).astype(jnp.float32),
        [q_cols + 2 * kv_cols, 128],
    )
    d_normed = narrow_scatter(d_normed_partial, relative)
    d_input_part, _ = rms_back(inputs, gain_attn, d_normed)
    d_tokens = d_resid + d_input_part
    attn_gain_grad = g_gains[:, 0]
    mlp_gain_grad = g_gains[:, 1]
    query_gain_grad = g_gains[:hd_local, 2]
    key_gain_grad = g_gains[:hd_local, 3]

    g_query = g_qkv[:, :q_cols]
    g_key = g_qkv[:, q_cols : q_cols + kv_cols]
    g_value = g_qkv[:, q_cols + kv_cols :]
    g_gate = jnp.concatenate([mlp_grads[h][0][:, :ff_half] for h in range(2)], axis=1)
    g_up = jnp.concatenate([mlp_grads[h][0][:, ff_half:] for h in range(2)], axis=1)
    g_down = jnp.concatenate([mlp_grads[h][1] for h in range(2)], axis=1).T
    output = (resid + narrow_scatter(down_partial, relative)).astype(jnp.bfloat16)
    return (
        output,
        d_tokens,
        attn_gain_grad,
        g_query,
        g_key,
        g_value,
        query_gain_grad,
        key_gain_grad,
        g_out_t.T,
        mlp_gain_grad,
        g_gate,
        g_up,
        g_down,
    )


def solution(mesh):
    in_specs = (
        P(("wide", "narrow"), None),
        P("wide", None),
        P(("wide", "narrow"), None),
        P("wide"),
        P("wide", "narrow"),
        P("wide", "narrow"),
        P("wide", "narrow"),
        P("wide"),
        P("wide"),
        P("narrow", "wide"),
        P("wide"),
        P("wide", "narrow"),
        P("wide", "narrow"),
        P("narrow", "wide"),
    )
    out_specs = (
        P(("wide", "narrow"), None),
        P(("wide", "narrow"), None),
        P("wide"),
        P("wide", "narrow"),
        P("wide", "narrow"),
        P("wide", "narrow"),
        P("wide"),
        P("wide"),
        P("narrow", "wide"),
        P("wide"),
        P("wide", "narrow"),
        P("wide", "narrow"),
        P("narrow", "wide"),
    )
    return jax.shard_map(shards_body, mesh=mesh, in_specs=in_specs, out_specs=out_specs, check_vma=False)
```

```python
import jax
import jax.numpy as jnp
from jax import lax
from jax.sharding import PartitionSpec as P


H = 16
KV = 8
HD = 128


EPS = 1e-06
ROPE_BASE = 1000000.0
NEG_FILL = -1e30

XPERM = [(0, 1), (1, 0), (2, 3), (3, 2)]
YPERM = [(0, 2), (2, 0), (1, 3), (3, 1)]
BLOCK_XOR = (0, 1, 2, 3, 0, 2, 1, 3)


def rms_apply(values, gain):
    return values * lax.rsqrt(jnp.mean(values * values, axis=-1, keepdims=True) + EPS) * gain


def rms_back(values, gain, grad):
    scale = lax.rsqrt(jnp.mean(values * values, axis=-1, keepdims=True) + EPS)
    weighted = grad * gain
    inner = jnp.mean(weighted * values, axis=-1, keepdims=True)
    d_values = scale * weighted - values * (scale * scale * scale) * inner
    return (d_values, grad * values * scale)


def rotate(values):
    half = values.shape[-1] // 2
    return jnp.concatenate([-values[..., half:], values[..., :half]], axis=-1)


def rotate_back(values):
    half = values.shape[-1] // 2
    return jnp.concatenate([values[..., half:], -values[..., :half]], axis=-1)


def doc_positions(doc_rows):
    index = lax.broadcasted_iota(jnp.int32, doc_rows.shape, 1)
    change = jnp.concatenate(
        [jnp.ones((doc_rows.shape[0], 1), jnp.bool_), doc_rows[:, 1:] != doc_rows[:, :-1]], axis=1
    )
    begin = lax.cummax(jnp.where(change, index, 0), axis=1)
    return index - begin


def rope_from_positions(position):
    freqs = ROPE_BASE ** (-(jnp.arange(HD // 2, dtype=jnp.float32) * (2.0 / HD)))
    angle = position.astype(jnp.float32)[..., None] * freqs
    cosine = jnp.cos(angle)
    sine = jnp.sin(angle)
    return (jnp.concatenate([cosine, cosine], axis=-1), jnp.concatenate([sine, sine], axis=-1))


def contract_rows(left, right):
    return lax.dot_general(
        left, right, (((0,), (0,)), ((), ())), preferred_element_type=jnp.float32
    )


def times_transposed(left, right):
    return lax.dot_general(
        left, right, (((1,), (1,)), ((), ())), preferred_element_type=jnp.float32
    )


def relative_ok(seq_count):
    return lax.axis_size("narrow") == 4 and seq_count == 1


def relative_rows(vec):
    n = lax.axis_index("narrow")
    half = vec.shape[0] // 8
    split = vec.reshape(4, 2, half)
    pieces = []
    for blk, flip in enumerate(BLOCK_XOR):
        source = split[:, 1 if blk >= 4 else 0]
        pieces.append(lax.dynamic_index_in_dim(source, jnp.bitwise_xor(n, flip), 0, keepdims=False))
    return jnp.concatenate(pieces)


def narrow_allreduce(v):
    if lax.axis_size("narrow") != 4:
        return lax.psum(v, "narrow")
    v = v + lax.ppermute(v, "narrow", XPERM)
    return v + lax.ppermute(v, "narrow", YPERM)


def narrow_gather(x, relative):
    if not relative:
        return lax.all_gather(x, "narrow", axis=0, tiled=True)
    half = x.shape[0] // 2
    a, b = x[:half], x[half:]
    a_x = lax.ppermute(a, "narrow", XPERM)
    b_y = lax.ppermute(b, "narrow", YPERM)
    a_pair = jnp.concatenate([a, a_x], axis=0)
    b_pair = jnp.concatenate([b, b_y], axis=0)
    a_pair_y = lax.ppermute(a_pair, "narrow", YPERM)
    b_pair_x = lax.ppermute(b_pair, "narrow", XPERM)
    return jnp.concatenate([a_pair, a_pair_y, b_pair, b_pair_x], axis=0)


def narrow_scatter(x, relative):
    if not relative:
        return lax.psum_scatter(
            x.astype(jnp.bfloat16), "narrow", scatter_dimension=0, tiled=True
        ).astype(jnp.float32)
    rows, c = x.shape
    half = rows // 8
    blocks = x.reshape(8, half, c)
    a_got = lax.ppermute(blocks[2:4].astype(jnp.bfloat16), "narrow", YPERM)
    b_got = lax.ppermute(blocks[6:8].astype(jnp.bfloat16), "narrow", XPERM)
    a_sum = blocks[0:2] + a_got.astype(jnp.float32)
    b_sum = blocks[4:6] + b_got.astype(jnp.float32)
    a_got2 = lax.ppermute(a_sum[1].astype(jnp.bfloat16), "narrow", XPERM)
    b_got2 = lax.ppermute(b_sum[1].astype(jnp.bfloat16), "narrow", YPERM)
    return jnp.concatenate(
        [a_sum[0] + a_got2.astype(jnp.float32), b_sum[0] + b_got2.astype(jnp.float32)], axis=0
    )


def split_cols(joined, widths):
    out = []
    start = 0
    for w in widths:
        out.append(joined[:, start : start + w])
        start += w
    return out


def wide_gather(blocks):
    joined = lax.all_gather(jnp.concatenate(blocks, axis=1), "wide", axis=0, tiled=True)
    return split_cols(joined, [blk.shape[1] for blk in blocks])


def shards_body(
    tokens,
    doc_ids,
    cotangent,
    attn_gain,
    w_query,
    w_key,
    w_value,
    query_gain,
    key_gain,
    w_out,
    mlp_gain,
    w_gate,
    w_up,
    w_down,
):
    narrow_size = lax.axis_size("narrow")
    wide_size = lax.axis_size("wide")
    heads_here = H // narrow_size
    groups_here = KV // narrow_size
    repeat = H // KV
    seq_count, length = doc_ids.shape
    rows_group = seq_count * length
    scale = HD ** (-0.5)
    d_local = attn_gain.shape[0]
    hd_local = query_gain.shape[0]
    q_cols = w_query.shape[1]
    kv_cols = w_key.shape[1]
    ff_cols = w_gate.shape[1]
    ff_half = ff_cols // 2
    relative = relative_ok(seq_count)

    tokens_all = narrow_gather(tokens, relative)
    grad_rows = narrow_gather(cotangent, relative)

    pad_hd = ((0, d_local - hd_local),)
    gain_block = jnp.pad(
        jnp.stack(
            [attn_gain, mlp_gain, jnp.pad(query_gain, pad_hd), jnp.pad(key_gain, pad_hd)], axis=1
        ),
        ((0, 0), (0, 124)),
    )
    qkv_w, out_wt, gains_all = wide_gather(
        [jnp.concatenate([w_query, w_key, w_value], axis=1), w_out.T, gain_block]
    )
    gain_attn = gains_all[:, 0].astype(jnp.float32)
    gain_mlp = gains_all[:, 1].astype(jnp.float32)
    gains_split = gains_all.reshape(wide_size, d_local, 128)
    gain_query = gains_split[:, :hd_local, 2].reshape(-1).astype(jnp.float32)
    gain_key = gains_split[:, :hd_local, 3].reshape(-1).astype(jnp.float32)
    down_t = w_down.T
    mlp_sets = []
    for h in range(2):
        cols = slice(h * ff_half, (h + 1) * ff_half)
        mlp_sets.append(wide_gather([w_gate[:, cols], w_up[:, cols], down_t[:, cols]]))

    if relative:
        order = relative_rows(jnp.arange(rows_group, dtype=jnp.int32))
        doc_row = relative_rows(doc_ids[0])
        position = relative_rows(doc_positions(doc_ids)[0])
    else:
        order = jnp.arange(rows_group, dtype=jnp.int32)
        doc_row = doc_ids.reshape(-1)
        position = doc_positions(doc_ids).reshape(-1)
    cosine, sine = rope_from_positions(position)
    cos_heads = cosine[:, None, :]
    sin_heads = sine[:, None, :]
    allowed = (order[None, :] <= order[:, None]) & (doc_row[None, :] == doc_row[:, None])
    if not relative:
        seq_of = jnp.arange(rows_group, dtype=jnp.int32) // length
        allowed = allowed & (seq_of[None, :] == seq_of[:, None])

    inputs = tokens.astype(jnp.float32)
    normed_all = rms_apply(tokens_all.astype(jnp.float32), gain_attn).astype(jnp.bfloat16)
    qkv = jnp.dot(normed_all, qkv_w, preferred_element_type=jnp.float32)
    q_pre = qkv[:, :q_cols].reshape(rows_group, heads_here, HD)
    k_pre = qkv[:, q_cols : q_cols + kv_cols].reshape(rows_group, groups_here, HD)
    v_use = qkv[:, q_cols + kv_cols :].astype(jnp.bfloat16).reshape(rows_group, groups_here, HD)
    q_norm = rms_apply(q_pre, gain_query)
    k_norm = rms_apply(k_pre, gain_key)
    q_use = (q_norm * cos_heads + rotate(q_norm) * sin_heads).astype(jnp.bfloat16)
    k_use = (k_norm * cos_heads + rotate(k_norm) * sin_heads).astype(jnp.bfloat16)
    q_grouped = q_use.reshape(rows_group, groups_here, repeat, HD)

    scores = jnp.einsum("qgrd,kgd->grqk", q_grouped, k_use, preferred_element_type=jnp.float32) * scale
    scores = jnp.where(allowed, scores, NEG_FILL)
    top = jnp.max(scores, axis=-1, keepdims=True)
    weights = jnp.exp(scores - top)
    total = jnp.sum(weights, axis=-1, keepdims=True)
    probs = weights / total
    mixed = jnp.einsum(
        "grqk,kgd->qgrd", probs.astype(jnp.bfloat16), v_use, preferred_element_type=jnp.float32
    )
    log_totals = (top + jnp.log(total))[..., 0]
    attended = mixed.astype(jnp.bfloat16).reshape(rows_group, heads_here * HD)

    resid = inputs + narrow_scatter(times_transposed(attended, out_wt), relative)
    mlp_in = rms_apply(resid, gain_mlp).astype(jnp.bfloat16)
    mlp_all = narrow_gather(mlp_in, relative)

    down_partial = None
    d_mlp_partial = None
    mlp_grads = []
    for h in range(2):
        gate_w, up_w, down_wt = mlp_sets[h]
        gate = jnp.dot(mlp_all, gate_w, preferred_element_type=jnp.float32)
        up = jnp.dot(mlp_all, up_w, preferred_element_type=jnp.float32)
        sigmoid = jax.nn.sigmoid(gate)
        hidden = (gate * sigmoid * up).astype(jnp.bfloat16)
        part = times_transposed(hidden, down_wt)
        down_partial = part if down_partial is None else down_partial + part
        d_hidden = jnp.dot(grad_rows, down_wt, preferred_element_type=jnp.float32)
        d_up = (d_hidden * gate * sigmoid).astype(jnp.bfloat16)
        d_gate = (d_hidden * up * sigmoid * (1.0 + gate * (1.0 - sigmoid))).astype(jnp.bfloat16)
        part = times_transposed(d_gate, gate_w) + times_transposed(d_up, up_w)
        d_mlp_partial = part if d_mlp_partial is None else d_mlp_partial + part
        g_down_t = contract_rows(grad_rows, hidden)
        g_gate_up = contract_rows(mlp_all, jnp.concatenate([d_gate, d_up], axis=1))
        joined = jnp.concatenate(
            [g_gate_up.astype(jnp.bfloat16), g_down_t.astype(jnp.bfloat16)], axis=1
        )
        if h == 0:
            joined, mlp_sets[1] = lax.optimization_barrier((joined, mlp_sets[1]))
            mlp_grads.append(lax.psum_scatter(joined, "wide", scatter_dimension=0, tiled=True))
        else:
            last_joined = joined

    d_mlp_in = narrow_scatter(d_mlp_partial, relative)
    d_part, mlp_gain_terms = rms_back(resid, gain_mlp, d_mlp_in)
    grad_mlp_gain = jnp.sum(mlp_gain_terms, axis=0)
    d_resid = cotangent.astype(jnp.float32) + d_part
    p_scores = (
        jnp.einsum("qgrd,kgd->grqk", q_grouped, k_use, preferred_element_type=jnp.float32) * scale
    )
    p_probs = jnp.where(allowed, jnp.exp(p_scores - log_totals[..., None]), 0.0)
    d_resid_low, last_joined = lax.optimization_barrier((d_resid.astype(jnp.bfloat16), last_joined))
    mlp_grads.append(lax.psum_scatter(last_joined, "wide", scatter_dimension=0, tiled=True))
    branch_rows = narrow_gather(d_resid_low, relative)
    out_grad = contract_rows(branch_rows, attended).astype(jnp.bfloat16)
    d_attended = jnp.dot(branch_rows, out_wt, preferred_element_type=jnp.float32).astype(jnp.bfloat16)
    d_mixed = d_attended.reshape(rows_group, groups_here, repeat, HD)

    d_probs = jnp.einsum("qgrd,kgd->grqk", d_mixed, v_use, preferred_element_type=jnp.float32)
    inner = jnp.sum(p_probs * d_probs, axis=-1, keepdims=True)
    d_scores = (p_probs * (d_probs - inner)).astype(jnp.bfloat16)
    d_query = jnp.einsum("grqk,kgd->qgrd", d_scores, k_use, preferred_element_type=jnp.float32) * scale
    d_key = jnp.einsum("grqk,qgrd->kgd", d_scores, q_grouped, preferred_element_type=jnp.float32) * scale
    d_value = jnp.einsum(
        "grqk,qgrd->kgd", p_probs.astype(jnp.bfloat16), d_mixed, preferred_element_type=jnp.float32
    ).astype(jnp.bfloat16)

    d_query = d_query.reshape(rows_group, heads_here, HD)
    d_q_norm = d_query * cos_heads + rotate_back(d_query * sin_heads)
    d_k_norm = d_key * cos_heads + rotate_back(d_key * sin_heads)
    d_q_pre, query_terms = rms_back(q_pre, gain_query, d_q_norm)
    d_k_pre, key_terms = rms_back(k_pre, gain_key, d_k_norm)
    grad_query_gain = jnp.sum(query_terms, axis=(0, 1))
    grad_key_gain = jnp.sum(key_terms, axis=(0, 1))
    d_qkv = jnp.concatenate(
        [
            d_q_pre.astype(jnp.bfloat16).reshape(rows_group, heads_here * HD),
            d_k_pre.astype(jnp.bfloat16).reshape(rows_group, groups_here * HD),
            d_value.reshape(rows_group, groups_here * HD),
        ],
        axis=1,
    )
    d_normed_partial = times_transposed(d_qkv, qkv_w)
    tokens_all_f = tokens_all.astype(jnp.float32)
    scale_all = lax.rsqrt(jnp.mean(tokens_all_f * tokens_all_f, axis=-1, keepdims=True) + EPS)
    attn_gain_part = jnp.sum(d_normed_partial * tokens_all_f * scale_all, axis=0)
    gain_parts = narrow_allreduce(
        jnp.concatenate([attn_gain_part, grad_mlp_gain, grad_query_gain, grad_key_gain])
    )
    d_full = d_local * wide_size
    hd_full = hd_local * wide_size

    def by_chunk(vec, size):
        return jnp.pad(vec.reshape(wide_size, size), ((0, 0), (0, d_local - size)))

    gain_block = jnp.stack(
        [
            by_chunk(gain_parts[:d_full], d_local),
            by_chunk(gain_parts[d_full : 2 * d_full], d_local),
            by_chunk(gain_parts[2 * d_full : 2 * d_full + hd_full], hd_local),
            by_chunk(gain_parts[2 * d_full + hd_full :], hd_local),
        ],
        axis=-1,
    ).reshape(d_full, 4)
    gain_block = jnp.pad(gain_block, ((0, 0), (0, 124)))
    qkv_grad = jnp.concatenate(
        [
            out_grad,
            contract_rows(normed_all, d_qkv).astype(jnp.bfloat16),
            gain_block.astype(jnp.bfloat16),
        ],
        axis=1,
    )
    mlp_grads, qkv_grad = lax.optimization_barrier((mlp_grads, qkv_grad))
    mlp_grads = [split_cols(g.astype(jnp.float32), [2 * ff_half, ff_half]) for g in mlp_grads]
    last_grads = lax.psum_scatter(qkv_grad, "wide", scatter_dimension=0, tiled=True)
    g_out_t, g_qkv, g_gains = split_cols(
        last_grads.astype(jnp.float32), [q_cols, q_cols + 2 * kv_cols, 128]
    )
    d_normed = narrow_scatter(d_normed_partial, relative)
    d_input_part, _ = rms_back(inputs, gain_attn, d_normed)
    d_tokens = d_resid + d_input_part
    attn_gain_grad = g_gains[:, 0]
    mlp_gain_grad = g_gains[:, 1]
    query_gain_grad = g_gains[:hd_local, 2]
    key_gain_grad = g_gains[:hd_local, 3]

    g_query = g_qkv[:, :q_cols]
    g_key = g_qkv[:, q_cols : q_cols + kv_cols]
    g_value = g_qkv[:, q_cols + kv_cols :]
    g_gate = jnp.concatenate([mlp_grads[h][0][:, :ff_half] for h in range(2)], axis=1)
    g_up = jnp.concatenate([mlp_grads[h][0][:, ff_half:] for h in range(2)], axis=1)
    g_down = jnp.concatenate([mlp_grads[h][1] for h in range(2)], axis=1).T
    output = (resid + narrow_scatter(down_partial, relative)).astype(jnp.bfloat16)
    return (
        output,
        d_tokens,
        attn_gain_grad,
        g_query,
        g_key,
        g_value,
        query_gain_grad,
        key_gain_grad,
        g_out_t.T,
        mlp_gain_grad,
        g_gate,
        g_up,
        g_down,
    )


def solution(mesh):
    in_specs = (
        P(("wide", "narrow"), None),
        P("wide", None),
        P(("wide", "narrow"), None),
        P("wide"),
        P("wide", "narrow"),
        P("wide", "narrow"),
        P("wide", "narrow"),
        P("wide"),
        P("wide"),
        P("narrow", "wide"),
        P("wide"),
        P("wide", "narrow"),
        P("wide", "narrow"),
        P("narrow", "wide"),
    )
    out_specs = (
        P(("wide", "narrow"), None),
        P(("wide", "narrow"), None),
        P("wide"),
        P("wide", "narrow"),
        P("wide", "narrow"),
        P("wide", "narrow"),
        P("wide"),
        P("wide"),
        P("narrow", "wide"),
        P("wide"),
        P("wide", "narrow"),
        P("wide", "narrow"),
        P("narrow", "wide"),
    )
    return jax.shard_map(shards_body, mesh=mesh, in_specs=in_specs, out_specs=out_specs, check_vma=False)
```

```python
import jax
import jax.numpy as jnp
from jax import lax
from jax.sharding import PartitionSpec as P


H = 16
KV = 8
HD = 128


EPS = 1e-06
ROPE_BASE = 1000000.0
NEG_FILL = -1e30

XPERM = [(0, 1), (1, 0), (2, 3), (3, 2)]
YPERM = [(0, 2), (2, 0), (1, 3), (3, 1)]
BLOCK_XOR = (0, 1, 2, 3, 0, 2, 1, 3)


def rms_apply(values, gain):
    return values * lax.rsqrt(jnp.mean(values * values, axis=-1, keepdims=True) + EPS) * gain


def rms_back(values, gain, grad):
    scale = lax.rsqrt(jnp.mean(values * values, axis=-1, keepdims=True) + EPS)
    weighted = grad * gain
    inner = jnp.mean(weighted * values, axis=-1, keepdims=True)
    d_values = scale * weighted - values * (scale * scale * scale) * inner
    return (d_values, grad * values * scale)


def rotate(values):
    half = values.shape[-1] // 2
    return jnp.concatenate([-values[..., half:], values[..., :half]], axis=-1)


def rotate_back(values):
    half = values.shape[-1] // 2
    return jnp.concatenate([values[..., half:], -values[..., :half]], axis=-1)


def doc_positions(doc_rows):
    index = lax.broadcasted_iota(jnp.int32, doc_rows.shape, 1)
    change = jnp.concatenate(
        [jnp.ones((doc_rows.shape[0], 1), jnp.bool_), doc_rows[:, 1:] != doc_rows[:, :-1]], axis=1
    )
    begin = lax.cummax(jnp.where(change, index, 0), axis=1)
    return index - begin


def rope_from_positions(position):
    freqs = ROPE_BASE ** (-(jnp.arange(HD // 2, dtype=jnp.float32) * (2.0 / HD)))
    angle = position.astype(jnp.float32)[..., None] * freqs
    cosine = jnp.cos(angle)
    sine = jnp.sin(angle)
    return (jnp.concatenate([cosine, cosine], axis=-1), jnp.concatenate([sine, sine], axis=-1))


def contract_rows(left, right):
    return lax.dot_general(
        left, right, (((0,), (0,)), ((), ())), preferred_element_type=jnp.float32
    )


def times_transposed(left, right):
    return lax.dot_general(
        left, right, (((1,), (1,)), ((), ())), preferred_element_type=jnp.float32
    )


def relative_ok(seq_count):
    return lax.axis_size("narrow") == 4 and seq_count == 1


def relative_rows(vec):
    n = lax.axis_index("narrow")
    half = vec.shape[0] // 8
    split = vec.reshape(4, 2, half)
    pieces = []
    for blk, flip in enumerate(BLOCK_XOR):
        source = split[:, 1 if blk >= 4 else 0]
        pieces.append(lax.dynamic_index_in_dim(source, jnp.bitwise_xor(n, flip), 0, keepdims=False))
    return jnp.concatenate(pieces)


def narrow_allreduce(v):
    if lax.axis_size("narrow") != 4:
        return lax.psum(v, "narrow")
    v = v + lax.ppermute(v, "narrow", XPERM)
    return v + lax.ppermute(v, "narrow", YPERM)


def narrow_gather(x, relative):
    if not relative:
        return lax.all_gather(x, "narrow", axis=0, tiled=True)
    half = x.shape[0] // 2
    a, b = x[:half], x[half:]
    a_x = lax.ppermute(a, "narrow", XPERM)
    b_y = lax.ppermute(b, "narrow", YPERM)
    a_pair = jnp.concatenate([a, a_x], axis=0)
    b_pair = jnp.concatenate([b, b_y], axis=0)
    a_pair_y = lax.ppermute(a_pair, "narrow", YPERM)
    b_pair_x = lax.ppermute(b_pair, "narrow", XPERM)
    return jnp.concatenate([a_pair, a_pair_y, b_pair, b_pair_x], axis=0)


def narrow_scatter(x, relative):
    if not relative:
        return lax.psum_scatter(
            x.astype(jnp.bfloat16), "narrow", scatter_dimension=0, tiled=True
        ).astype(jnp.float32)
    rows, c = x.shape
    half = rows // 8
    blocks = x.reshape(8, half, c)
    a_got = lax.ppermute(blocks[2:4].astype(jnp.bfloat16), "narrow", YPERM)
    b_got = lax.ppermute(blocks[6:8].astype(jnp.bfloat16), "narrow", XPERM)
    a_sum = blocks[0:2] + a_got.astype(jnp.float32)
    b_sum = blocks[4:6] + b_got.astype(jnp.float32)
    a_got2 = lax.ppermute(a_sum[1].astype(jnp.bfloat16), "narrow", XPERM)
    b_got2 = lax.ppermute(b_sum[1].astype(jnp.bfloat16), "narrow", YPERM)
    return jnp.concatenate(
        [a_sum[0] + a_got2.astype(jnp.float32), b_sum[0] + b_got2.astype(jnp.float32)], axis=0
    )


def split_cols(joined, widths):
    out = []
    start = 0
    for w in widths:
        out.append(joined[:, start : start + w])
        start += w
    return out


def wide_gather(blocks):
    joined = lax.all_gather(jnp.concatenate(blocks, axis=1), "wide", axis=0, tiled=True)
    return split_cols(joined, [blk.shape[1] for blk in blocks])


def shards_body(
    tokens,
    doc_ids,
    cotangent,
    attn_gain,
    w_query,
    w_key,
    w_value,
    query_gain,
    key_gain,
    w_out,
    mlp_gain,
    w_gate,
    w_up,
    w_down,
):
    narrow_size = lax.axis_size("narrow")
    wide_size = lax.axis_size("wide")
    heads_here = H // narrow_size
    groups_here = KV // narrow_size
    repeat = H // KV
    seq_count, length = doc_ids.shape
    rows_group = seq_count * length
    scale = HD ** (-0.5)
    d_local = attn_gain.shape[0]
    hd_local = query_gain.shape[0]
    q_cols = w_query.shape[1]
    kv_cols = w_key.shape[1]
    ff_cols = w_gate.shape[1]
    ff_half = ff_cols // 2
    relative = relative_ok(seq_count)

    tokens_all = narrow_gather(tokens, relative)
    grad_rows = narrow_gather(cotangent, relative)

    pad_hd = ((0, d_local - hd_local),)
    gain_block = jnp.pad(
        jnp.stack(
            [attn_gain, mlp_gain, jnp.pad(query_gain, pad_hd), jnp.pad(key_gain, pad_hd)], axis=1
        ),
        ((0, 0), (0, 124)),
    )
    qkv_w, out_wt, gains_all = wide_gather(
        [jnp.concatenate([w_query, w_key, w_value], axis=1), w_out.T, gain_block]
    )
    gain_attn = gains_all[:, 0].astype(jnp.float32)
    gain_mlp = gains_all[:, 1].astype(jnp.float32)
    gains_split = gains_all.reshape(wide_size, d_local, 128)
    gain_query = gains_split[:, :hd_local, 2].reshape(-1).astype(jnp.float32)
    gain_key = gains_split[:, :hd_local, 3].reshape(-1).astype(jnp.float32)
    down_t = w_down.T
    mlp_sets = []
    for h in range(2):
        cols = slice(h * ff_half, (h + 1) * ff_half)
        mlp_sets.append(
            wide_gather([jnp.concatenate([w_gate[:, cols], w_up[:, cols]], axis=1), down_t[:, cols]])
        )

    if relative:
        order = relative_rows(jnp.arange(rows_group, dtype=jnp.int32))
        doc_row = relative_rows(doc_ids[0])
        position = relative_rows(doc_positions(doc_ids)[0])
    else:
        order = jnp.arange(rows_group, dtype=jnp.int32)
        doc_row = doc_ids.reshape(-1)
        position = doc_positions(doc_ids).reshape(-1)
    cosine, sine = rope_from_positions(position)
    cos_heads = cosine[:, None, :]
    sin_heads = sine[:, None, :]
    allowed = (order[None, :] <= order[:, None]) & (doc_row[None, :] == doc_row[:, None])
    if not relative:
        seq_of = jnp.arange(rows_group, dtype=jnp.int32) // length
        allowed = allowed & (seq_of[None, :] == seq_of[:, None])

    inputs = tokens.astype(jnp.float32)
    normed_all = rms_apply(tokens_all.astype(jnp.float32), gain_attn).astype(jnp.bfloat16)
    qkv = jnp.dot(normed_all, qkv_w, preferred_element_type=jnp.float32)
    q_pre = qkv[:, :q_cols].reshape(rows_group, heads_here, HD)
    k_pre = qkv[:, q_cols : q_cols + kv_cols].reshape(rows_group, groups_here, HD)
    v_use = qkv[:, q_cols + kv_cols :].astype(jnp.bfloat16).reshape(rows_group, groups_here, HD)
    q_norm = rms_apply(q_pre, gain_query)
    k_norm = rms_apply(k_pre, gain_key)
    q_use = (q_norm * cos_heads + rotate(q_norm) * sin_heads).astype(jnp.bfloat16)
    k_use = (k_norm * cos_heads + rotate(k_norm) * sin_heads).astype(jnp.bfloat16)
    q_grouped = q_use.reshape(rows_group, groups_here, repeat, HD)

    scores = jnp.einsum("qgrd,kgd->grqk", q_grouped, k_use, preferred_element_type=jnp.float32) * scale
    scores = jnp.where(allowed, scores, NEG_FILL)
    top = jnp.max(scores, axis=-1, keepdims=True)
    weights = jnp.exp(scores - top)
    total = jnp.sum(weights, axis=-1, keepdims=True)
    probs = weights / total
    mixed = jnp.einsum(
        "grqk,kgd->qgrd", probs.astype(jnp.bfloat16), v_use, preferred_element_type=jnp.float32
    )
    log_totals = (top + jnp.log(total))[..., 0]
    attended = mixed.astype(jnp.bfloat16).reshape(rows_group, heads_here * HD)

    resid = inputs + narrow_scatter(times_transposed(attended, out_wt), relative)
    mlp_in = rms_apply(resid, gain_mlp).astype(jnp.bfloat16)
    mlp_all = narrow_gather(mlp_in, relative)

    down_partial = None
    d_mlp_partial = None
    mlp_grads = []
    for h in range(2):
        gate_up_w, down_wt = mlp_sets[h]
        gate_up = jnp.dot(mlp_all, gate_up_w, preferred_element_type=jnp.float32)
        gate = gate_up[:, :ff_half]
        up = gate_up[:, ff_half:]
        sigmoid = jax.nn.sigmoid(gate)
        hidden = (gate * sigmoid * up).astype(jnp.bfloat16)
        part = times_transposed(hidden, down_wt)
        down_partial = part if down_partial is None else down_partial + part
        d_hidden = jnp.dot(grad_rows, down_wt, preferred_element_type=jnp.float32)
        d_up = (d_hidden * gate * sigmoid).astype(jnp.bfloat16)
        d_gate = (d_hidden * up * sigmoid * (1.0 + gate * (1.0 - sigmoid))).astype(jnp.bfloat16)
        d_gate_up = jnp.concatenate([d_gate, d_up], axis=1)
        part = times_transposed(d_gate_up, gate_up_w)
        d_mlp_partial = part if d_mlp_partial is None else d_mlp_partial + part
        g_down_t = contract_rows(grad_rows, hidden)
        g_gate_up = contract_rows(mlp_all, d_gate_up)
        joined = jnp.concatenate(
            [g_gate_up.astype(jnp.bfloat16), g_down_t.astype(jnp.bfloat16)], axis=1
        )
        if h == 0:
            joined, mlp_sets[1] = lax.optimization_barrier((joined, mlp_sets[1]))
            mlp_grads.append(lax.psum_scatter(joined, "wide", scatter_dimension=0, tiled=True))
        else:
            last_joined = joined

    d_mlp_in = narrow_scatter(d_mlp_partial, relative)
    d_part, mlp_gain_terms = rms_back(resid, gain_mlp, d_mlp_in)
    grad_mlp_gain = jnp.sum(mlp_gain_terms, axis=0)
    d_resid = cotangent.astype(jnp.float32) + d_part
    p_scores = (
        jnp.einsum("qgrd,kgd->grqk", q_grouped, k_use, preferred_element_type=jnp.float32) * scale
    )
    p_probs = jnp.where(allowed, jnp.exp(p_scores - log_totals[..., None]), 0.0)
    d_resid_low, last_joined = lax.optimization_barrier((d_resid.astype(jnp.bfloat16), last_joined))
    mlp_grads.append(lax.psum_scatter(last_joined, "wide", scatter_dimension=0, tiled=True))
    branch_rows = narrow_gather(d_resid_low, relative)
    out_grad = contract_rows(branch_rows, attended).astype(jnp.bfloat16)
    mlp_grads, out_grad = lax.optimization_barrier((mlp_grads, out_grad))
    mlp_grads = [split_cols(g.astype(jnp.float32), [2 * ff_half, ff_half]) for g in mlp_grads]
    g_out_t = lax.psum_scatter(out_grad, "wide", scatter_dimension=0, tiled=True).astype(jnp.float32)
    d_attended = jnp.dot(branch_rows, out_wt, preferred_element_type=jnp.float32).astype(jnp.bfloat16)
    d_mixed = d_attended.reshape(rows_group, groups_here, repeat, HD)

    d_probs = jnp.einsum("qgrd,kgd->grqk", d_mixed, v_use, preferred_element_type=jnp.float32)
    inner = jnp.sum(p_probs * d_probs, axis=-1, keepdims=True)
    d_scores = (p_probs * (d_probs - inner)).astype(jnp.bfloat16)
    d_query = jnp.einsum("grqk,kgd->qgrd", d_scores, k_use, preferred_element_type=jnp.float32) * scale
    d_key = jnp.einsum("grqk,qgrd->kgd", d_scores, q_grouped, preferred_element_type=jnp.float32) * scale
    d_value = jnp.einsum(
        "grqk,qgrd->kgd", p_probs.astype(jnp.bfloat16), d_mixed, preferred_element_type=jnp.float32
    ).astype(jnp.bfloat16)

    d_query = d_query.reshape(rows_group, heads_here, HD)
    d_q_norm = d_query * cos_heads + rotate_back(d_query * sin_heads)
    d_k_norm = d_key * cos_heads + rotate_back(d_key * sin_heads)
    d_q_pre, query_terms = rms_back(q_pre, gain_query, d_q_norm)
    d_k_pre, key_terms = rms_back(k_pre, gain_key, d_k_norm)
    grad_query_gain = jnp.sum(query_terms, axis=(0, 1))
    grad_key_gain = jnp.sum(key_terms, axis=(0, 1))
    d_qkv = jnp.concatenate(
        [
            d_q_pre.astype(jnp.bfloat16).reshape(rows_group, heads_here * HD),
            d_k_pre.astype(jnp.bfloat16).reshape(rows_group, groups_here * HD),
            d_value.reshape(rows_group, groups_here * HD),
        ],
        axis=1,
    )
    d_normed_partial = times_transposed(d_qkv, qkv_w)
    tokens_all_f = tokens_all.astype(jnp.float32)
    scale_all = lax.rsqrt(jnp.mean(tokens_all_f * tokens_all_f, axis=-1, keepdims=True) + EPS)
    attn_gain_part = jnp.sum(d_normed_partial * tokens_all_f * scale_all, axis=0)
    gain_parts = narrow_allreduce(
        jnp.concatenate([attn_gain_part, grad_mlp_gain, grad_query_gain, grad_key_gain])
    )
    d_full = d_local * wide_size
    hd_full = hd_local * wide_size

    def by_chunk(vec, size):
        return jnp.pad(vec.reshape(wide_size, size), ((0, 0), (0, d_local - size)))

    gain_block = jnp.stack(
        [
            by_chunk(gain_parts[:d_full], d_local),
            by_chunk(gain_parts[d_full : 2 * d_full], d_local),
            by_chunk(gain_parts[2 * d_full : 2 * d_full + hd_full], hd_local),
            by_chunk(gain_parts[2 * d_full + hd_full :], hd_local),
        ],
        axis=-1,
    ).reshape(d_full, 4)
    gain_block = jnp.pad(gain_block, ((0, 0), (0, 124)))
    qkv_grad = jnp.concatenate(
        [contract_rows(normed_all, d_qkv).astype(jnp.bfloat16), gain_block.astype(jnp.bfloat16)], axis=1
    )
    g_out_t, qkv_grad = lax.optimization_barrier((g_out_t, qkv_grad))
    g_qkv, g_gains = split_cols(
        lax.psum_scatter(qkv_grad, "wide", scatter_dimension=0, tiled=True).astype(jnp.float32),
        [q_cols + 2 * kv_cols, 128],
    )
    d_normed = narrow_scatter(d_normed_partial, relative)
    d_input_part, _ = rms_back(inputs, gain_attn, d_normed)
    d_tokens = d_resid + d_input_part
    attn_gain_grad = g_gains[:, 0]
    mlp_gain_grad = g_gains[:, 1]
    query_gain_grad = g_gains[:hd_local, 2]
    key_gain_grad = g_gains[:hd_local, 3]

    g_query = g_qkv[:, :q_cols]
    g_key = g_qkv[:, q_cols : q_cols + kv_cols]
    g_value = g_qkv[:, q_cols + kv_cols :]
    g_gate = jnp.concatenate([mlp_grads[h][0][:, :ff_half] for h in range(2)], axis=1)
    g_up = jnp.concatenate([mlp_grads[h][0][:, ff_half:] for h in range(2)], axis=1)
    g_down = jnp.concatenate([mlp_grads[h][1] for h in range(2)], axis=1).T
    output = (resid + narrow_scatter(down_partial, relative)).astype(jnp.bfloat16)
    return (
        output,
        d_tokens,
        attn_gain_grad,
        g_query,
        g_key,
        g_value,
        query_gain_grad,
        key_gain_grad,
        g_out_t.T,
        mlp_gain_grad,
        g_gate,
        g_up,
        g_down,
    )


def solution(mesh):
    in_specs = (
        P(("wide", "narrow"), None),
        P("wide", None),
        P(("wide", "narrow"), None),
        P("wide"),
        P("wide", "narrow"),
        P("wide", "narrow"),
        P("wide", "narrow"),
        P("wide"),
        P("wide"),
        P("narrow", "wide"),
        P("wide"),
        P("wide", "narrow"),
        P("wide", "narrow"),
        P("narrow", "wide"),
    )
    out_specs = (
        P(("wide", "narrow"), None),
        P(("wide", "narrow"), None),
        P("wide"),
        P("wide", "narrow"),
        P("wide", "narrow"),
        P("wide", "narrow"),
        P("wide"),
        P("wide"),
        P("narrow", "wide"),
        P("wide"),
        P("wide", "narrow"),
        P("wide", "narrow"),
        P("narrow", "wide"),
    )
    return jax.shard_map(shards_body, mesh=mesh, in_specs=in_specs, out_specs=out_specs, check_vma=False)
```

```python
import jax
import jax.numpy as jnp
from jax import lax
from jax.sharding import PartitionSpec as P


H = 16
KV = 8
HD = 128


EPS = 1e-06
ROPE_BASE = 1000000.0
NEG_FILL = -1e30

XPERM = [(0, 1), (1, 0), (2, 3), (3, 2)]
YPERM = [(0, 2), (2, 0), (1, 3), (3, 1)]
BLOCK_XOR = (0, 1, 2, 3, 0, 2, 1, 3)


def rms_apply(values, gain):
    return values * lax.rsqrt(jnp.mean(values * values, axis=-1, keepdims=True) + EPS) * gain


def rms_back(values, gain, grad):
    scale = lax.rsqrt(jnp.mean(values * values, axis=-1, keepdims=True) + EPS)
    weighted = grad * gain
    inner = jnp.mean(weighted * values, axis=-1, keepdims=True)
    d_values = scale * weighted - values * (scale * scale * scale) * inner
    return (d_values, grad * values * scale)


def rotate(values):
    half = values.shape[-1] // 2
    return jnp.concatenate([-values[..., half:], values[..., :half]], axis=-1)


def rotate_back(values):
    half = values.shape[-1] // 2
    return jnp.concatenate([values[..., half:], -values[..., :half]], axis=-1)


def doc_positions(doc_rows):
    index = lax.broadcasted_iota(jnp.int32, doc_rows.shape, 1)
    change = jnp.concatenate(
        [jnp.ones((doc_rows.shape[0], 1), jnp.bool_), doc_rows[:, 1:] != doc_rows[:, :-1]], axis=1
    )
    begin = lax.cummax(jnp.where(change, index, 0), axis=1)
    return index - begin


def rope_from_positions(position):
    freqs = ROPE_BASE ** (-(jnp.arange(HD // 2, dtype=jnp.float32) * (2.0 / HD)))
    angle = position.astype(jnp.float32)[..., None] * freqs
    cosine = jnp.cos(angle)
    sine = jnp.sin(angle)
    return (jnp.concatenate([cosine, cosine], axis=-1), jnp.concatenate([sine, sine], axis=-1))


def contract_rows(left, right):
    return lax.dot_general(
        left, right, (((0,), (0,)), ((), ())), preferred_element_type=jnp.float32
    )


def times_transposed(left, right):
    return lax.dot_general(
        left, right, (((1,), (1,)), ((), ())), preferred_element_type=jnp.float32
    )


def relative_ok(seq_count):
    return lax.axis_size("narrow") == 4 and seq_count == 1


def relative_rows(vec):
    n = lax.axis_index("narrow")
    half = vec.shape[0] // 8
    split = vec.reshape(4, 2, half)
    pieces = []
    for blk, flip in enumerate(BLOCK_XOR):
        source = split[:, 1 if blk >= 4 else 0]
        pieces.append(lax.dynamic_index_in_dim(source, jnp.bitwise_xor(n, flip), 0, keepdims=False))
    return jnp.concatenate(pieces)


def narrow_allreduce(v):
    if lax.axis_size("narrow") != 4:
        return lax.psum(v, "narrow")
    v = v + lax.ppermute(v, "narrow", XPERM)
    return v + lax.ppermute(v, "narrow", YPERM)


def narrow_gather(x, relative):
    if not relative:
        return lax.all_gather(x, "narrow", axis=0, tiled=True)
    half = x.shape[0] // 2
    a, b = x[:half], x[half:]
    a_x = lax.ppermute(a, "narrow", XPERM)
    b_y = lax.ppermute(b, "narrow", YPERM)
    a_pair = jnp.concatenate([a, a_x], axis=0)
    b_pair = jnp.concatenate([b, b_y], axis=0)
    a_pair_y = lax.ppermute(a_pair, "narrow", YPERM)
    b_pair_x = lax.ppermute(b_pair, "narrow", XPERM)
    return jnp.concatenate([a_pair, a_pair_y, b_pair, b_pair_x], axis=0)


def narrow_scatter(x, relative):
    if not relative:
        return lax.psum_scatter(
            x.astype(jnp.bfloat16), "narrow", scatter_dimension=0, tiled=True
        ).astype(jnp.float32)
    rows, c = x.shape
    half = rows // 8
    blocks = x.reshape(8, half, c)
    a_got = lax.ppermute(blocks[2:4].astype(jnp.bfloat16), "narrow", YPERM)
    b_got = lax.ppermute(blocks[6:8].astype(jnp.bfloat16), "narrow", XPERM)
    a_sum = blocks[0:2] + a_got.astype(jnp.float32)
    b_sum = blocks[4:6] + b_got.astype(jnp.float32)
    a_got2 = lax.ppermute(a_sum[1].astype(jnp.bfloat16), "narrow", XPERM)
    b_got2 = lax.ppermute(b_sum[1].astype(jnp.bfloat16), "narrow", YPERM)
    return jnp.concatenate(
        [a_sum[0] + a_got2.astype(jnp.float32), b_sum[0] + b_got2.astype(jnp.float32)], axis=0
    )


def split_cols(joined, widths):
    out = []
    start = 0
    for w in widths:
        out.append(joined[:, start : start + w])
        start += w
    return out


def wide_gather(blocks):
    joined = lax.all_gather(jnp.concatenate(blocks, axis=1), "wide", axis=0, tiled=True)
    return split_cols(joined, [blk.shape[1] for blk in blocks])


def shards_body(
    tokens,
    doc_ids,
    cotangent,
    attn_gain,
    w_query,
    w_key,
    w_value,
    query_gain,
    key_gain,
    w_out,
    mlp_gain,
    w_gate,
    w_up,
    w_down,
):
    narrow_size = lax.axis_size("narrow")
    wide_size = lax.axis_size("wide")
    heads_here = H // narrow_size
    groups_here = KV // narrow_size
    repeat = H // KV
    seq_count, length = doc_ids.shape
    rows_group = seq_count * length
    scale = HD ** (-0.5)
    d_local = attn_gain.shape[0]
    hd_local = query_gain.shape[0]
    q_cols = w_query.shape[1]
    kv_cols = w_key.shape[1]
    ff_cols = w_gate.shape[1]
    ff_half = ff_cols // 2
    relative = relative_ok(seq_count)

    tokens_all = narrow_gather(tokens, relative)
    grad_rows = narrow_gather(cotangent, relative)

    pad_hd = ((0, d_local - hd_local),)
    gain_block = jnp.pad(
        jnp.stack(
            [attn_gain, mlp_gain, jnp.pad(query_gain, pad_hd), jnp.pad(key_gain, pad_hd)], axis=1
        ),
        ((0, 0), (0, 124)),
    )
    qkv_w, out_wt, gains_all = wide_gather(
        [jnp.concatenate([w_query, w_key, w_value], axis=1), w_out.T, gain_block]
    )
    gain_attn = gains_all[:, 0].astype(jnp.float32)
    gain_mlp = gains_all[:, 1].astype(jnp.float32)
    gains_split = gains_all.reshape(wide_size, d_local, 128)
    gain_query = gains_split[:, :hd_local, 2].reshape(-1).astype(jnp.float32)
    gain_key = gains_split[:, :hd_local, 3].reshape(-1).astype(jnp.float32)
    down_t = w_down.T
    mlp_sets = []
    for h in range(2):
        cols = slice(h * ff_half, (h + 1) * ff_half)
        mlp_sets.append(
            wide_gather([jnp.concatenate([w_gate[:, cols], w_up[:, cols]], axis=1), down_t[:, cols]])
        )

    if relative:
        order = relative_rows(jnp.arange(rows_group, dtype=jnp.int32))
        doc_row = relative_rows(doc_ids[0])
        position = relative_rows(doc_positions(doc_ids)[0])
    else:
        order = jnp.arange(rows_group, dtype=jnp.int32)
        doc_row = doc_ids.reshape(-1)
        position = doc_positions(doc_ids).reshape(-1)
    cosine, sine = rope_from_positions(position)
    cos_heads = cosine[:, None, :]
    sin_heads = sine[:, None, :]
    allowed = (order[None, :] <= order[:, None]) & (doc_row[None, :] == doc_row[:, None])
    if not relative:
        seq_of = jnp.arange(rows_group, dtype=jnp.int32) // length
        allowed = allowed & (seq_of[None, :] == seq_of[:, None])

    inputs = tokens.astype(jnp.float32)
    normed_all = rms_apply(tokens_all.astype(jnp.float32), gain_attn).astype(jnp.bfloat16)
    qkv = jnp.dot(normed_all, qkv_w, preferred_element_type=jnp.float32)
    q_pre = qkv[:, :q_cols].reshape(rows_group, heads_here, HD)
    k_pre = qkv[:, q_cols : q_cols + kv_cols].reshape(rows_group, groups_here, HD)
    v_use = qkv[:, q_cols + kv_cols :].astype(jnp.bfloat16).reshape(rows_group, groups_here, HD)
    q_norm = rms_apply(q_pre, gain_query)
    k_norm = rms_apply(k_pre, gain_key)
    q_use = (q_norm * cos_heads + rotate(q_norm) * sin_heads).astype(jnp.bfloat16)
    k_use = (k_norm * cos_heads + rotate(k_norm) * sin_heads).astype(jnp.bfloat16)
    q_grouped = q_use.reshape(rows_group, groups_here, repeat, HD)

    scores = jnp.einsum("qgrd,kgd->grqk", q_grouped, k_use, preferred_element_type=jnp.float32) * scale
    scores = jnp.where(allowed, scores, NEG_FILL)
    top = jnp.max(scores, axis=-1, keepdims=True)
    weights = jnp.exp(scores - top)
    total = jnp.sum(weights, axis=-1, keepdims=True)
    probs = weights / total
    mixed = jnp.einsum(
        "grqk,kgd->qgrd", probs.astype(jnp.bfloat16), v_use, preferred_element_type=jnp.float32
    )
    log_totals = (top + jnp.log(total))[..., 0]
    attended = mixed.astype(jnp.bfloat16).reshape(rows_group, heads_here * HD)

    resid = inputs + narrow_scatter(times_transposed(attended, out_wt), relative)
    mlp_in = rms_apply(resid, gain_mlp).astype(jnp.bfloat16)
    mlp_all = narrow_gather(mlp_in, relative)

    down_partial = None
    d_mlp_partial = None
    mlp_grads = []
    for h in range(2):
        gate_up_w, down_wt = mlp_sets[h]
        gate_up = jnp.dot(mlp_all, gate_up_w, preferred_element_type=jnp.float32)
        gate = gate_up[:, :ff_half]
        up = gate_up[:, ff_half:]
        sigmoid = jax.nn.sigmoid(gate)
        hidden = (gate * sigmoid * up).astype(jnp.bfloat16)
        d_hidden = jnp.dot(grad_rows, down_wt, preferred_element_type=jnp.float32)
        d_up = (d_hidden * gate * sigmoid).astype(jnp.bfloat16)
        d_gate = (d_hidden * up * sigmoid * (1.0 + gate * (1.0 - sigmoid))).astype(jnp.bfloat16)
        d_gate_up = jnp.concatenate([d_gate, d_up], axis=1)
        if h == 1:
            d_mlp_partial = d_mlp_partial + times_transposed(d_gate_up, gate_up_w)
            down_partial = down_partial + times_transposed(hidden, down_wt)
        g_down_t = contract_rows(grad_rows, hidden)
        g_gate_up = contract_rows(mlp_all, d_gate_up)
        joined = jnp.concatenate(
            [g_gate_up.astype(jnp.bfloat16), g_down_t.astype(jnp.bfloat16)], axis=1
        )
        if h == 0:
            joined, mlp_sets[1], hidden, d_gate_up = lax.optimization_barrier(
                (joined, mlp_sets[1], hidden, d_gate_up)
            )
            mlp_grads.append(lax.psum_scatter(joined, "wide", scatter_dimension=0, tiled=True))
            d_mlp_partial = times_transposed(d_gate_up, gate_up_w)
            down_partial = times_transposed(hidden, down_wt)
        else:
            last_joined = joined

    d_mlp_in = narrow_scatter(d_mlp_partial, relative)
    d_part, mlp_gain_terms = rms_back(resid, gain_mlp, d_mlp_in)
    grad_mlp_gain = jnp.sum(mlp_gain_terms, axis=0)
    d_resid = cotangent.astype(jnp.float32) + d_part
    p_scores = (
        jnp.einsum("qgrd,kgd->grqk", q_grouped, k_use, preferred_element_type=jnp.float32) * scale
    )
    p_probs = jnp.where(allowed, jnp.exp(p_scores - log_totals[..., None]), 0.0)
    d_resid_low, last_joined = lax.optimization_barrier((d_resid.astype(jnp.bfloat16), last_joined))
    branch_rows = narrow_gather(d_resid_low, relative)
    out_grad = contract_rows(branch_rows, attended).astype(jnp.bfloat16)
    mlp_grads.append(
        lax.psum_scatter(
            jnp.concatenate([last_joined, out_grad], axis=1), "wide", scatter_dimension=0, tiled=True
        )
    )
    d_attended = jnp.dot(branch_rows, out_wt, preferred_element_type=jnp.float32).astype(jnp.bfloat16)
    d_mixed = d_attended.reshape(rows_group, groups_here, repeat, HD)

    d_probs = jnp.einsum("qgrd,kgd->grqk", d_mixed, v_use, preferred_element_type=jnp.float32)
    inner = jnp.sum(p_probs * d_probs, axis=-1, keepdims=True)
    d_scores = (p_probs * (d_probs - inner)).astype(jnp.bfloat16)
    d_query = jnp.einsum("grqk,kgd->qgrd", d_scores, k_use, preferred_element_type=jnp.float32) * scale
    d_key = jnp.einsum("grqk,qgrd->kgd", d_scores, q_grouped, preferred_element_type=jnp.float32) * scale
    d_value = jnp.einsum(
        "grqk,qgrd->kgd", p_probs.astype(jnp.bfloat16), d_mixed, preferred_element_type=jnp.float32
    ).astype(jnp.bfloat16)

    d_query = d_query.reshape(rows_group, heads_here, HD)
    d_q_norm = d_query * cos_heads + rotate_back(d_query * sin_heads)
    d_k_norm = d_key * cos_heads + rotate_back(d_key * sin_heads)
    d_q_pre, query_terms = rms_back(q_pre, gain_query, d_q_norm)
    d_k_pre, key_terms = rms_back(k_pre, gain_key, d_k_norm)
    grad_query_gain = jnp.sum(query_terms, axis=(0, 1))
    grad_key_gain = jnp.sum(key_terms, axis=(0, 1))
    d_qkv = jnp.concatenate(
        [
            d_q_pre.astype(jnp.bfloat16).reshape(rows_group, heads_here * HD),
            d_k_pre.astype(jnp.bfloat16).reshape(rows_group, groups_here * HD),
            d_value.reshape(rows_group, groups_here * HD),
        ],
        axis=1,
    )
    d_normed_partial = times_transposed(d_qkv, qkv_w)
    tokens_all_f = tokens_all.astype(jnp.float32)
    scale_all = lax.rsqrt(jnp.mean(tokens_all_f * tokens_all_f, axis=-1, keepdims=True) + EPS)
    attn_gain_part = jnp.sum(d_normed_partial * tokens_all_f * scale_all, axis=0)
    gain_parts = narrow_allreduce(
        jnp.concatenate([attn_gain_part, grad_mlp_gain, grad_query_gain, grad_key_gain])
    )
    d_full = d_local * wide_size
    hd_full = hd_local * wide_size

    def by_chunk(vec, size):
        return jnp.pad(vec.reshape(wide_size, size), ((0, 0), (0, d_local - size)))

    gain_block = jnp.stack(
        [
            by_chunk(gain_parts[:d_full], d_local),
            by_chunk(gain_parts[d_full : 2 * d_full], d_local),
            by_chunk(gain_parts[2 * d_full : 2 * d_full + hd_full], hd_local),
            by_chunk(gain_parts[2 * d_full + hd_full :], hd_local),
        ],
        axis=-1,
    ).reshape(d_full, 4)
    gain_block = jnp.pad(gain_block, ((0, 0), (0, 124)))
    qkv_grad = jnp.concatenate(
        [contract_rows(normed_all, d_qkv).astype(jnp.bfloat16), gain_block.astype(jnp.bfloat16)], axis=1
    )
    mlp_grads, qkv_grad = lax.optimization_barrier((mlp_grads, qkv_grad))
    mlp_grads = [g.astype(jnp.float32) for g in mlp_grads]
    g_out_t = mlp_grads[1][:, 3 * ff_half :]
    mlp_grads = [split_cols(g[:, : 3 * ff_half], [2 * ff_half, ff_half]) for g in mlp_grads]
    g_qkv, g_gains = split_cols(
        lax.psum_scatter(qkv_grad, "wide", scatter_dimension=0, tiled=True).astype(jnp.float32),
        [q_cols + 2 * kv_cols, 128],
    )
    d_normed = narrow_scatter(d_normed_partial, relative)
    d_input_part, _ = rms_back(inputs, gain_attn, d_normed)
    d_tokens = d_resid + d_input_part
    attn_gain_grad = g_gains[:, 0]
    mlp_gain_grad = g_gains[:, 1]
    query_gain_grad = g_gains[:hd_local, 2]
    key_gain_grad = g_gains[:hd_local, 3]

    g_query = g_qkv[:, :q_cols]
    g_key = g_qkv[:, q_cols : q_cols + kv_cols]
    g_value = g_qkv[:, q_cols + kv_cols :]
    g_gate = jnp.concatenate([mlp_grads[h][0][:, :ff_half] for h in range(2)], axis=1)
    g_up = jnp.concatenate([mlp_grads[h][0][:, ff_half:] for h in range(2)], axis=1)
    g_down = jnp.concatenate([mlp_grads[h][1] for h in range(2)], axis=1).T
    output = (resid + narrow_scatter(down_partial, relative)).astype(jnp.bfloat16)
    return (
        output,
        d_tokens,
        attn_gain_grad,
        g_query,
        g_key,
        g_value,
        query_gain_grad,
        key_gain_grad,
        g_out_t.T,
        mlp_gain_grad,
        g_gate,
        g_up,
        g_down,
    )


def solution(mesh):
    in_specs = (
        P(("wide", "narrow"), None),
        P("wide", None),
        P(("wide", "narrow"), None),
        P("wide"),
        P("wide", "narrow"),
        P("wide", "narrow"),
        P("wide", "narrow"),
        P("wide"),
        P("wide"),
        P("narrow", "wide"),
        P("wide"),
        P("wide", "narrow"),
        P("wide", "narrow"),
        P("narrow", "wide"),
    )
    out_specs = (
        P(("wide", "narrow"), None),
        P(("wide", "narrow"), None),
        P("wide"),
        P("wide", "narrow"),
        P("wide", "narrow"),
        P("wide", "narrow"),
        P("wide"),
        P("wide"),
        P("narrow", "wide"),
        P("wide"),
        P("wide", "narrow"),
        P("wide", "narrow"),
        P("narrow", "wide"),
    )
    return jax.shard_map(shards_body, mesh=mesh, in_specs=in_specs, out_specs=out_specs, check_vma=False)
```

```python
import jax
import jax.numpy as jnp
from jax import lax
from jax.sharding import PartitionSpec as P


H = 16
KV = 8
HD = 128


EPS = 1e-06
ROPE_BASE = 1000000.0
NEG_FILL = -1e30

XPERM = [(0, 1), (1, 0), (2, 3), (3, 2)]
YPERM = [(0, 2), (2, 0), (1, 3), (3, 1)]
BLOCK_XOR = (0, 1, 2, 3, 0, 2, 1, 3)


def rms_apply(values, gain):
    return values * lax.rsqrt(jnp.mean(values * values, axis=-1, keepdims=True) + EPS) * gain


def rms_back(values, gain, grad):
    scale = lax.rsqrt(jnp.mean(values * values, axis=-1, keepdims=True) + EPS)
    weighted = grad * gain
    inner = jnp.mean(weighted * values, axis=-1, keepdims=True)
    d_values = scale * weighted - values * (scale * scale * scale) * inner
    return (d_values, grad * values * scale)


def rotate(values):
    half = values.shape[-1] // 2
    return jnp.concatenate([-values[..., half:], values[..., :half]], axis=-1)


def rotate_back(values):
    half = values.shape[-1] // 2
    return jnp.concatenate([values[..., half:], -values[..., :half]], axis=-1)


def doc_positions(doc_rows):
    index = lax.broadcasted_iota(jnp.int32, doc_rows.shape, 1)
    change = jnp.concatenate(
        [jnp.ones((doc_rows.shape[0], 1), jnp.bool_), doc_rows[:, 1:] != doc_rows[:, :-1]], axis=1
    )
    begin = lax.cummax(jnp.where(change, index, 0), axis=1)
    return index - begin


def rope_from_positions(position):
    freqs = ROPE_BASE ** (-(jnp.arange(HD // 2, dtype=jnp.float32) * (2.0 / HD)))
    angle = position.astype(jnp.float32)[..., None] * freqs
    cosine = jnp.cos(angle)
    sine = jnp.sin(angle)
    return (jnp.concatenate([cosine, cosine], axis=-1), jnp.concatenate([sine, sine], axis=-1))


def contract_rows(left, right):
    return lax.dot_general(
        left, right, (((0,), (0,)), ((), ())), preferred_element_type=jnp.float32
    )


def times_transposed(left, right):
    return lax.dot_general(
        left, right, (((1,), (1,)), ((), ())), preferred_element_type=jnp.float32
    )


def relative_ok(seq_count):
    return lax.axis_size("narrow") == 4 and seq_count == 1


def relative_rows(vec):
    n = lax.axis_index("narrow")
    half = vec.shape[0] // 8
    split = vec.reshape(4, 2, half)
    pieces = []
    for blk, flip in enumerate(BLOCK_XOR):
        source = split[:, 1 if blk >= 4 else 0]
        pieces.append(lax.dynamic_index_in_dim(source, jnp.bitwise_xor(n, flip), 0, keepdims=False))
    return jnp.concatenate(pieces)


def narrow_allreduce(v):
    if lax.axis_size("narrow") != 4:
        return lax.psum(v, "narrow")
    v = v + lax.ppermute(v, "narrow", XPERM)
    return v + lax.ppermute(v, "narrow", YPERM)


def narrow_gather(x, relative):
    if not relative:
        return lax.all_gather(x, "narrow", axis=0, tiled=True)
    half = x.shape[0] // 2
    a, b = x[:half], x[half:]
    a_x = lax.ppermute(a, "narrow", XPERM)
    b_y = lax.ppermute(b, "narrow", YPERM)
    a_pair = jnp.concatenate([a, a_x], axis=0)
    b_pair = jnp.concatenate([b, b_y], axis=0)
    a_pair_y = lax.ppermute(a_pair, "narrow", YPERM)
    b_pair_x = lax.ppermute(b_pair, "narrow", XPERM)
    return jnp.concatenate([a_pair, a_pair_y, b_pair, b_pair_x], axis=0)


def narrow_scatter(x, relative):
    if not relative:
        return lax.psum_scatter(
            x.astype(jnp.bfloat16), "narrow", scatter_dimension=0, tiled=True
        ).astype(jnp.float32)
    rows, c = x.shape
    half = rows // 8
    blocks = x.reshape(8, half, c)
    a_got = lax.ppermute(blocks[2:4].astype(jnp.bfloat16), "narrow", YPERM)
    b_got = lax.ppermute(blocks[6:8].astype(jnp.bfloat16), "narrow", XPERM)
    a_sum = blocks[0:2] + a_got.astype(jnp.float32)
    b_sum = blocks[4:6] + b_got.astype(jnp.float32)
    a_got2 = lax.ppermute(a_sum[1].astype(jnp.bfloat16), "narrow", XPERM)
    b_got2 = lax.ppermute(b_sum[1].astype(jnp.bfloat16), "narrow", YPERM)
    return jnp.concatenate(
        [a_sum[0] + a_got2.astype(jnp.float32), b_sum[0] + b_got2.astype(jnp.float32)], axis=0
    )


def split_cols(joined, widths):
    out = []
    start = 0
    for w in widths:
        out.append(joined[:, start : start + w])
        start += w
    return out


def wide_gather(blocks):
    joined = lax.all_gather(jnp.concatenate(blocks, axis=1), "wide", axis=0, tiled=True)
    return split_cols(joined, [blk.shape[1] for blk in blocks])


def shards_body(
    tokens,
    doc_ids,
    cotangent,
    attn_gain,
    w_query,
    w_key,
    w_value,
    query_gain,
    key_gain,
    w_out,
    mlp_gain,
    w_gate,
    w_up,
    w_down,
):
    narrow_size = lax.axis_size("narrow")
    wide_size = lax.axis_size("wide")
    heads_here = H // narrow_size
    groups_here = KV // narrow_size
    repeat = H // KV
    seq_count, length = doc_ids.shape
    rows_group = seq_count * length
    scale = HD ** (-0.5)
    d_local = attn_gain.shape[0]
    hd_local = query_gain.shape[0]
    q_cols = w_query.shape[1]
    kv_cols = w_key.shape[1]
    ff_cols = w_gate.shape[1]
    ff_half = ff_cols // 2
    relative = relative_ok(seq_count)

    tokens_all = narrow_gather(tokens, relative)
    grad_rows = narrow_gather(cotangent, relative)

    pad_hd = ((0, d_local - hd_local),)
    gain_block = jnp.pad(
        jnp.stack(
            [attn_gain, mlp_gain, jnp.pad(query_gain, pad_hd), jnp.pad(key_gain, pad_hd)], axis=1
        ),
        ((0, 0), (0, 124)),
    )
    qkv_w, out_wt, gains_all = wide_gather(
        [jnp.concatenate([w_query, w_key, w_value], axis=1), w_out.T, gain_block]
    )
    gain_attn = gains_all[:, 0].astype(jnp.float32)
    gain_mlp = gains_all[:, 1].astype(jnp.float32)
    gains_split = gains_all.reshape(wide_size, d_local, 128)
    gain_query = gains_split[:, :hd_local, 2].reshape(-1).astype(jnp.float32)
    gain_key = gains_split[:, :hd_local, 3].reshape(-1).astype(jnp.float32)
    down_t = w_down.T
    mlp_sets = []
    for h in range(2):
        cols = slice(h * ff_half, (h + 1) * ff_half)
        mlp_sets.append(
            wide_gather([jnp.concatenate([w_gate[:, cols], w_up[:, cols]], axis=1), down_t[:, cols]])
        )

    if relative:
        order = relative_rows(jnp.arange(rows_group, dtype=jnp.int32))
        doc_row = relative_rows(doc_ids[0])
        position = relative_rows(doc_positions(doc_ids)[0])
    else:
        order = jnp.arange(rows_group, dtype=jnp.int32)
        doc_row = doc_ids.reshape(-1)
        position = doc_positions(doc_ids).reshape(-1)
    cosine, sine = rope_from_positions(position)
    cos_heads = cosine[:, None, :]
    sin_heads = sine[:, None, :]
    allowed = (order[None, :] <= order[:, None]) & (doc_row[None, :] == doc_row[:, None])
    if not relative:
        seq_of = jnp.arange(rows_group, dtype=jnp.int32) // length
        allowed = allowed & (seq_of[None, :] == seq_of[:, None])

    inputs = tokens.astype(jnp.float32)
    normed_all = rms_apply(tokens_all.astype(jnp.float32), gain_attn).astype(jnp.bfloat16)
    qkv = jnp.dot(normed_all, qkv_w, preferred_element_type=jnp.float32)
    q_pre = qkv[:, :q_cols].reshape(rows_group, heads_here, HD)
    k_pre = qkv[:, q_cols : q_cols + kv_cols].reshape(rows_group, groups_here, HD)
    v_use = qkv[:, q_cols + kv_cols :].astype(jnp.bfloat16).reshape(rows_group, groups_here, HD)
    q_norm = rms_apply(q_pre, gain_query)
    k_norm = rms_apply(k_pre, gain_key)
    q_use = (q_norm * cos_heads + rotate(q_norm) * sin_heads).astype(jnp.bfloat16)
    k_use = (k_norm * cos_heads + rotate(k_norm) * sin_heads).astype(jnp.bfloat16)
    q_grouped = q_use.reshape(rows_group, groups_here, repeat, HD)

    scores = jnp.einsum("qgrd,kgd->grqk", q_grouped, k_use, preferred_element_type=jnp.float32) * scale
    scores = jnp.where(allowed, scores, NEG_FILL)
    top = jnp.max(scores, axis=-1, keepdims=True)
    weights = jnp.exp(scores - top)
    total = jnp.sum(weights, axis=-1, keepdims=True)
    probs = weights / total
    mixed = jnp.einsum(
        "grqk,kgd->qgrd", probs.astype(jnp.bfloat16), v_use, preferred_element_type=jnp.float32
    )
    log_totals = (top + jnp.log(total))[..., 0]
    attended = mixed.astype(jnp.bfloat16).reshape(rows_group, heads_here * HD)

    resid = inputs + narrow_scatter(times_transposed(attended, out_wt), relative)
    mlp_in = rms_apply(resid, gain_mlp).astype(jnp.bfloat16)
    mlp_all = narrow_gather(mlp_in, relative)

    down_partial = None
    d_mlp_partial = None
    mlp_grads = []
    for h in range(2):
        gate_up_w, down_wt = mlp_sets[h]
        gate_up = jnp.dot(mlp_all, gate_up_w, preferred_element_type=jnp.float32)
        gate = gate_up[:, :ff_half]
        up = gate_up[:, ff_half:]
        sigmoid = jax.nn.sigmoid(gate)
        hidden = (gate * sigmoid * up).astype(jnp.bfloat16)
        part = times_transposed(hidden, down_wt)
        down_partial = part if down_partial is None else down_partial + part
        d_hidden = jnp.dot(grad_rows, down_wt, preferred_element_type=jnp.float32)
        d_up = (d_hidden * gate * sigmoid).astype(jnp.bfloat16)
        d_gate = (d_hidden * up * sigmoid * (1.0 + gate * (1.0 - sigmoid))).astype(jnp.bfloat16)
        d_gate_up = jnp.concatenate([d_gate, d_up], axis=1)
        part = times_transposed(d_gate_up, gate_up_w)
        d_mlp_partial = part if d_mlp_partial is None else d_mlp_partial + part
        g_down_t = contract_rows(grad_rows, hidden)
        g_gate_up = contract_rows(mlp_all, d_gate_up)
        joined = jnp.concatenate(
            [g_gate_up.astype(jnp.bfloat16), g_down_t.astype(jnp.bfloat16)], axis=1
        )
        if h == 0:
            joined, mlp_sets[1] = lax.optimization_barrier((joined, mlp_sets[1]))
            mlp_grads.append(lax.psum_scatter(joined, "wide", scatter_dimension=0, tiled=True))
        else:
            last_joined = joined

    d_mlp_in = narrow_scatter(d_mlp_partial, relative)
    d_part, mlp_gain_terms = rms_back(resid, gain_mlp, d_mlp_in)
    grad_mlp_gain = jnp.sum(mlp_gain_terms, axis=0)
    d_resid = cotangent.astype(jnp.float32) + d_part
    p_scores = (
        jnp.einsum("qgrd,kgd->grqk", q_grouped, k_use, preferred_element_type=jnp.float32) * scale
    )
    p_probs = jnp.where(allowed, jnp.exp(p_scores - log_totals[..., None]), 0.0)
    d_resid_low, last_joined = lax.optimization_barrier((d_resid.astype(jnp.bfloat16), last_joined))
    branch_rows = narrow_gather(d_resid_low, relative)
    out_grad = contract_rows(branch_rows, attended).astype(jnp.bfloat16)
    mlp_grads.append(
        lax.psum_scatter(
            jnp.concatenate([last_joined, out_grad], axis=1), "wide", scatter_dimension=0, tiled=True
        )
    )
    d_attended = jnp.dot(branch_rows, out_wt, preferred_element_type=jnp.float32).astype(jnp.bfloat16)
    d_mixed = d_attended.reshape(rows_group, groups_here, repeat, HD)

    d_probs = jnp.einsum("qgrd,kgd->grqk", d_mixed, v_use, preferred_element_type=jnp.float32)
    inner = jnp.sum(p_probs * d_probs, axis=-1, keepdims=True)
    d_scores = (p_probs * (d_probs - inner)).astype(jnp.bfloat16)
    d_query = jnp.einsum("grqk,kgd->qgrd", d_scores, k_use, preferred_element_type=jnp.float32) * scale
    d_key = jnp.einsum("grqk,qgrd->kgd", d_scores, q_grouped, preferred_element_type=jnp.float32) * scale
    d_value = jnp.einsum(
        "grqk,qgrd->kgd", p_probs.astype(jnp.bfloat16), d_mixed, preferred_element_type=jnp.float32
    ).astype(jnp.bfloat16)

    d_query = d_query.reshape(rows_group, heads_here, HD)
    d_q_norm = d_query * cos_heads + rotate_back(d_query * sin_heads)
    d_k_norm = d_key * cos_heads + rotate_back(d_key * sin_heads)
    d_q_pre, query_terms = rms_back(q_pre, gain_query, d_q_norm)
    d_k_pre, key_terms = rms_back(k_pre, gain_key, d_k_norm)
    grad_query_gain = jnp.sum(query_terms, axis=(0, 1))
    grad_key_gain = jnp.sum(key_terms, axis=(0, 1))
    d_qkv = jnp.concatenate(
        [
            d_q_pre.astype(jnp.bfloat16).reshape(rows_group, heads_here * HD),
            d_k_pre.astype(jnp.bfloat16).reshape(rows_group, groups_here * HD),
            d_value.reshape(rows_group, groups_here * HD),
        ],
        axis=1,
    )
    d_normed_partial = times_transposed(d_qkv, qkv_w)
    tokens_all_f = tokens_all.astype(jnp.float32)
    scale_all = lax.rsqrt(jnp.mean(tokens_all_f * tokens_all_f, axis=-1, keepdims=True) + EPS)
    attn_gain_part = jnp.sum(d_normed_partial * tokens_all_f * scale_all, axis=0)
    gain_parts = narrow_allreduce(
        jnp.concatenate([attn_gain_part, grad_mlp_gain, grad_query_gain, grad_key_gain])
    )
    d_full = d_local * wide_size
    hd_full = hd_local * wide_size

    def by_chunk(vec, size):
        return jnp.pad(vec.reshape(wide_size, size), ((0, 0), (0, d_local - size)))

    gain_block = jnp.stack(
        [
            by_chunk(gain_parts[:d_full], d_local),
            by_chunk(gain_parts[d_full : 2 * d_full], d_local),
            by_chunk(gain_parts[2 * d_full : 2 * d_full + hd_full], hd_local),
            by_chunk(gain_parts[2 * d_full + hd_full :], hd_local),
        ],
        axis=-1,
    ).reshape(d_full, 4)
    gain_block = jnp.pad(gain_block, ((0, 0), (0, 124)))
    qkv_grad = jnp.concatenate(
        [contract_rows(normed_all, d_qkv).astype(jnp.bfloat16), gain_block.astype(jnp.bfloat16)], axis=1
    )
    mlp_grads, qkv_grad = lax.optimization_barrier((mlp_grads, qkv_grad))
    mlp_grads = [g.astype(jnp.float32) for g in mlp_grads]
    g_out_t = mlp_grads[1][:, 3 * ff_half :]
    mlp_grads = [split_cols(g[:, : 3 * ff_half], [2 * ff_half, ff_half]) for g in mlp_grads]
    g_qkv, g_gains = split_cols(
        lax.psum_scatter(qkv_grad, "wide", scatter_dimension=0, tiled=True).astype(jnp.float32),
        [q_cols + 2 * kv_cols, 128],
    )
    d_normed = narrow_scatter(d_normed_partial, relative)
    d_input_part, _ = rms_back(inputs, gain_attn, d_normed)
    d_tokens = d_resid + d_input_part
    attn_gain_grad = g_gains[:, 0]
    mlp_gain_grad = g_gains[:, 1]
    query_gain_grad = g_gains[:hd_local, 2]
    key_gain_grad = g_gains[:hd_local, 3]

    g_query = g_qkv[:, :q_cols]
    g_key = g_qkv[:, q_cols : q_cols + kv_cols]
    g_value = g_qkv[:, q_cols + kv_cols :]
    g_gate = jnp.concatenate([mlp_grads[h][0][:, :ff_half] for h in range(2)], axis=1)
    g_up = jnp.concatenate([mlp_grads[h][0][:, ff_half:] for h in range(2)], axis=1)
    g_down = jnp.concatenate([mlp_grads[h][1] for h in range(2)], axis=1).T
    output = (resid + narrow_scatter(down_partial, relative)).astype(jnp.bfloat16)
    return (
        output,
        d_tokens,
        attn_gain_grad,
        g_query,
        g_key,
        g_value,
        query_gain_grad,
        key_gain_grad,
        g_out_t.T,
        mlp_gain_grad,
        g_gate,
        g_up,
        g_down,
    )


def solution(mesh):
    in_specs = (
        P(("wide", "narrow"), None),
        P("wide", None),
        P(("wide", "narrow"), None),
        P("wide"),
        P("wide", "narrow"),
        P("wide", "narrow"),
        P("wide", "narrow"),
        P("wide"),
        P("wide"),
        P("narrow", "wide"),
        P("wide"),
        P("wide", "narrow"),
        P("wide", "narrow"),
        P("narrow", "wide"),
    )
    out_specs = (
        P(("wide", "narrow"), None),
        P(("wide", "narrow"), None),
        P("wide"),
        P("wide", "narrow"),
        P("wide", "narrow"),
        P("wide", "narrow"),
        P("wide"),
        P("wide"),
        P("narrow", "wide"),
        P("wide"),
        P("wide", "narrow"),
        P("wide", "narrow"),
        P("narrow", "wide"),
    )
    return jax.shard_map(shards_body, mesh=mesh, in_specs=in_specs, out_specs=out_specs, check_vma=False)
```

```python
import jax
import jax.numpy as jnp
from jax import lax
from jax.sharding import PartitionSpec as P


H = 16
KV = 8
HD = 128


EPS = 1e-06
ROPE_BASE = 1000000.0
NEG_FILL = -1e30

XPERM = [(0, 1), (1, 0), (2, 3), (3, 2)]
YPERM = [(0, 2), (2, 0), (1, 3), (3, 1)]
BLOCK_XOR = (0, 1, 2, 3, 0, 2, 1, 3)


def rms_apply(values, gain):
    return values * lax.rsqrt(jnp.mean(values * values, axis=-1, keepdims=True) + EPS) * gain


def rms_back(values, gain, grad):
    scale = lax.rsqrt(jnp.mean(values * values, axis=-1, keepdims=True) + EPS)
    weighted = grad * gain
    inner = jnp.mean(weighted * values, axis=-1, keepdims=True)
    d_values = scale * weighted - values * (scale * scale * scale) * inner
    return (d_values, grad * values * scale)


def rotate(values):
    half = values.shape[-1] // 2
    return jnp.concatenate([-values[..., half:], values[..., :half]], axis=-1)


def rotate_back(values):
    half = values.shape[-1] // 2
    return jnp.concatenate([values[..., half:], -values[..., :half]], axis=-1)


def doc_positions(doc_rows):
    index = lax.broadcasted_iota(jnp.int32, doc_rows.shape, 1)
    change = jnp.concatenate(
        [jnp.ones((doc_rows.shape[0], 1), jnp.bool_), doc_rows[:, 1:] != doc_rows[:, :-1]], axis=1
    )
    begin = lax.cummax(jnp.where(change, index, 0), axis=1)
    return index - begin


def rope_from_positions(position):
    freqs = ROPE_BASE ** (-(jnp.arange(HD // 2, dtype=jnp.float32) * (2.0 / HD)))
    angle = position.astype(jnp.float32)[..., None] * freqs
    cosine = jnp.cos(angle)
    sine = jnp.sin(angle)
    return (jnp.concatenate([cosine, cosine], axis=-1), jnp.concatenate([sine, sine], axis=-1))


def contract_rows(left, right):
    return lax.dot_general(
        left, right, (((0,), (0,)), ((), ())), preferred_element_type=jnp.float32
    )


def times_transposed(left, right):
    return lax.dot_general(
        left, right, (((1,), (1,)), ((), ())), preferred_element_type=jnp.float32
    )


def relative_ok(seq_count):
    return lax.axis_size("narrow") == 4 and seq_count == 1


def relative_rows(vec):
    n = lax.axis_index("narrow")
    half = vec.shape[0] // 8
    split = vec.reshape(4, 2, half)
    pieces = []
    for blk, flip in enumerate(BLOCK_XOR):
        source = split[:, 1 if blk >= 4 else 0]
        pieces.append(lax.dynamic_index_in_dim(source, jnp.bitwise_xor(n, flip), 0, keepdims=False))
    return jnp.concatenate(pieces)


def narrow_allreduce(v):
    if lax.axis_size("narrow") != 4:
        return lax.psum(v, "narrow")
    v = v + lax.ppermute(v, "narrow", XPERM)
    return v + lax.ppermute(v, "narrow", YPERM)


def narrow_gather(x, relative):
    if not relative:
        return lax.all_gather(x, "narrow", axis=0, tiled=True)
    half = x.shape[0] // 2
    a, b = x[:half], x[half:]
    a_x = lax.ppermute(a, "narrow", XPERM)
    b_y = lax.ppermute(b, "narrow", YPERM)
    a_pair = jnp.concatenate([a, a_x], axis=0)
    b_pair = jnp.concatenate([b, b_y], axis=0)
    a_pair_y = lax.ppermute(a_pair, "narrow", YPERM)
    b_pair_x = lax.ppermute(b_pair, "narrow", XPERM)
    return jnp.concatenate([a_pair, a_pair_y, b_pair, b_pair_x], axis=0)


def narrow_scatter(x, relative):
    if not relative:
        return lax.psum_scatter(
            x.astype(jnp.bfloat16), "narrow", scatter_dimension=0, tiled=True
        ).astype(jnp.float32)
    rows, c = x.shape
    half = rows // 8
    blocks = x.reshape(8, half, c)
    a_got = lax.ppermute(blocks[2:4].astype(jnp.bfloat16), "narrow", YPERM)
    b_got = lax.ppermute(blocks[6:8].astype(jnp.bfloat16), "narrow", XPERM)
    a_sum = blocks[0:2] + a_got.astype(jnp.float32)
    b_sum = blocks[4:6] + b_got.astype(jnp.float32)
    a_got2 = lax.ppermute(a_sum[1].astype(jnp.bfloat16), "narrow", XPERM)
    b_got2 = lax.ppermute(b_sum[1].astype(jnp.bfloat16), "narrow", YPERM)
    return jnp.concatenate(
        [a_sum[0] + a_got2.astype(jnp.float32), b_sum[0] + b_got2.astype(jnp.float32)], axis=0
    )


def split_cols(joined, widths):
    out = []
    start = 0
    for w in widths:
        out.append(joined[:, start : start + w])
        start += w
    return out


def wide_gather(blocks):
    joined = lax.all_gather(jnp.concatenate(blocks, axis=1), "wide", axis=0, tiled=True)
    return split_cols(joined, [blk.shape[1] for blk in blocks])


def shards_body(
    tokens,
    doc_ids,
    cotangent,
    attn_gain,
    w_query,
    w_key,
    w_value,
    query_gain,
    key_gain,
    w_out,
    mlp_gain,
    w_gate,
    w_up,
    w_down,
):
    narrow_size = lax.axis_size("narrow")
    wide_size = lax.axis_size("wide")
    heads_here = H // narrow_size
    groups_here = KV // narrow_size
    repeat = H // KV
    seq_count, length = doc_ids.shape
    rows_group = seq_count * length
    scale = HD ** (-0.5)
    d_local = attn_gain.shape[0]
    hd_local = query_gain.shape[0]
    q_cols = w_query.shape[1]
    kv_cols = w_key.shape[1]
    ff_cols = w_gate.shape[1]
    ff_first = max(128, (2 * ff_cols // 3) // 128 * 128)
    ff_parts = (ff_first, ff_cols - ff_first)
    ff_starts = (0, ff_first)
    relative = relative_ok(seq_count)

    tokens_all = narrow_gather(tokens, relative)
    grad_rows = narrow_gather(cotangent, relative)

    pad_hd = ((0, d_local - hd_local),)
    gain_block = jnp.pad(
        jnp.stack(
            [attn_gain, mlp_gain, jnp.pad(query_gain, pad_hd), jnp.pad(key_gain, pad_hd)], axis=1
        ),
        ((0, 0), (0, 124)),
    )
    qkv_w, out_wt, gains_all = wide_gather(
        [jnp.concatenate([w_query, w_key, w_value], axis=1), w_out.T, gain_block]
    )
    gain_attn = gains_all[:, 0].astype(jnp.float32)
    gain_mlp = gains_all[:, 1].astype(jnp.float32)
    gains_split = gains_all.reshape(wide_size, d_local, 128)
    gain_query = gains_split[:, :hd_local, 2].reshape(-1).astype(jnp.float32)
    gain_key = gains_split[:, :hd_local, 3].reshape(-1).astype(jnp.float32)
    down_t = w_down.T
    mlp_sets = []
    for h in range(2):
        cols = slice(ff_starts[h], ff_starts[h] + ff_parts[h])
        mlp_sets.append(
            wide_gather([jnp.concatenate([w_gate[:, cols], w_up[:, cols]], axis=1), down_t[:, cols]])
        )

    if relative:
        order = relative_rows(jnp.arange(rows_group, dtype=jnp.int32))
        doc_row = relative_rows(doc_ids[0])
        position = relative_rows(doc_positions(doc_ids)[0])
    else:
        order = jnp.arange(rows_group, dtype=jnp.int32)
        doc_row = doc_ids.reshape(-1)
        position = doc_positions(doc_ids).reshape(-1)
    cosine, sine = rope_from_positions(position)
    cos_heads = cosine[:, None, :]
    sin_heads = sine[:, None, :]
    allowed = (order[None, :] <= order[:, None]) & (doc_row[None, :] == doc_row[:, None])
    if not relative:
        seq_of = jnp.arange(rows_group, dtype=jnp.int32) // length
        allowed = allowed & (seq_of[None, :] == seq_of[:, None])

    inputs = tokens.astype(jnp.float32)
    normed_all = rms_apply(tokens_all.astype(jnp.float32), gain_attn).astype(jnp.bfloat16)
    qkv = jnp.dot(normed_all, qkv_w, preferred_element_type=jnp.float32)
    q_pre = qkv[:, :q_cols].reshape(rows_group, heads_here, HD)
    k_pre = qkv[:, q_cols : q_cols + kv_cols].reshape(rows_group, groups_here, HD)
    v_use = qkv[:, q_cols + kv_cols :].astype(jnp.bfloat16).reshape(rows_group, groups_here, HD)
    q_norm = rms_apply(q_pre, gain_query)
    k_norm = rms_apply(k_pre, gain_key)
    q_use = (q_norm * cos_heads + rotate(q_norm) * sin_heads).astype(jnp.bfloat16)
    k_use = (k_norm * cos_heads + rotate(k_norm) * sin_heads).astype(jnp.bfloat16)
    q_grouped = q_use.reshape(rows_group, groups_here, repeat, HD)

    scores = jnp.einsum("qgrd,kgd->grqk", q_grouped, k_use, preferred_element_type=jnp.float32) * scale
    scores = jnp.where(allowed, scores, NEG_FILL)
    top = jnp.max(scores, axis=-1, keepdims=True)
    weights = jnp.exp(scores - top)
    total = jnp.sum(weights, axis=-1, keepdims=True)
    probs = weights / total
    mixed = jnp.einsum(
        "grqk,kgd->qgrd", probs.astype(jnp.bfloat16), v_use, preferred_element_type=jnp.float32
    )
    log_totals = (top + jnp.log(total))[..., 0]
    attended = mixed.astype(jnp.bfloat16).reshape(rows_group, heads_here * HD)

    resid = inputs + narrow_scatter(times_transposed(attended, out_wt), relative)
    mlp_in = rms_apply(resid, gain_mlp).astype(jnp.bfloat16)
    mlp_all = narrow_gather(mlp_in, relative)

    down_partial = None
    d_mlp_partial = None
    mlp_grads = []
    for h in range(2):
        gate_up_w, down_wt = mlp_sets[h]
        gate_up = jnp.dot(mlp_all, gate_up_w, preferred_element_type=jnp.float32)
        gate = gate_up[:, : ff_parts[h]]
        up = gate_up[:, ff_parts[h] :]
        sigmoid = jax.nn.sigmoid(gate)
        hidden = (gate * sigmoid * up).astype(jnp.bfloat16)
        part = times_transposed(hidden, down_wt)
        down_partial = part if down_partial is None else down_partial + part
        d_hidden = jnp.dot(grad_rows, down_wt, preferred_element_type=jnp.float32)
        d_up = (d_hidden * gate * sigmoid).astype(jnp.bfloat16)
        d_gate = (d_hidden * up * sigmoid * (1.0 + gate * (1.0 - sigmoid))).astype(jnp.bfloat16)
        d_gate_up = jnp.concatenate([d_gate, d_up], axis=1)
        part = times_transposed(d_gate_up, gate_up_w)
        d_mlp_partial = part if d_mlp_partial is None else d_mlp_partial + part
        g_down_t = contract_rows(grad_rows, hidden)
        g_gate_up = contract_rows(mlp_all, d_gate_up)
        joined = jnp.concatenate(
            [g_gate_up.astype(jnp.bfloat16), g_down_t.astype(jnp.bfloat16)], axis=1
        )
        if h == 0:
            joined, mlp_sets[1] = lax.optimization_barrier((joined, mlp_sets[1]))
            mlp_grads.append(lax.psum_scatter(joined, "wide", scatter_dimension=0, tiled=True))
        else:
            last_joined = joined

    d_mlp_in = narrow_scatter(d_mlp_partial, relative)
    d_part, mlp_gain_terms = rms_back(resid, gain_mlp, d_mlp_in)
    grad_mlp_gain = jnp.sum(mlp_gain_terms, axis=0)
    d_resid = cotangent.astype(jnp.float32) + d_part
    p_scores = (
        jnp.einsum("qgrd,kgd->grqk", q_grouped, k_use, preferred_element_type=jnp.float32) * scale
    )
    p_probs = jnp.where(allowed, jnp.exp(p_scores - log_totals[..., None]), 0.0)
    d_resid_low, last_joined = lax.optimization_barrier((d_resid.astype(jnp.bfloat16), last_joined))
    mlp_grads.append(lax.psum_scatter(last_joined, "wide", scatter_dimension=0, tiled=True))
    branch_rows = narrow_gather(d_resid_low, relative)
    out_grad = contract_rows(branch_rows, attended).astype(jnp.bfloat16)
    mlp_grads, out_grad = lax.optimization_barrier((mlp_grads, out_grad))
    mlp_grads = [
        split_cols(g.astype(jnp.float32), [2 * ff_parts[h], ff_parts[h]]) for h, g in enumerate(mlp_grads)
    ]
    g_out_t = lax.psum_scatter(out_grad, "wide", scatter_dimension=0, tiled=True).astype(jnp.float32)
    d_attended = jnp.dot(branch_rows, out_wt, preferred_element_type=jnp.float32).astype(jnp.bfloat16)
    d_mixed = d_attended.reshape(rows_group, groups_here, repeat, HD)

    d_probs = jnp.einsum("qgrd,kgd->grqk", d_mixed, v_use, preferred_element_type=jnp.float32)
    inner = jnp.sum(p_probs * d_probs, axis=-1, keepdims=True)
    d_scores = (p_probs * (d_probs - inner)).astype(jnp.bfloat16)
    d_query = jnp.einsum("grqk,kgd->qgrd", d_scores, k_use, preferred_element_type=jnp.float32) * scale
    d_key = jnp.einsum("grqk,qgrd->kgd", d_scores, q_grouped, preferred_element_type=jnp.float32) * scale
    d_value = jnp.einsum(
        "grqk,qgrd->kgd", p_probs.astype(jnp.bfloat16), d_mixed, preferred_element_type=jnp.float32
    ).astype(jnp.bfloat16)

    d_query = d_query.reshape(rows_group, heads_here, HD)
    d_q_norm = d_query * cos_heads + rotate_back(d_query * sin_heads)
    d_k_norm = d_key * cos_heads + rotate_back(d_key * sin_heads)
    d_q_pre, query_terms = rms_back(q_pre, gain_query, d_q_norm)
    d_k_pre, key_terms = rms_back(k_pre, gain_key, d_k_norm)
    grad_query_gain = jnp.sum(query_terms, axis=(0, 1))
    grad_key_gain = jnp.sum(key_terms, axis=(0, 1))
    d_qkv = jnp.concatenate(
        [
            d_q_pre.astype(jnp.bfloat16).reshape(rows_group, heads_here * HD),
            d_k_pre.astype(jnp.bfloat16).reshape(rows_group, groups_here * HD),
            d_value.reshape(rows_group, groups_here * HD),
        ],
        axis=1,
    )
    d_normed_partial = times_transposed(d_qkv, qkv_w)
    tokens_all_f = tokens_all.astype(jnp.float32)
    scale_all = lax.rsqrt(jnp.mean(tokens_all_f * tokens_all_f, axis=-1, keepdims=True) + EPS)
    attn_gain_part = jnp.sum(d_normed_partial * tokens_all_f * scale_all, axis=0)
    gain_parts = narrow_allreduce(
        jnp.concatenate([attn_gain_part, grad_mlp_gain, grad_query_gain, grad_key_gain])
    )
    d_full = d_local * wide_size
    hd_full = hd_local * wide_size

    def by_chunk(vec, size):
        return jnp.pad(vec.reshape(wide_size, size), ((0, 0), (0, d_local - size)))

    gain_block = jnp.stack(
        [
            by_chunk(gain_parts[:d_full], d_local),
            by_chunk(gain_parts[d_full : 2 * d_full], d_local),
            by_chunk(gain_parts[2 * d_full : 2 * d_full + hd_full], hd_local),
            by_chunk(gain_parts[2 * d_full + hd_full :], hd_local),
        ],
        axis=-1,
    ).reshape(d_full, 4)
    gain_block = jnp.pad(gain_block, ((0, 0), (0, 124)))
    qkv_grad = jnp.concatenate(
        [contract_rows(normed_all, d_qkv).astype(jnp.bfloat16), gain_block.astype(jnp.bfloat16)], axis=1
    )
    g_out_t, qkv_grad = lax.optimization_barrier((g_out_t, qkv_grad))
    g_qkv, g_gains = split_cols(
        lax.psum_scatter(qkv_grad, "wide", scatter_dimension=0, tiled=True).astype(jnp.float32),
        [q_cols + 2 * kv_cols, 128],
    )
    d_normed = narrow_scatter(d_normed_partial, relative)
    d_input_part, _ = rms_back(inputs, gain_attn, d_normed)
    d_tokens = d_resid + d_input_part
    attn_gain_grad = g_gains[:, 0]
    mlp_gain_grad = g_gains[:, 1]
    query_gain_grad = g_gains[:hd_local, 2]
    key_gain_grad = g_gains[:hd_local, 3]

    g_query = g_qkv[:, :q_cols]
    g_key = g_qkv[:, q_cols : q_cols + kv_cols]
    g_value = g_qkv[:, q_cols + kv_cols :]
    g_gate = jnp.concatenate([mlp_grads[h][0][:, : ff_parts[h]] for h in range(2)], axis=1)
    g_up = jnp.concatenate([mlp_grads[h][0][:, ff_parts[h] :] for h in range(2)], axis=1)
    g_down = jnp.concatenate([mlp_grads[h][1] for h in range(2)], axis=1).T
    output = (resid + narrow_scatter(down_partial, relative)).astype(jnp.bfloat16)
    return (
        output,
        d_tokens,
        attn_gain_grad,
        g_query,
        g_key,
        g_value,
        query_gain_grad,
        key_gain_grad,
        g_out_t.T,
        mlp_gain_grad,
        g_gate,
        g_up,
        g_down,
    )


def solution(mesh):
    in_specs = (
        P(("wide", "narrow"), None),
        P("wide", None),
        P(("wide", "narrow"), None),
        P("wide"),
        P("wide", "narrow"),
        P("wide", "narrow"),
        P("wide", "narrow"),
        P("wide"),
        P("wide"),
        P("narrow", "wide"),
        P("wide"),
        P("wide", "narrow"),
        P("wide", "narrow"),
        P("narrow", "wide"),
    )
    out_specs = (
        P(("wide", "narrow"), None),
        P(("wide", "narrow"), None),
        P("wide"),
        P("wide", "narrow"),
        P("wide", "narrow"),
        P("wide", "narrow"),
        P("wide"),
        P("wide"),
        P("narrow", "wide"),
        P("wide"),
        P("wide", "narrow"),
        P("wide", "narrow"),
        P("narrow", "wide"),
    )
    return jax.shard_map(shards_body, mesh=mesh, in_specs=in_specs, out_specs=out_specs, check_vma=False)
```

```python
import jax
import jax.numpy as jnp
from jax import lax
from jax.sharding import PartitionSpec as P


H = 16
KV = 8
HD = 128


EPS = 1e-06
ROPE_BASE = 1000000.0
NEG_FILL = -1e30

XPERM = [(0, 1), (1, 0), (2, 3), (3, 2)]
YPERM = [(0, 2), (2, 0), (1, 3), (3, 1)]
BLOCK_XOR = (0, 1, 2, 3, 0, 2, 1, 3)


def rms_apply(values, gain):
    return values * lax.rsqrt(jnp.mean(values * values, axis=-1, keepdims=True) + EPS) * gain


def rms_back(values, gain, grad):
    scale = lax.rsqrt(jnp.mean(values * values, axis=-1, keepdims=True) + EPS)
    weighted = grad * gain
    inner = jnp.mean(weighted * values, axis=-1, keepdims=True)
    d_values = scale * weighted - values * (scale * scale * scale) * inner
    return (d_values, grad * values * scale)


def rotate(values):
    half = values.shape[-1] // 2
    return jnp.concatenate([-values[..., half:], values[..., :half]], axis=-1)


def rotate_back(values):
    half = values.shape[-1] // 2
    return jnp.concatenate([values[..., half:], -values[..., :half]], axis=-1)


def doc_positions(doc_rows):
    index = lax.broadcasted_iota(jnp.int32, doc_rows.shape, 1)
    change = jnp.concatenate(
        [jnp.ones((doc_rows.shape[0], 1), jnp.bool_), doc_rows[:, 1:] != doc_rows[:, :-1]], axis=1
    )
    begin = lax.cummax(jnp.where(change, index, 0), axis=1)
    return index - begin


def rope_from_positions(position):
    freqs = ROPE_BASE ** (-(jnp.arange(HD // 2, dtype=jnp.float32) * (2.0 / HD)))
    angle = position.astype(jnp.float32)[..., None] * freqs
    cosine = jnp.cos(angle)
    sine = jnp.sin(angle)
    return (jnp.concatenate([cosine, cosine], axis=-1), jnp.concatenate([sine, sine], axis=-1))


def contract_rows(left, right):
    return lax.dot_general(
        left, right, (((0,), (0,)), ((), ())), preferred_element_type=jnp.float32
    )


def times_transposed(left, right):
    return lax.dot_general(
        left, right, (((1,), (1,)), ((), ())), preferred_element_type=jnp.float32
    )


def relative_ok(seq_count):
    return lax.axis_size("narrow") == 4 and seq_count == 1


def relative_rows(vec):
    n = lax.axis_index("narrow")
    half = vec.shape[0] // 8
    split = vec.reshape(4, 2, half)
    pieces = []
    for blk, flip in enumerate(BLOCK_XOR):
        source = split[:, 1 if blk >= 4 else 0]
        pieces.append(lax.dynamic_index_in_dim(source, jnp.bitwise_xor(n, flip), 0, keepdims=False))
    return jnp.concatenate(pieces)


def narrow_allreduce(v):
    if lax.axis_size("narrow") != 4:
        return lax.psum(v, "narrow")
    v = v + lax.ppermute(v, "narrow", XPERM)
    return v + lax.ppermute(v, "narrow", YPERM)


def narrow_gather(x, relative):
    if not relative:
        return lax.all_gather(x, "narrow", axis=0, tiled=True)
    half = x.shape[0] // 2
    a, b = x[:half], x[half:]
    a_x = lax.ppermute(a, "narrow", XPERM)
    b_y = lax.ppermute(b, "narrow", YPERM)
    a_pair = jnp.concatenate([a, a_x], axis=0)
    b_pair = jnp.concatenate([b, b_y], axis=0)
    a_pair_y = lax.ppermute(a_pair, "narrow", YPERM)
    b_pair_x = lax.ppermute(b_pair, "narrow", XPERM)
    return jnp.concatenate([a_pair, a_pair_y, b_pair, b_pair_x], axis=0)


def narrow_scatter(x, relative):
    if not relative:
        return lax.psum_scatter(
            x.astype(jnp.bfloat16), "narrow", scatter_dimension=0, tiled=True
        ).astype(jnp.float32)
    rows, c = x.shape
    half = rows // 8
    blocks = x.reshape(8, half, c)
    a_got = lax.ppermute(blocks[2:4].astype(jnp.bfloat16), "narrow", YPERM)
    b_got = lax.ppermute(blocks[6:8].astype(jnp.bfloat16), "narrow", XPERM)
    a_sum = blocks[0:2] + a_got.astype(jnp.float32)
    b_sum = blocks[4:6] + b_got.astype(jnp.float32)
    a_got2 = lax.ppermute(a_sum[1].astype(jnp.bfloat16), "narrow", XPERM)
    b_got2 = lax.ppermute(b_sum[1].astype(jnp.bfloat16), "narrow", YPERM)
    return jnp.concatenate(
        [a_sum[0] + a_got2.astype(jnp.float32), b_sum[0] + b_got2.astype(jnp.float32)], axis=0
    )


def split_cols(joined, widths):
    out = []
    start = 0
    for w in widths:
        out.append(joined[:, start : start + w])
        start += w
    return out


def wide_gather(blocks):
    joined = lax.all_gather(jnp.concatenate(blocks, axis=1), "wide", axis=0, tiled=True)
    return split_cols(joined, [blk.shape[1] for blk in blocks])


def shards_body(
    tokens,
    doc_ids,
    cotangent,
    attn_gain,
    w_query,
    w_key,
    w_value,
    query_gain,
    key_gain,
    w_out,
    mlp_gain,
    w_gate,
    w_up,
    w_down,
):
    narrow_size = lax.axis_size("narrow")
    wide_size = lax.axis_size("wide")
    heads_here = H // narrow_size
    groups_here = KV // narrow_size
    repeat = H // KV
    seq_count, length = doc_ids.shape
    rows_group = seq_count * length
    scale = HD ** (-0.5)
    d_local = attn_gain.shape[0]
    hd_local = query_gain.shape[0]
    q_cols = w_query.shape[1]
    kv_cols = w_key.shape[1]
    ff_cols = w_gate.shape[1]
    ff_first = max(128, (2 * ff_cols // 3) // 128 * 128)
    ff_parts = (ff_first, ff_cols - ff_first)
    ff_starts = (0, ff_first)
    relative = relative_ok(seq_count)

    tokens_all = narrow_gather(tokens, relative)
    grad_rows = narrow_gather(cotangent, relative)

    pad_hd = ((0, d_local - hd_local),)
    gain_block = jnp.pad(
        jnp.stack(
            [attn_gain, mlp_gain, jnp.pad(query_gain, pad_hd), jnp.pad(key_gain, pad_hd)], axis=1
        ),
        ((0, 0), (0, 124)),
    )
    qkv_w, out_wt, gains_all = wide_gather(
        [jnp.concatenate([w_query, w_key, w_value], axis=1), w_out.T, gain_block]
    )
    gain_attn = gains_all[:, 0].astype(jnp.float32)
    gain_mlp = gains_all[:, 1].astype(jnp.float32)
    gains_split = gains_all.reshape(wide_size, d_local, 128)
    gain_query = gains_split[:, :hd_local, 2].reshape(-1).astype(jnp.float32)
    gain_key = gains_split[:, :hd_local, 3].reshape(-1).astype(jnp.float32)
    down_t = w_down.T
    mlp_sets = []
    for h in range(2):
        cols = slice(ff_starts[h], ff_starts[h] + ff_parts[h])
        mlp_sets.append(
            wide_gather([jnp.concatenate([w_gate[:, cols], w_up[:, cols]], axis=1), down_t[:, cols]])
        )

    if relative:
        order = relative_rows(jnp.arange(rows_group, dtype=jnp.int32))
        doc_row = relative_rows(doc_ids[0])
        position = relative_rows(doc_positions(doc_ids)[0])
    else:
        order = jnp.arange(rows_group, dtype=jnp.int32)
        doc_row = doc_ids.reshape(-1)
        position = doc_positions(doc_ids).reshape(-1)
    cosine, sine = rope_from_positions(position)
    cos_heads = cosine[:, None, :]
    sin_heads = sine[:, None, :]
    allowed = (order[None, :] <= order[:, None]) & (doc_row[None, :] == doc_row[:, None])
    if not relative:
        seq_of = jnp.arange(rows_group, dtype=jnp.int32) // length
        allowed = allowed & (seq_of[None, :] == seq_of[:, None])

    inputs = tokens.astype(jnp.float32)
    normed_all = rms_apply(tokens_all.astype(jnp.float32), gain_attn).astype(jnp.bfloat16)
    qkv = jnp.dot(normed_all, qkv_w, preferred_element_type=jnp.float32)
    q_pre = qkv[:, :q_cols].reshape(rows_group, heads_here, HD)
    k_pre = qkv[:, q_cols : q_cols + kv_cols].reshape(rows_group, groups_here, HD)
    v_use = qkv[:, q_cols + kv_cols :].astype(jnp.bfloat16).reshape(rows_group, groups_here, HD)
    q_norm = rms_apply(q_pre, gain_query)
    k_norm = rms_apply(k_pre, gain_key)
    q_use = (q_norm * cos_heads + rotate(q_norm) * sin_heads).astype(jnp.bfloat16)
    k_use = (k_norm * cos_heads + rotate(k_norm) * sin_heads).astype(jnp.bfloat16)
    q_grouped = q_use.reshape(rows_group, groups_here, repeat, HD)

    scores = jnp.einsum("qgrd,kgd->grqk", q_grouped, k_use, preferred_element_type=jnp.float32) * scale
    scores = jnp.where(allowed, scores, NEG_FILL)
    top = jnp.max(scores, axis=-1, keepdims=True)
    weights = jnp.exp(scores - top)
    total = jnp.sum(weights, axis=-1, keepdims=True)
    probs = weights / total
    mixed = jnp.einsum(
        "grqk,kgd->qgrd", probs.astype(jnp.bfloat16), v_use, preferred_element_type=jnp.float32
    )
    log_totals = (top + jnp.log(total))[..., 0]
    attended = mixed.astype(jnp.bfloat16).reshape(rows_group, heads_here * HD)

    resid = inputs + narrow_scatter(times_transposed(attended, out_wt), relative)
    mlp_in = rms_apply(resid, gain_mlp).astype(jnp.bfloat16)
    mlp_all = narrow_gather(mlp_in, relative)

    down_partial = None
    d_mlp_partial = None
    mlp_grads = []
    for h in range(2):
        gate_up_w, down_wt = mlp_sets[h]
        gate_up = jnp.dot(mlp_all, gate_up_w, preferred_element_type=jnp.float32)
        gate = gate_up[:, : ff_parts[h]]
        up = gate_up[:, ff_parts[h] :]
        sigmoid = jax.nn.sigmoid(gate)
        hidden = (gate * sigmoid * up).astype(jnp.bfloat16)
        part = times_transposed(hidden, down_wt)
        down_partial = part if down_partial is None else down_partial + part
        d_hidden = jnp.dot(grad_rows, down_wt, preferred_element_type=jnp.float32)
        d_up = (d_hidden * gate * sigmoid).astype(jnp.bfloat16)
        d_gate = (d_hidden * up * sigmoid * (1.0 + gate * (1.0 - sigmoid))).astype(jnp.bfloat16)
        d_gate_up = jnp.concatenate([d_gate, d_up], axis=1)
        part = times_transposed(d_gate_up, gate_up_w)
        d_mlp_partial = part if d_mlp_partial is None else d_mlp_partial + part
        g_down_t = contract_rows(grad_rows, hidden)
        g_gate_up = contract_rows(mlp_all, d_gate_up)
        joined = jnp.concatenate(
            [g_gate_up.astype(jnp.bfloat16), g_down_t.astype(jnp.bfloat16)], axis=1
        )
        if h == 0:
            joined, mlp_sets[1] = lax.optimization_barrier((joined, mlp_sets[1]))
            mlp_grads.append(lax.psum_scatter(joined, "wide", scatter_dimension=0, tiled=True))
        else:
            last_joined = joined

    d_mlp_in = narrow_scatter(d_mlp_partial, relative)
    d_part, mlp_gain_terms = rms_back(resid, gain_mlp, d_mlp_in)
    grad_mlp_gain = jnp.sum(mlp_gain_terms, axis=0)
    d_resid = cotangent.astype(jnp.float32) + d_part
    p_scores = (
        jnp.einsum("qgrd,kgd->grqk", q_grouped, k_use, preferred_element_type=jnp.float32) * scale
    )
    p_probs = jnp.where(allowed, jnp.exp(p_scores - log_totals[..., None]), 0.0)
    d_resid_low, last_joined = lax.optimization_barrier((d_resid.astype(jnp.bfloat16), last_joined))
    mlp_grads.append(lax.psum_scatter(last_joined, "wide", scatter_dimension=0, tiled=True))
    branch_rows = narrow_gather(d_resid_low, relative)
    out_grad = contract_rows(branch_rows, attended).astype(jnp.bfloat16)
    d_attended = jnp.dot(branch_rows, out_wt, preferred_element_type=jnp.float32).astype(jnp.bfloat16)
    d_mixed = d_attended.reshape(rows_group, groups_here, repeat, HD)
    d_value = jnp.einsum(
        "grqk,qgrd->kgd", p_probs.astype(jnp.bfloat16), d_mixed, preferred_element_type=jnp.float32
    ).astype(jnp.bfloat16)
    value_grad = contract_rows(normed_all, d_value.reshape(rows_group, groups_here * HD))
    out_grad = jnp.concatenate([out_grad, value_grad.astype(jnp.bfloat16)], axis=1)
    mlp_grads, out_grad = lax.optimization_barrier((mlp_grads, out_grad))
    mlp_grads = [
        split_cols(g.astype(jnp.float32), [2 * ff_parts[h], ff_parts[h]]) for h, g in enumerate(mlp_grads)
    ]
    g_out_t, g_value = split_cols(
        lax.psum_scatter(out_grad, "wide", scatter_dimension=0, tiled=True).astype(jnp.float32),
        [q_cols, kv_cols],
    )

    d_probs = jnp.einsum("qgrd,kgd->grqk", d_mixed, v_use, preferred_element_type=jnp.float32)
    inner = jnp.sum(p_probs * d_probs, axis=-1, keepdims=True)
    d_scores = (p_probs * (d_probs - inner)).astype(jnp.bfloat16)
    d_query = jnp.einsum("grqk,kgd->qgrd", d_scores, k_use, preferred_element_type=jnp.float32) * scale
    d_key = jnp.einsum("grqk,qgrd->kgd", d_scores, q_grouped, preferred_element_type=jnp.float32) * scale

    d_query = d_query.reshape(rows_group, heads_here, HD)
    d_q_norm = d_query * cos_heads + rotate_back(d_query * sin_heads)
    d_k_norm = d_key * cos_heads + rotate_back(d_key * sin_heads)
    d_q_pre, query_terms = rms_back(q_pre, gain_query, d_q_norm)
    d_k_pre, key_terms = rms_back(k_pre, gain_key, d_k_norm)
    grad_query_gain = jnp.sum(query_terms, axis=(0, 1))
    grad_key_gain = jnp.sum(key_terms, axis=(0, 1))
    d_qkv = jnp.concatenate(
        [
            d_q_pre.astype(jnp.bfloat16).reshape(rows_group, heads_here * HD),
            d_k_pre.astype(jnp.bfloat16).reshape(rows_group, groups_here * HD),
            d_value.reshape(rows_group, groups_here * HD),
        ],
        axis=1,
    )
    d_normed_partial = times_transposed(d_qkv, qkv_w)
    tokens_all_f = tokens_all.astype(jnp.float32)
    scale_all = lax.rsqrt(jnp.mean(tokens_all_f * tokens_all_f, axis=-1, keepdims=True) + EPS)
    attn_gain_part = jnp.sum(d_normed_partial * tokens_all_f * scale_all, axis=0)
    gain_parts = narrow_allreduce(
        jnp.concatenate([attn_gain_part, grad_mlp_gain, grad_query_gain, grad_key_gain])
    )
    d_full = d_local * wide_size
    hd_full = hd_local * wide_size

    def by_chunk(vec, size):
        return jnp.pad(vec.reshape(wide_size, size), ((0, 0), (0, d_local - size)))

    gain_block = jnp.stack(
        [
            by_chunk(gain_parts[:d_full], d_local),
            by_chunk(gain_parts[d_full : 2 * d_full], d_local),
            by_chunk(gain_parts[2 * d_full : 2 * d_full + hd_full], hd_local),
            by_chunk(gain_parts[2 * d_full + hd_full :], hd_local),
        ],
        axis=-1,
    ).reshape(d_full, 4)
    gain_block = jnp.pad(gain_block, ((0, 0), (0, 124)))
    qk_cols = q_cols + kv_cols
    qkv_grad = jnp.concatenate(
        [
            contract_rows(normed_all, d_qkv[:, :qk_cols]).astype(jnp.bfloat16),
            gain_block.astype(jnp.bfloat16),
        ],
        axis=1,
    )
    g_out_t, qkv_grad = lax.optimization_barrier((g_out_t, qkv_grad))
    g_qkv, g_gains = split_cols(
        lax.psum_scatter(qkv_grad, "wide", scatter_dimension=0, tiled=True).astype(jnp.float32),
        [qk_cols, 128],
    )
    d_normed = narrow_scatter(d_normed_partial, relative)
    d_input_part, _ = rms_back(inputs, gain_attn, d_normed)
    d_tokens = d_resid + d_input_part
    attn_gain_grad = g_gains[:, 0]
    mlp_gain_grad = g_gains[:, 1]
    query_gain_grad = g_gains[:hd_local, 2]
    key_gain_grad = g_gains[:hd_local, 3]

    g_query = g_qkv[:, :q_cols]
    g_key = g_qkv[:, q_cols : q_cols + kv_cols]
    g_gate = jnp.concatenate([mlp_grads[h][0][:, : ff_parts[h]] for h in range(2)], axis=1)
    g_up = jnp.concatenate([mlp_grads[h][0][:, ff_parts[h] :] for h in range(2)], axis=1)
    g_down = jnp.concatenate([mlp_grads[h][1] for h in range(2)], axis=1).T
    output = (resid + narrow_scatter(down_partial, relative)).astype(jnp.bfloat16)
    return (
        output,
        d_tokens,
        attn_gain_grad,
        g_query,
        g_key,
        g_value,
        query_gain_grad,
        key_gain_grad,
        g_out_t.T,
        mlp_gain_grad,
        g_gate,
        g_up,
        g_down,
    )


def solution(mesh):
    in_specs = (
        P(("wide", "narrow"), None),
        P("wide", None),
        P(("wide", "narrow"), None),
        P("wide"),
        P("wide", "narrow"),
        P("wide", "narrow"),
        P("wide", "narrow"),
        P("wide"),
        P("wide"),
        P("narrow", "wide"),
        P("wide"),
        P("wide", "narrow"),
        P("wide", "narrow"),
        P("narrow", "wide"),
    )
    out_specs = (
        P(("wide", "narrow"), None),
        P(("wide", "narrow"), None),
        P("wide"),
        P("wide", "narrow"),
        P("wide", "narrow"),
        P("wide", "narrow"),
        P("wide"),
        P("wide"),
        P("narrow", "wide"),
        P("wide"),
        P("wide", "narrow"),
        P("wide", "narrow"),
        P("narrow", "wide"),
    )
    return jax.shard_map(shards_body, mesh=mesh, in_specs=in_specs, out_specs=out_specs, check_vma=False)
```

```python
import jax
import jax.numpy as jnp
from jax import lax
from jax.sharding import PartitionSpec as P


H = 16
KV = 8
HD = 128


EPS = 1e-06
ROPE_BASE = 1000000.0
NEG_FILL = -1e30

XPERM = [(0, 1), (1, 0), (2, 3), (3, 2)]
YPERM = [(0, 2), (2, 0), (1, 3), (3, 1)]
BLOCK_XOR = (0, 1, 2, 3, 0, 2, 1, 3)


def rms_apply(values, gain):
    return values * lax.rsqrt(jnp.mean(values * values, axis=-1, keepdims=True) + EPS) * gain


def rms_back(values, gain, grad):
    scale = lax.rsqrt(jnp.mean(values * values, axis=-1, keepdims=True) + EPS)
    weighted = grad * gain
    inner = jnp.mean(weighted * values, axis=-1, keepdims=True)
    d_values = scale * weighted - values * (scale * scale * scale) * inner
    return (d_values, grad * values * scale)


def rotate(values):
    half = values.shape[-1] // 2
    return jnp.concatenate([-values[..., half:], values[..., :half]], axis=-1)


def rotate_back(values):
    half = values.shape[-1] // 2
    return jnp.concatenate([values[..., half:], -values[..., :half]], axis=-1)


def doc_positions(doc_rows):
    index = lax.broadcasted_iota(jnp.int32, doc_rows.shape, 1)
    change = jnp.concatenate(
        [jnp.ones((doc_rows.shape[0], 1), jnp.bool_), doc_rows[:, 1:] != doc_rows[:, :-1]], axis=1
    )
    begin = lax.cummax(jnp.where(change, index, 0), axis=1)
    return index - begin


def rope_from_positions(position):
    freqs = ROPE_BASE ** (-(jnp.arange(HD // 2, dtype=jnp.float32) * (2.0 / HD)))
    angle = position.astype(jnp.float32)[..., None] * freqs
    cosine = jnp.cos(angle)
    sine = jnp.sin(angle)
    return (jnp.concatenate([cosine, cosine], axis=-1), jnp.concatenate([sine, sine], axis=-1))


def contract_rows(left, right):
    return lax.dot_general(
        left, right, (((0,), (0,)), ((), ())), preferred_element_type=jnp.float32
    )


def times_transposed(left, right):
    return lax.dot_general(
        left, right, (((1,), (1,)), ((), ())), preferred_element_type=jnp.float32
    )


def relative_ok(seq_count):
    return lax.axis_size("narrow") == 4 and seq_count == 1


def relative_rows(vec):
    n = lax.axis_index("narrow")
    half = vec.shape[0] // 8
    split = vec.reshape(4, 2, half)
    pieces = []
    for blk, flip in enumerate(BLOCK_XOR):
        source = split[:, 1 if blk >= 4 else 0]
        pieces.append(lax.dynamic_index_in_dim(source, jnp.bitwise_xor(n, flip), 0, keepdims=False))
    return jnp.concatenate(pieces)


def narrow_allreduce(v):
    if lax.axis_size("narrow") != 4:
        return lax.psum(v, "narrow")
    v = v + lax.ppermute(v, "narrow", XPERM)
    return v + lax.ppermute(v, "narrow", YPERM)


def narrow_gather(x, relative):
    if not relative:
        return lax.all_gather(x, "narrow", axis=0, tiled=True)
    half = x.shape[0] // 2
    a, b = x[:half], x[half:]
    a_x = lax.ppermute(a, "narrow", XPERM)
    b_y = lax.ppermute(b, "narrow", YPERM)
    a_pair = jnp.concatenate([a, a_x], axis=0)
    b_pair = jnp.concatenate([b, b_y], axis=0)
    a_pair_y = lax.ppermute(a_pair, "narrow", YPERM)
    b_pair_x = lax.ppermute(b_pair, "narrow", XPERM)
    return jnp.concatenate([a_pair, a_pair_y, b_pair, b_pair_x], axis=0)


def narrow_scatter(x, relative):
    if not relative:
        return lax.psum_scatter(
            x.astype(jnp.bfloat16), "narrow", scatter_dimension=0, tiled=True
        ).astype(jnp.float32)
    rows, c = x.shape
    half = rows // 8
    blocks = x.reshape(8, half, c)
    a_got = lax.ppermute(blocks[2:4].astype(jnp.bfloat16), "narrow", YPERM)
    b_got = lax.ppermute(blocks[6:8].astype(jnp.bfloat16), "narrow", XPERM)
    a_sum = blocks[0:2] + a_got.astype(jnp.float32)
    b_sum = blocks[4:6] + b_got.astype(jnp.float32)
    a_got2 = lax.ppermute(a_sum[1].astype(jnp.bfloat16), "narrow", XPERM)
    b_got2 = lax.ppermute(b_sum[1].astype(jnp.bfloat16), "narrow", YPERM)
    return jnp.concatenate(
        [a_sum[0] + a_got2.astype(jnp.float32), b_sum[0] + b_got2.astype(jnp.float32)], axis=0
    )


def split_cols(joined, widths):
    out = []
    start = 0
    for w in widths:
        out.append(joined[:, start : start + w])
        start += w
    return out


def wide_gather(blocks):
    joined = lax.all_gather(jnp.concatenate(blocks, axis=1), "wide", axis=0, tiled=True)
    return split_cols(joined, [blk.shape[1] for blk in blocks])


def shards_body(
    tokens,
    doc_ids,
    cotangent,
    attn_gain,
    w_query,
    w_key,
    w_value,
    query_gain,
    key_gain,
    w_out,
    mlp_gain,
    w_gate,
    w_up,
    w_down,
):
    narrow_size = lax.axis_size("narrow")
    wide_size = lax.axis_size("wide")
    heads_here = H // narrow_size
    groups_here = KV // narrow_size
    repeat = H // KV
    seq_count, length = doc_ids.shape
    rows_group = seq_count * length
    scale = HD ** (-0.5)
    d_local = attn_gain.shape[0]
    hd_local = query_gain.shape[0]
    q_cols = w_query.shape[1]
    kv_cols = w_key.shape[1]
    ff_cols = w_gate.shape[1]
    ff_half = ff_cols // 2
    relative = relative_ok(seq_count)

    tokens_all = narrow_gather(tokens, relative)
    grad_rows = narrow_gather(cotangent, relative)

    pad_hd = ((0, d_local - hd_local),)
    gain_block = jnp.pad(
        jnp.stack(
            [attn_gain, mlp_gain, jnp.pad(query_gain, pad_hd), jnp.pad(key_gain, pad_hd)], axis=1
        ),
        ((0, 0), (0, 124)),
    )
    qkv_w, out_wt, gains_all = wide_gather(
        [jnp.concatenate([w_query, w_key, w_value], axis=1), w_out.T, gain_block]
    )
    gain_attn = gains_all[:, 0].astype(jnp.float32)
    gain_mlp = gains_all[:, 1].astype(jnp.float32)
    gains_split = gains_all.reshape(wide_size, d_local, 128)
    gain_query = gains_split[:, :hd_local, 2].reshape(-1).astype(jnp.float32)
    gain_key = gains_split[:, :hd_local, 3].reshape(-1).astype(jnp.float32)
    down_t = w_down.T
    mlp_sets = []
    for h in range(2):
        cols = slice(h * ff_half, (h + 1) * ff_half)
        mlp_sets.append(
            wide_gather([jnp.concatenate([w_gate[:, cols], w_up[:, cols]], axis=1), down_t[:, cols]])
        )

    if relative:
        order = relative_rows(jnp.arange(rows_group, dtype=jnp.int32))
        doc_row = relative_rows(doc_ids[0])
        position = relative_rows(doc_positions(doc_ids)[0])
    else:
        order = jnp.arange(rows_group, dtype=jnp.int32)
        doc_row = doc_ids.reshape(-1)
        position = doc_positions(doc_ids).reshape(-1)
    cosine, sine = rope_from_positions(position)
    cos_heads = cosine[:, None, :]
    sin_heads = sine[:, None, :]
    allowed = (order[None, :] <= order[:, None]) & (doc_row[None, :] == doc_row[:, None])
    if not relative:
        seq_of = jnp.arange(rows_group, dtype=jnp.int32) // length
        allowed = allowed & (seq_of[None, :] == seq_of[:, None])

    inputs = tokens.astype(jnp.float32)
    normed_all = rms_apply(tokens_all.astype(jnp.float32), gain_attn).astype(jnp.bfloat16)
    qkv = jnp.dot(normed_all, qkv_w, preferred_element_type=jnp.float32)
    q_pre = qkv[:, :q_cols].reshape(rows_group, heads_here, HD)
    k_pre = qkv[:, q_cols : q_cols + kv_cols].reshape(rows_group, groups_here, HD)
    v_use = qkv[:, q_cols + kv_cols :].astype(jnp.bfloat16).reshape(rows_group, groups_here, HD)
    q_norm = rms_apply(q_pre, gain_query)
    k_norm = rms_apply(k_pre, gain_key)
    q_use = (q_norm * cos_heads + rotate(q_norm) * sin_heads).astype(jnp.bfloat16)
    k_use = (k_norm * cos_heads + rotate(k_norm) * sin_heads).astype(jnp.bfloat16)
    q_grouped = q_use.reshape(rows_group, groups_here, repeat, HD)

    scores = jnp.einsum("qgrd,kgd->grqk", q_grouped, k_use, preferred_element_type=jnp.float32) * scale
    scores = jnp.where(allowed, scores, NEG_FILL)
    top = jnp.max(scores, axis=-1, keepdims=True)
    weights = jnp.exp(scores - top)
    total = jnp.sum(weights, axis=-1, keepdims=True)
    probs = weights / total
    mixed = jnp.einsum(
        "grqk,kgd->qgrd", probs.astype(jnp.bfloat16), v_use, preferred_element_type=jnp.float32
    )
    log_totals = (top + jnp.log(total))[..., 0]
    attended = mixed.astype(jnp.bfloat16).reshape(rows_group, heads_here * HD)

    resid = inputs + narrow_scatter(times_transposed(attended, out_wt), relative)
    mlp_in = rms_apply(resid, gain_mlp).astype(jnp.bfloat16)
    mlp_all = narrow_gather(mlp_in, relative)

    down_partial = None
    d_mlp_partial = None
    mlp_grads = []
    for h in range(2):
        gate_up_w, down_wt = mlp_sets[h]
        gate_up = jnp.dot(mlp_all, gate_up_w, preferred_element_type=jnp.float32)
        gate = gate_up[:, :ff_half]
        up = gate_up[:, ff_half:]
        sigmoid = jax.nn.sigmoid(gate)
        hidden = (gate * sigmoid * up).astype(jnp.bfloat16)
        part = times_transposed(hidden, down_wt)
        down_partial = part if down_partial is None else down_partial + part
        d_hidden = jnp.dot(grad_rows, down_wt, preferred_element_type=jnp.float32)
        d_up = (d_hidden * gate * sigmoid).astype(jnp.bfloat16)
        d_gate = (d_hidden * up * sigmoid * (1.0 + gate * (1.0 - sigmoid))).astype(jnp.bfloat16)
        d_gate_up = jnp.concatenate([d_gate, d_up], axis=1)
        part = times_transposed(d_gate_up, gate_up_w)
        d_mlp_partial = part if d_mlp_partial is None else d_mlp_partial + part
        g_down_t = contract_rows(grad_rows, hidden)
        g_gate_up = contract_rows(mlp_all, d_gate_up)
        joined = jnp.concatenate(
            [g_gate_up.astype(jnp.bfloat16), g_down_t.astype(jnp.bfloat16)], axis=1
        )
        if h == 0:
            joined, mlp_sets[1] = lax.optimization_barrier((joined, mlp_sets[1]))
            mlp_grads.append(lax.psum_scatter(joined, "wide", scatter_dimension=0, tiled=True))
        else:
            last_joined = joined

    d_mlp_in = narrow_scatter(d_mlp_partial, relative)
    d_part, mlp_gain_terms = rms_back(resid, gain_mlp, d_mlp_in)
    grad_mlp_gain = jnp.sum(mlp_gain_terms, axis=0)
    d_resid = cotangent.astype(jnp.float32) + d_part
    p_scores = (
        jnp.einsum("qgrd,kgd->grqk", q_grouped, k_use, preferred_element_type=jnp.float32) * scale
    )
    p_probs = jnp.where(allowed, jnp.exp(p_scores - log_totals[..., None]), 0.0)
    d_resid_low = d_resid.astype(jnp.bfloat16)
    mlp_grads.append(lax.psum_scatter(last_joined, "wide", scatter_dimension=0, tiled=True))
    branch_rows = narrow_gather(d_resid_low, relative)
    out_grad = contract_rows(branch_rows, attended).astype(jnp.bfloat16)
    d_attended = jnp.dot(branch_rows, out_wt, preferred_element_type=jnp.float32).astype(jnp.bfloat16)
    d_mixed = d_attended.reshape(rows_group, groups_here, repeat, HD)
    d_value = jnp.einsum(
        "grqk,qgrd->kgd", p_probs.astype(jnp.bfloat16), d_mixed, preferred_element_type=jnp.float32
    ).astype(jnp.bfloat16)
    value_grad = contract_rows(normed_all, d_value.reshape(rows_group, groups_here * HD))
    out_grad = jnp.concatenate([out_grad, value_grad.astype(jnp.bfloat16)], axis=1)
    mlp_grads, out_grad = lax.optimization_barrier((mlp_grads, out_grad))
    mlp_grads = [split_cols(g.astype(jnp.float32), [2 * ff_half, ff_half]) for g in mlp_grads]
    g_out_t, g_value = split_cols(
        lax.psum_scatter(out_grad, "wide", scatter_dimension=0, tiled=True).astype(jnp.float32),
        [q_cols, kv_cols],
    )

    d_probs = jnp.einsum("qgrd,kgd->grqk", d_mixed, v_use, preferred_element_type=jnp.float32)
    inner = jnp.sum(p_probs * d_probs, axis=-1, keepdims=True)
    d_scores = (p_probs * (d_probs - inner)).astype(jnp.bfloat16)
    d_query = jnp.einsum("grqk,kgd->qgrd", d_scores, k_use, preferred_element_type=jnp.float32) * scale
    d_key = jnp.einsum("grqk,qgrd->kgd", d_scores, q_grouped, preferred_element_type=jnp.float32) * scale

    d_query = d_query.reshape(rows_group, heads_here, HD)
    d_q_norm = d_query * cos_heads + rotate_back(d_query * sin_heads)
    d_k_norm = d_key * cos_heads + rotate_back(d_key * sin_heads)
    d_q_pre, query_terms = rms_back(q_pre, gain_query, d_q_norm)
    d_k_pre, key_terms = rms_back(k_pre, gain_key, d_k_norm)
    grad_query_gain = jnp.sum(query_terms, axis=(0, 1))
    grad_key_gain = jnp.sum(key_terms, axis=(0, 1))
    d_qkv = jnp.concatenate(
        [
            d_q_pre.astype(jnp.bfloat16).reshape(rows_group, heads_here * HD),
            d_k_pre.astype(jnp.bfloat16).reshape(rows_group, groups_here * HD),
            d_value.reshape(rows_group, groups_here * HD),
        ],
        axis=1,
    )
    d_normed_partial = times_transposed(d_qkv, qkv_w)
    tokens_all_f = tokens_all.astype(jnp.float32)
    scale_all = lax.rsqrt(jnp.mean(tokens_all_f * tokens_all_f, axis=-1, keepdims=True) + EPS)
    attn_gain_part = jnp.sum(d_normed_partial * tokens_all_f * scale_all, axis=0)
    gain_parts = narrow_allreduce(
        jnp.concatenate([attn_gain_part, grad_mlp_gain, grad_query_gain, grad_key_gain])
    )
    d_full = d_local * wide_size
    hd_full = hd_local * wide_size

    def by_chunk(vec, size):
        return jnp.pad(vec.reshape(wide_size, size), ((0, 0), (0, d_local - size)))

    gain_block = jnp.stack(
        [
            by_chunk(gain_parts[:d_full], d_local),
            by_chunk(gain_parts[d_full : 2 * d_full], d_local),
            by_chunk(gain_parts[2 * d_full : 2 * d_full + hd_full], hd_local),
            by_chunk(gain_parts[2 * d_full + hd_full :], hd_local),
        ],
        axis=-1,
    ).reshape(d_full, 4)
    gain_block = jnp.pad(gain_block, ((0, 0), (0, 124)))
    qk_cols = q_cols + kv_cols
    qkv_grad = jnp.concatenate(
        [
            contract_rows(normed_all, d_qkv[:, :qk_cols]).astype(jnp.bfloat16),
            gain_block.astype(jnp.bfloat16),
        ],
        axis=1,
    )
    g_out_t, qkv_grad = lax.optimization_barrier((g_out_t, qkv_grad))
    g_qkv, g_gains = split_cols(
        lax.psum_scatter(qkv_grad, "wide", scatter_dimension=0, tiled=True).astype(jnp.float32),
        [qk_cols, 128],
    )
    d_normed = narrow_scatter(d_normed_partial, relative)
    d_input_part, _ = rms_back(inputs, gain_attn, d_normed)
    d_tokens = d_resid + d_input_part
    attn_gain_grad = g_gains[:, 0]
    mlp_gain_grad = g_gains[:, 1]
    query_gain_grad = g_gains[:hd_local, 2]
    key_gain_grad = g_gains[:hd_local, 3]

    g_query = g_qkv[:, :q_cols]
    g_key = g_qkv[:, q_cols : q_cols + kv_cols]
    g_gate = jnp.concatenate([mlp_grads[h][0][:, :ff_half] for h in range(2)], axis=1)
    g_up = jnp.concatenate([mlp_grads[h][0][:, ff_half:] for h in range(2)], axis=1)
    g_down = jnp.concatenate([mlp_grads[h][1] for h in range(2)], axis=1).T
    output = (resid + narrow_scatter(down_partial, relative)).astype(jnp.bfloat16)
    return (
        output,
        d_tokens,
        attn_gain_grad,
        g_query,
        g_key,
        g_value,
        query_gain_grad,
        key_gain_grad,
        g_out_t.T,
        mlp_gain_grad,
        g_gate,
        g_up,
        g_down,
    )


def solution(mesh):
    in_specs = (
        P(("wide", "narrow"), None),
        P("wide", None),
        P(("wide", "narrow"), None),
        P("wide"),
        P("wide", "narrow"),
        P("wide", "narrow"),
        P("wide", "narrow"),
        P("wide"),
        P("wide"),
        P("narrow", "wide"),
        P("wide"),
        P("wide", "narrow"),
        P("wide", "narrow"),
        P("narrow", "wide"),
    )
    out_specs = (
        P(("wide", "narrow"), None),
        P(("wide", "narrow"), None),
        P("wide"),
        P("wide", "narrow"),
        P("wide", "narrow"),
        P("wide", "narrow"),
        P("wide"),
        P("wide"),
        P("narrow", "wide"),
        P("wide"),
        P("wide", "narrow"),
        P("wide", "narrow"),
        P("narrow", "wide"),
    )
    return jax.shard_map(shards_body, mesh=mesh, in_specs=in_specs, out_specs=out_specs, check_vma=False)
```

```python
import jax
import jax.numpy as jnp
from jax import lax
from jax.sharding import PartitionSpec as P


H = 16
KV = 8
HD = 128


EPS = 1e-06
ROPE_BASE = 1000000.0
NEG_FILL = -1e30

XPERM = [(0, 1), (1, 0), (2, 3), (3, 2)]
YPERM = [(0, 2), (2, 0), (1, 3), (3, 1)]
BLOCK_XOR = (0, 1, 2, 3, 0, 2, 1, 3)


def rms_apply(values, gain):
    return values * lax.rsqrt(jnp.mean(values * values, axis=-1, keepdims=True) + EPS) * gain


def rms_back(values, gain, grad):
    scale = lax.rsqrt(jnp.mean(values * values, axis=-1, keepdims=True) + EPS)
    weighted = grad * gain
    inner = jnp.mean(weighted * values, axis=-1, keepdims=True)
    d_values = scale * weighted - values * (scale * scale * scale) * inner
    return (d_values, grad * values * scale)


def rotate(values):
    half = values.shape[-1] // 2
    return jnp.concatenate([-values[..., half:], values[..., :half]], axis=-1)


def rotate_back(values):
    half = values.shape[-1] // 2
    return jnp.concatenate([values[..., half:], -values[..., :half]], axis=-1)


def doc_positions(doc_rows):
    index = lax.broadcasted_iota(jnp.int32, doc_rows.shape, 1)
    change = jnp.concatenate(
        [jnp.ones((doc_rows.shape[0], 1), jnp.bool_), doc_rows[:, 1:] != doc_rows[:, :-1]], axis=1
    )
    begin = lax.cummax(jnp.where(change, index, 0), axis=1)
    return index - begin


def rope_from_positions(position):
    freqs = ROPE_BASE ** (-(jnp.arange(HD // 2, dtype=jnp.float32) * (2.0 / HD)))
    angle = position.astype(jnp.float32)[..., None] * freqs
    cosine = jnp.cos(angle)
    sine = jnp.sin(angle)
    return (jnp.concatenate([cosine, cosine], axis=-1), jnp.concatenate([sine, sine], axis=-1))


def contract_rows(left, right):
    return lax.dot_general(
        left, right, (((0,), (0,)), ((), ())), preferred_element_type=jnp.float32
    )


def times_transposed(left, right):
    return lax.dot_general(
        left, right, (((1,), (1,)), ((), ())), preferred_element_type=jnp.float32
    )


def relative_ok(seq_count):
    return lax.axis_size("narrow") == 4 and seq_count == 1


def relative_rows(vec):
    n = lax.axis_index("narrow")
    half = vec.shape[0] // 8
    split = vec.reshape(4, 2, half)
    pieces = []
    for blk, flip in enumerate(BLOCK_XOR):
        source = split[:, 1 if blk >= 4 else 0]
        pieces.append(lax.dynamic_index_in_dim(source, jnp.bitwise_xor(n, flip), 0, keepdims=False))
    return jnp.concatenate(pieces)


def narrow_allreduce(v):
    if lax.axis_size("narrow") != 4:
        return lax.psum(v, "narrow")
    v = v + lax.ppermute(v, "narrow", XPERM)
    return v + lax.ppermute(v, "narrow", YPERM)


def narrow_gather(x, relative):
    if not relative:
        return lax.all_gather(x, "narrow", axis=0, tiled=True)
    half = x.shape[0] // 2
    a, b = x[:half], x[half:]
    a_x = lax.ppermute(a, "narrow", XPERM)
    b_y = lax.ppermute(b, "narrow", YPERM)
    a_pair = jnp.concatenate([a, a_x], axis=0)
    b_pair = jnp.concatenate([b, b_y], axis=0)
    a_pair_y = lax.ppermute(a_pair, "narrow", YPERM)
    b_pair_x = lax.ppermute(b_pair, "narrow", XPERM)
    return jnp.concatenate([a_pair, a_pair_y, b_pair, b_pair_x], axis=0)


def narrow_scatter(x, relative):
    if not relative:
        return lax.psum_scatter(
            x.astype(jnp.bfloat16), "narrow", scatter_dimension=0, tiled=True
        ).astype(jnp.float32)
    rows, c = x.shape
    half = rows // 8
    blocks = x.reshape(8, half, c)
    a_got = lax.ppermute(blocks[2:4].astype(jnp.bfloat16), "narrow", YPERM)
    b_got = lax.ppermute(blocks[6:8].astype(jnp.bfloat16), "narrow", XPERM)
    a_sum = blocks[0:2] + a_got.astype(jnp.float32)
    b_sum = blocks[4:6] + b_got.astype(jnp.float32)
    a_got2 = lax.ppermute(a_sum[1].astype(jnp.bfloat16), "narrow", XPERM)
    b_got2 = lax.ppermute(b_sum[1].astype(jnp.bfloat16), "narrow", YPERM)
    return jnp.concatenate(
        [a_sum[0] + a_got2.astype(jnp.float32), b_sum[0] + b_got2.astype(jnp.float32)], axis=0
    )


def split_cols(joined, widths):
    out = []
    start = 0
    for w in widths:
        out.append(joined[:, start : start + w])
        start += w
    return out


def wide_gather(blocks):
    joined = lax.all_gather(jnp.concatenate(blocks, axis=1), "wide", axis=0, tiled=True)
    return split_cols(joined, [blk.shape[1] for blk in blocks])


def shards_body(
    tokens,
    doc_ids,
    cotangent,
    attn_gain,
    w_query,
    w_key,
    w_value,
    query_gain,
    key_gain,
    w_out,
    mlp_gain,
    w_gate,
    w_up,
    w_down,
):
    narrow_size = lax.axis_size("narrow")
    wide_size = lax.axis_size("wide")
    heads_here = H // narrow_size
    groups_here = KV // narrow_size
    repeat = H // KV
    seq_count, length = doc_ids.shape
    rows_group = seq_count * length
    scale = HD ** (-0.5)
    d_local = attn_gain.shape[0]
    hd_local = query_gain.shape[0]
    q_cols = w_query.shape[1]
    kv_cols = w_key.shape[1]
    ff_cols = w_gate.shape[1]
    ff_half = ff_cols // 2
    relative = relative_ok(seq_count)

    tokens_all = narrow_gather(tokens, relative)
    grad_rows = narrow_gather(cotangent, relative)

    pad_hd = ((0, d_local - hd_local),)
    gain_block = jnp.pad(
        jnp.stack(
            [attn_gain, mlp_gain, jnp.pad(query_gain, pad_hd), jnp.pad(key_gain, pad_hd)], axis=1
        ),
        ((0, 0), (0, 124)),
    )
    qkv_w, out_wt, gains_all = wide_gather(
        [jnp.concatenate([w_query, w_key, w_value], axis=1), w_out.T, gain_block]
    )
    gain_attn = gains_all[:, 0].astype(jnp.float32)
    gain_mlp = gains_all[:, 1].astype(jnp.float32)
    gains_split = gains_all.reshape(wide_size, d_local, 128)
    gain_query = gains_split[:, :hd_local, 2].reshape(-1).astype(jnp.float32)
    gain_key = gains_split[:, :hd_local, 3].reshape(-1).astype(jnp.float32)
    down_t = w_down.T
    mlp_sets = []
    for h in range(2):
        cols = slice(h * ff_half, (h + 1) * ff_half)
        mlp_sets.append(
            wide_gather([jnp.concatenate([w_gate[:, cols], w_up[:, cols]], axis=1), down_t[:, cols]])
        )

    if relative:
        order = relative_rows(jnp.arange(rows_group, dtype=jnp.int32))
        doc_row = relative_rows(doc_ids[0])
        position = relative_rows(doc_positions(doc_ids)[0])
    else:
        order = jnp.arange(rows_group, dtype=jnp.int32)
        doc_row = doc_ids.reshape(-1)
        position = doc_positions(doc_ids).reshape(-1)
    cosine, sine = rope_from_positions(position)
    cos_heads = cosine[:, None, :]
    sin_heads = sine[:, None, :]
    allowed = (order[None, :] <= order[:, None]) & (doc_row[None, :] == doc_row[:, None])
    if not relative:
        seq_of = jnp.arange(rows_group, dtype=jnp.int32) // length
        allowed = allowed & (seq_of[None, :] == seq_of[:, None])

    inputs = tokens.astype(jnp.float32)
    normed_all = rms_apply(tokens_all.astype(jnp.float32), gain_attn).astype(jnp.bfloat16)
    qkv = jnp.dot(normed_all, qkv_w, preferred_element_type=jnp.float32)
    q_pre = qkv[:, :q_cols].reshape(rows_group, heads_here, HD)
    k_pre = qkv[:, q_cols : q_cols + kv_cols].reshape(rows_group, groups_here, HD)
    v_use = qkv[:, q_cols + kv_cols :].astype(jnp.bfloat16).reshape(rows_group, groups_here, HD)
    q_norm = rms_apply(q_pre, gain_query)
    k_norm = rms_apply(k_pre, gain_key)
    q_use = (q_norm * cos_heads + rotate(q_norm) * sin_heads).astype(jnp.bfloat16)
    k_use = (k_norm * cos_heads + rotate(k_norm) * sin_heads).astype(jnp.bfloat16)
    q_grouped = q_use.reshape(rows_group, groups_here, repeat, HD)

    scores = jnp.einsum("qgrd,kgd->grqk", q_grouped, k_use, preferred_element_type=jnp.float32) * scale
    scores = jnp.where(allowed, scores, NEG_FILL)
    top = jnp.max(scores, axis=-1, keepdims=True)
    weights = jnp.exp(scores - top)
    total = jnp.sum(weights, axis=-1, keepdims=True)
    probs = weights / total
    mixed = jnp.einsum(
        "grqk,kgd->qgrd", probs.astype(jnp.bfloat16), v_use, preferred_element_type=jnp.float32
    )
    log_totals = (top + jnp.log(total))[..., 0]
    attended = mixed.astype(jnp.bfloat16).reshape(rows_group, heads_here * HD)

    resid = inputs + narrow_scatter(times_transposed(attended, out_wt), relative)
    mlp_in = rms_apply(resid, gain_mlp).astype(jnp.bfloat16)
    mlp_all = narrow_gather(mlp_in, relative)

    down_partial = None
    d_mlp_partial = None
    mlp_grads = []
    for h in range(2):
        gate_up_w, down_wt = mlp_sets[h]
        gate_up = jnp.dot(mlp_all, gate_up_w, preferred_element_type=jnp.float32)
        gate = gate_up[:, :ff_half]
        up = gate_up[:, ff_half:]
        sigmoid = jax.nn.sigmoid(gate)
        hidden = (gate * sigmoid * up).astype(jnp.bfloat16)
        part = times_transposed(hidden, down_wt)
        down_partial = part if down_partial is None else down_partial + part
        d_hidden = jnp.dot(grad_rows, down_wt, preferred_element_type=jnp.float32)
        d_up = (d_hidden * gate * sigmoid).astype(jnp.bfloat16)
        d_gate = (d_hidden * up * sigmoid * (1.0 + gate * (1.0 - sigmoid))).astype(jnp.bfloat16)
        d_gate_up = jnp.concatenate([d_gate, d_up], axis=1)
        part = times_transposed(d_gate_up, gate_up_w)
        d_mlp_partial = part if d_mlp_partial is None else d_mlp_partial + part
        g_down_t = contract_rows(grad_rows, hidden)
        g_gate_up = contract_rows(mlp_all, d_gate_up)
        joined = jnp.concatenate(
            [g_gate_up.astype(jnp.bfloat16), g_down_t.astype(jnp.bfloat16)], axis=1
        )
        if h == 0:
            joined, mlp_sets[1] = lax.optimization_barrier((joined, mlp_sets[1]))
            mlp_grads.append(lax.psum_scatter(joined, "wide", scatter_dimension=0, tiled=True))
        else:
            last_joined = joined

    d_mlp_in = narrow_scatter(d_mlp_partial, relative)
    d_part, mlp_gain_terms = rms_back(resid, gain_mlp, d_mlp_in)
    grad_mlp_gain = jnp.sum(mlp_gain_terms, axis=0)
    d_resid = cotangent.astype(jnp.float32) + d_part
    p_scores = (
        jnp.einsum("qgrd,kgd->grqk", q_grouped, k_use, preferred_element_type=jnp.float32) * scale
    )
    p_probs = jnp.where(allowed, jnp.exp(p_scores - log_totals[..., None]), 0.0)
    d_resid_low = d_resid.astype(jnp.bfloat16)
    mlp_grads.append(lax.psum_scatter(last_joined, "wide", scatter_dimension=0, tiled=True))
    branch_rows = narrow_gather(d_resid_low, relative)
    out_grad = contract_rows(branch_rows, attended).astype(jnp.bfloat16)
    d_attended = jnp.dot(branch_rows, out_wt, preferred_element_type=jnp.float32).astype(jnp.bfloat16)
    d_mixed = d_attended.reshape(rows_group, groups_here, repeat, HD)
    d_value = jnp.einsum(
        "grqk,qgrd->kgd", p_probs.astype(jnp.bfloat16), d_mixed, preferred_element_type=jnp.float32
    ).astype(jnp.bfloat16)
    value_grad = contract_rows(normed_all, d_value.reshape(rows_group, groups_here * HD))
    out_grad = jnp.concatenate([out_grad, value_grad.astype(jnp.bfloat16)], axis=1)
    mlp_grads = [split_cols(g.astype(jnp.float32), [2 * ff_half, ff_half]) for g in mlp_grads]
    out_summed = lax.psum_scatter(out_grad, "wide", scatter_dimension=0, tiled=True)
    g_out_t, g_value = split_cols(out_summed.astype(jnp.float32), [q_cols, kv_cols])

    d_probs = jnp.einsum("qgrd,kgd->grqk", d_mixed, v_use, preferred_element_type=jnp.float32)
    inner = jnp.sum(p_probs * d_probs, axis=-1, keepdims=True)
    d_scores = (p_probs * (d_probs - inner)).astype(jnp.bfloat16)
    d_query = jnp.einsum("grqk,kgd->qgrd", d_scores, k_use, preferred_element_type=jnp.float32) * scale
    d_key = jnp.einsum("grqk,qgrd->kgd", d_scores, q_grouped, preferred_element_type=jnp.float32) * scale

    d_query = d_query.reshape(rows_group, heads_here, HD)
    d_q_norm = d_query * cos_heads + rotate_back(d_query * sin_heads)
    d_k_norm = d_key * cos_heads + rotate_back(d_key * sin_heads)
    d_q_pre, query_terms = rms_back(q_pre, gain_query, d_q_norm)
    d_k_pre, key_terms = rms_back(k_pre, gain_key, d_k_norm)
    grad_query_gain = jnp.sum(query_terms, axis=(0, 1))
    grad_key_gain = jnp.sum(key_terms, axis=(0, 1))
    d_qkv = jnp.concatenate(
        [
            d_q_pre.astype(jnp.bfloat16).reshape(rows_group, heads_here * HD),
            d_k_pre.astype(jnp.bfloat16).reshape(rows_group, groups_here * HD),
            d_value.reshape(rows_group, groups_here * HD),
        ],
        axis=1,
    )
    d_normed_partial = times_transposed(d_qkv, qkv_w)
    tokens_all_f = tokens_all.astype(jnp.float32)
    scale_all = lax.rsqrt(jnp.mean(tokens_all_f * tokens_all_f, axis=-1, keepdims=True) + EPS)
    attn_gain_part = jnp.sum(d_normed_partial * tokens_all_f * scale_all, axis=0)
    gain_parts = narrow_allreduce(
        jnp.concatenate([attn_gain_part, grad_mlp_gain, grad_query_gain, grad_key_gain])
    )
    d_full = d_local * wide_size
    hd_full = hd_local * wide_size

    def by_chunk(vec, size):
        return jnp.pad(vec.reshape(wide_size, size), ((0, 0), (0, d_local - size)))

    gain_block = jnp.stack(
        [
            by_chunk(gain_parts[:d_full], d_local),
            by_chunk(gain_parts[d_full : 2 * d_full], d_local),
            by_chunk(gain_parts[2 * d_full : 2 * d_full + hd_full], hd_local),
            by_chunk(gain_parts[2 * d_full + hd_full :], hd_local),
        ],
        axis=-1,
    ).reshape(d_full, 4)
    gain_block = jnp.pad(gain_block, ((0, 0), (0, 124)))
    qk_cols = q_cols + kv_cols
    qkv_grad = jnp.concatenate(
        [
            contract_rows(normed_all, d_qkv[:, :qk_cols]).astype(jnp.bfloat16),
            gain_block.astype(jnp.bfloat16),
        ],
        axis=1,
    )
    g_out_t, qkv_grad = lax.optimization_barrier((g_out_t, qkv_grad))
    g_qkv, g_gains = split_cols(
        lax.psum_scatter(qkv_grad, "wide", scatter_dimension=0, tiled=True).astype(jnp.float32),
        [qk_cols, 128],
    )
    d_normed = narrow_scatter(d_normed_partial, relative)
    d_input_part, _ = rms_back(inputs, gain_attn, d_normed)
    d_tokens = d_resid + d_input_part
    attn_gain_grad = g_gains[:, 0]
    mlp_gain_grad = g_gains[:, 1]
    query_gain_grad = g_gains[:hd_local, 2]
    key_gain_grad = g_gains[:hd_local, 3]

    g_query = g_qkv[:, :q_cols]
    g_key = g_qkv[:, q_cols : q_cols + kv_cols]
    g_gate = jnp.concatenate([mlp_grads[h][0][:, :ff_half] for h in range(2)], axis=1)
    g_up = jnp.concatenate([mlp_grads[h][0][:, ff_half:] for h in range(2)], axis=1)
    g_down = jnp.concatenate([mlp_grads[h][1] for h in range(2)], axis=1).T
    output = (resid + narrow_scatter(down_partial, relative)).astype(jnp.bfloat16)
    return (
        output,
        d_tokens,
        attn_gain_grad,
        g_query,
        g_key,
        g_value,
        query_gain_grad,
        key_gain_grad,
        g_out_t.T,
        mlp_gain_grad,
        g_gate,
        g_up,
        g_down,
    )


def solution(mesh):
    in_specs = (
        P(("wide", "narrow"), None),
        P("wide", None),
        P(("wide", "narrow"), None),
        P("wide"),
        P("wide", "narrow"),
        P("wide", "narrow"),
        P("wide", "narrow"),
        P("wide"),
        P("wide"),
        P("narrow", "wide"),
        P("wide"),
        P("wide", "narrow"),
        P("wide", "narrow"),
        P("narrow", "wide"),
    )
    out_specs = (
        P(("wide", "narrow"), None),
        P(("wide", "narrow"), None),
        P("wide"),
        P("wide", "narrow"),
        P("wide", "narrow"),
        P("wide", "narrow"),
        P("wide"),
        P("wide"),
        P("narrow", "wide"),
        P("wide"),
        P("wide", "narrow"),
        P("wide", "narrow"),
        P("narrow", "wide"),
    )
    return jax.shard_map(shards_body, mesh=mesh, in_specs=in_specs, out_specs=out_specs, check_vma=False)
```

```python
import jax
import jax.numpy as jnp
from jax import lax
from jax.sharding import PartitionSpec as P


H = 16
KV = 8
HD = 128


EPS = 1e-06
ROPE_BASE = 1000000.0
NEG_FILL = -1e30

XPERM = [(0, 1), (1, 0), (2, 3), (3, 2)]
YPERM = [(0, 2), (2, 0), (1, 3), (3, 1)]
BLOCK_XOR = (0, 1, 2, 3, 0, 2, 1, 3)


def rms_apply(values, gain):
    return values * lax.rsqrt(jnp.mean(values * values, axis=-1, keepdims=True) + EPS) * gain


def rms_back(values, gain, grad):
    scale = lax.rsqrt(jnp.mean(values * values, axis=-1, keepdims=True) + EPS)
    weighted = grad * gain
    inner = jnp.mean(weighted * values, axis=-1, keepdims=True)
    d_values = scale * weighted - values * (scale * scale * scale) * inner
    return (d_values, grad * values * scale)


def rotate(values):
    half = values.shape[-1] // 2
    return jnp.concatenate([-values[..., half:], values[..., :half]], axis=-1)


def rotate_back(values):
    half = values.shape[-1] // 2
    return jnp.concatenate([values[..., half:], -values[..., :half]], axis=-1)


def doc_positions(doc_rows):
    index = lax.broadcasted_iota(jnp.int32, doc_rows.shape, 1)
    change = jnp.concatenate(
        [jnp.ones((doc_rows.shape[0], 1), jnp.bool_), doc_rows[:, 1:] != doc_rows[:, :-1]], axis=1
    )
    begin = lax.cummax(jnp.where(change, index, 0), axis=1)
    return index - begin


def rope_from_positions(position):
    freqs = ROPE_BASE ** (-(jnp.arange(HD // 2, dtype=jnp.float32) * (2.0 / HD)))
    angle = position.astype(jnp.float32)[..., None] * freqs
    cosine = jnp.cos(angle)
    sine = jnp.sin(angle)
    return (jnp.concatenate([cosine, cosine], axis=-1), jnp.concatenate([sine, sine], axis=-1))


def contract_rows(left, right):
    return lax.dot_general(
        left, right, (((0,), (0,)), ((), ())), preferred_element_type=jnp.float32
    )


def times_transposed(left, right):
    return lax.dot_general(
        left, right, (((1,), (1,)), ((), ())), preferred_element_type=jnp.float32
    )


def relative_ok(seq_count):
    return lax.axis_size("narrow") == 4 and seq_count == 1


def relative_rows(vec):
    n = lax.axis_index("narrow")
    half = vec.shape[0] // 8
    split = vec.reshape(4, 2, half)
    pieces = []
    for blk, flip in enumerate(BLOCK_XOR):
        source = split[:, 1 if blk >= 4 else 0]
        pieces.append(lax.dynamic_index_in_dim(source, jnp.bitwise_xor(n, flip), 0, keepdims=False))
    return jnp.concatenate(pieces)


def narrow_allreduce(v):
    if lax.axis_size("narrow") != 4:
        return lax.psum(v, "narrow")
    v = v + lax.ppermute(v, "narrow", XPERM)
    return v + lax.ppermute(v, "narrow", YPERM)


def narrow_gather(x, relative):
    if not relative:
        return lax.all_gather(x, "narrow", axis=0, tiled=True)
    half = x.shape[0] // 2
    a, b = x[:half], x[half:]
    a_x = lax.ppermute(a, "narrow", XPERM)
    b_y = lax.ppermute(b, "narrow", YPERM)
    a_pair = jnp.concatenate([a, a_x], axis=0)
    b_pair = jnp.concatenate([b, b_y], axis=0)
    a_pair_y = lax.ppermute(a_pair, "narrow", YPERM)
    b_pair_x = lax.ppermute(b_pair, "narrow", XPERM)
    return jnp.concatenate([a_pair, a_pair_y, b_pair, b_pair_x], axis=0)


def narrow_scatter(x, relative):
    if not relative:
        return lax.psum_scatter(
            x.astype(jnp.bfloat16), "narrow", scatter_dimension=0, tiled=True
        ).astype(jnp.float32)
    rows, c = x.shape
    half = rows // 8
    blocks = x.reshape(8, half, c)
    a_got = lax.ppermute(blocks[2:4].astype(jnp.bfloat16), "narrow", YPERM)
    b_got = lax.ppermute(blocks[6:8].astype(jnp.bfloat16), "narrow", XPERM)
    a_sum = blocks[0:2] + a_got.astype(jnp.float32)
    b_sum = blocks[4:6] + b_got.astype(jnp.float32)
    a_got2 = lax.ppermute(a_sum[1].astype(jnp.bfloat16), "narrow", XPERM)
    b_got2 = lax.ppermute(b_sum[1].astype(jnp.bfloat16), "narrow", YPERM)
    return jnp.concatenate(
        [a_sum[0] + a_got2.astype(jnp.float32), b_sum[0] + b_got2.astype(jnp.float32)], axis=0
    )


def split_cols(joined, widths):
    out = []
    start = 0
    for w in widths:
        out.append(joined[:, start : start + w])
        start += w
    return out


def wide_gather(blocks):
    joined = lax.all_gather(jnp.concatenate(blocks, axis=1), "wide", axis=0, tiled=True)
    return split_cols(joined, [blk.shape[1] for blk in blocks])


def qkv_scatter(grad):
    return lax.psum_scatter(grad, "wide", scatter_dimension=0, tiled=True)


def shards_body(
    tokens,
    doc_ids,
    cotangent,
    attn_gain,
    w_query,
    w_key,
    w_value,
    query_gain,
    key_gain,
    w_out,
    mlp_gain,
    w_gate,
    w_up,
    w_down,
):
    narrow_size = lax.axis_size("narrow")
    wide_size = lax.axis_size("wide")
    heads_here = H // narrow_size
    groups_here = KV // narrow_size
    repeat = H // KV
    seq_count, length = doc_ids.shape
    rows_group = seq_count * length
    scale = HD ** (-0.5)
    d_local = attn_gain.shape[0]
    hd_local = query_gain.shape[0]
    q_cols = w_query.shape[1]
    kv_cols = w_key.shape[1]
    ff_cols = w_gate.shape[1]
    ff_half = ff_cols // 2
    relative = relative_ok(seq_count)

    tokens_all = narrow_gather(tokens, relative)
    grad_rows = narrow_gather(cotangent, relative)

    pad_hd = ((0, d_local - hd_local),)
    gain_block = jnp.pad(
        jnp.stack(
            [attn_gain, mlp_gain, jnp.pad(query_gain, pad_hd), jnp.pad(key_gain, pad_hd)], axis=1
        ),
        ((0, 0), (0, 124)),
    )
    qkv_w, out_wt, gains_all = wide_gather(
        [jnp.concatenate([w_query, w_key, w_value], axis=1), w_out.T, gain_block]
    )
    gain_attn = gains_all[:, 0].astype(jnp.float32)
    gain_mlp = gains_all[:, 1].astype(jnp.float32)
    gains_split = gains_all.reshape(wide_size, d_local, 128)
    gain_query = gains_split[:, :hd_local, 2].reshape(-1).astype(jnp.float32)
    gain_key = gains_split[:, :hd_local, 3].reshape(-1).astype(jnp.float32)
    down_t = w_down.T
    mlp_sets = []
    for h in range(2):
        cols = slice(h * ff_half, (h + 1) * ff_half)
        mlp_sets.append(
            wide_gather([jnp.concatenate([w_gate[:, cols], w_up[:, cols]], axis=1), down_t[:, cols]])
        )

    if relative:
        order = relative_rows(jnp.arange(rows_group, dtype=jnp.int32))
        doc_row = relative_rows(doc_ids[0])
        position = relative_rows(doc_positions(doc_ids)[0])
    else:
        order = jnp.arange(rows_group, dtype=jnp.int32)
        doc_row = doc_ids.reshape(-1)
        position = doc_positions(doc_ids).reshape(-1)
    cosine, sine = rope_from_positions(position)
    cos_heads = cosine[:, None, :]
    sin_heads = sine[:, None, :]
    allowed = (order[None, :] <= order[:, None]) & (doc_row[None, :] == doc_row[:, None])
    if not relative:
        seq_of = jnp.arange(rows_group, dtype=jnp.int32) // length
        allowed = allowed & (seq_of[None, :] == seq_of[:, None])

    inputs = tokens.astype(jnp.float32)
    normed_all = rms_apply(tokens_all.astype(jnp.float32), gain_attn).astype(jnp.bfloat16)
    qkv = jnp.dot(normed_all, qkv_w, preferred_element_type=jnp.float32)
    q_pre = qkv[:, :q_cols].reshape(rows_group, heads_here, HD)
    k_pre = qkv[:, q_cols : q_cols + kv_cols].reshape(rows_group, groups_here, HD)
    v_use = qkv[:, q_cols + kv_cols :].astype(jnp.bfloat16).reshape(rows_group, groups_here, HD)
    q_norm = rms_apply(q_pre, gain_query)
    k_norm = rms_apply(k_pre, gain_key)
    q_use = (q_norm * cos_heads + rotate(q_norm) * sin_heads).astype(jnp.bfloat16)
    k_use = (k_norm * cos_heads + rotate(k_norm) * sin_heads).astype(jnp.bfloat16)
    q_grouped = q_use.reshape(rows_group, groups_here, repeat, HD)

    scores = jnp.einsum("qgrd,kgd->grqk", q_grouped, k_use, preferred_element_type=jnp.float32) * scale
    scores = jnp.where(allowed, scores, NEG_FILL)
    top = jnp.max(scores, axis=-1, keepdims=True)
    weights = jnp.exp(scores - top)
    total = jnp.sum(weights, axis=-1, keepdims=True)
    probs = weights / total
    mixed = jnp.einsum(
        "grqk,kgd->qgrd", probs.astype(jnp.bfloat16), v_use, preferred_element_type=jnp.float32
    )
    log_totals = (top + jnp.log(total))[..., 0]
    attended = mixed.astype(jnp.bfloat16).reshape(rows_group, heads_here * HD)

    resid = inputs + narrow_scatter(times_transposed(attended, out_wt), relative)
    mlp_in = rms_apply(resid, gain_mlp).astype(jnp.bfloat16)
    mlp_all = narrow_gather(mlp_in, relative)

    down_partial = None
    d_mlp_partial = None
    mlp_grads = []
    for h in range(2):
        gate_up_w, down_wt = mlp_sets[h]
        gate_up = jnp.dot(mlp_all, gate_up_w, preferred_element_type=jnp.float32)
        gate = gate_up[:, :ff_half]
        up = gate_up[:, ff_half:]
        sigmoid = jax.nn.sigmoid(gate)
        hidden = (gate * sigmoid * up).astype(jnp.bfloat16)
        part = times_transposed(hidden, down_wt)
        down_partial = part if down_partial is None else down_partial + part
        d_hidden = jnp.dot(grad_rows, down_wt, preferred_element_type=jnp.float32)
        d_up = (d_hidden * gate * sigmoid).astype(jnp.bfloat16)
        d_gate = (d_hidden * up * sigmoid * (1.0 + gate * (1.0 - sigmoid))).astype(jnp.bfloat16)
        d_gate_up = jnp.concatenate([d_gate, d_up], axis=1)
        part = times_transposed(d_gate_up, gate_up_w)
        d_mlp_partial = part if d_mlp_partial is None else d_mlp_partial + part
        g_down_t = contract_rows(grad_rows, hidden)
        g_gate_up = contract_rows(mlp_all, d_gate_up)
        joined = jnp.concatenate(
            [g_gate_up.astype(jnp.bfloat16), g_down_t.astype(jnp.bfloat16)], axis=1
        )
        if h == 0:
            joined, mlp_sets[1] = lax.optimization_barrier((joined, mlp_sets[1]))
            mlp_grads.append(lax.psum_scatter(joined, "wide", scatter_dimension=0, tiled=True))
        else:
            last_joined = joined

    d_mlp_in = narrow_scatter(d_mlp_partial, relative)
    d_part, mlp_gain_terms = rms_back(resid, gain_mlp, d_mlp_in)
    grad_mlp_gain = jnp.sum(mlp_gain_terms, axis=0)
    d_resid = cotangent.astype(jnp.float32) + d_part
    p_scores = (
        jnp.einsum("qgrd,kgd->grqk", q_grouped, k_use, preferred_element_type=jnp.float32) * scale
    )
    p_probs = jnp.where(allowed, jnp.exp(p_scores - log_totals[..., None]), 0.0)
    d_resid_low = d_resid.astype(jnp.bfloat16)
    mlp_grads.append(lax.psum_scatter(last_joined, "wide", scatter_dimension=0, tiled=True))
    branch_rows = narrow_gather(d_resid_low, relative)
    out_grad = contract_rows(branch_rows, attended).astype(jnp.bfloat16)
    d_attended = jnp.dot(branch_rows, out_wt, preferred_element_type=jnp.float32).astype(jnp.bfloat16)
    d_mixed = d_attended.reshape(rows_group, groups_here, repeat, HD)
    d_value = jnp.einsum(
        "grqk,qgrd->kgd", p_probs.astype(jnp.bfloat16), d_mixed, preferred_element_type=jnp.float32
    ).astype(jnp.bfloat16)
    value_grad = contract_rows(normed_all, d_value.reshape(rows_group, groups_here * HD))
    out_grad = jnp.concatenate([out_grad, value_grad.astype(jnp.bfloat16)], axis=1)
    mlp_grads = [split_cols(g.astype(jnp.float32), [2 * ff_half, ff_half]) for g in mlp_grads]
    out_summed = lax.psum_scatter(out_grad, "wide", scatter_dimension=0, tiled=True)
    g_out_t, g_value = split_cols(out_summed.astype(jnp.float32), [q_cols, kv_cols])

    d_probs = jnp.einsum("qgrd,kgd->grqk", d_mixed, v_use, preferred_element_type=jnp.float32)
    inner = jnp.sum(p_probs * d_probs, axis=-1, keepdims=True)
    d_scores = (p_probs * (d_probs - inner)).astype(jnp.bfloat16)
    d_query = jnp.einsum("grqk,kgd->qgrd", d_scores, k_use, preferred_element_type=jnp.float32) * scale
    d_key = jnp.einsum("grqk,qgrd->kgd", d_scores, q_grouped, preferred_element_type=jnp.float32) * scale

    d_query = d_query.reshape(rows_group, heads_here, HD)
    d_q_norm = d_query * cos_heads + rotate_back(d_query * sin_heads)
    d_k_norm = d_key * cos_heads + rotate_back(d_key * sin_heads)
    d_q_pre, query_terms = rms_back(q_pre, gain_query, d_q_norm)
    d_k_pre, key_terms = rms_back(k_pre, gain_key, d_k_norm)
    grad_query_gain = jnp.sum(query_terms, axis=(0, 1))
    grad_key_gain = jnp.sum(key_terms, axis=(0, 1))
    d_qkv = jnp.concatenate(
        [
            d_q_pre.astype(jnp.bfloat16).reshape(rows_group, heads_here * HD),
            d_k_pre.astype(jnp.bfloat16).reshape(rows_group, groups_here * HD),
            d_value.reshape(rows_group, groups_here * HD),
        ],
        axis=1,
    )
    d_normed_partial = times_transposed(d_qkv, qkv_w)
    tokens_all_f = tokens_all.astype(jnp.float32)
    scale_all = lax.rsqrt(jnp.mean(tokens_all_f * tokens_all_f, axis=-1, keepdims=True) + EPS)
    attn_gain_part = jnp.sum(d_normed_partial * tokens_all_f * scale_all, axis=0)
    gain_parts = narrow_allreduce(
        jnp.concatenate([attn_gain_part, grad_mlp_gain, grad_query_gain, grad_key_gain])
    )
    d_full = d_local * wide_size
    hd_full = hd_local * wide_size

    def by_chunk(vec, size):
        return jnp.pad(vec.reshape(wide_size, size), ((0, 0), (0, d_local - size)))

    gain_block = jnp.stack(
        [
            by_chunk(gain_parts[:d_full], d_local),
            by_chunk(gain_parts[d_full : 2 * d_full], d_local),
            by_chunk(gain_parts[2 * d_full : 2 * d_full + hd_full], hd_local),
            by_chunk(gain_parts[2 * d_full + hd_full :], hd_local),
        ],
        axis=-1,
    ).reshape(d_full, 4)
    gain_block = jnp.pad(gain_block, ((0, 0), (0, 124)))
    qk_cols = q_cols + kv_cols
    qkv_grad = jnp.concatenate(
        [
            contract_rows(normed_all, d_qkv[:, :qk_cols]).astype(jnp.bfloat16),
            gain_block.astype(jnp.bfloat16),
        ],
        axis=1,
    )
    g_qkv, g_gains = split_cols(
        qkv_scatter(qkv_grad).astype(jnp.float32),
        [qk_cols, 128],
    )
    d_normed = narrow_scatter(d_normed_partial, relative)
    d_input_part, _ = rms_back(inputs, gain_attn, d_normed)
    d_tokens = d_resid + d_input_part
    attn_gain_grad = g_gains[:, 0]
    mlp_gain_grad = g_gains[:, 1]
    query_gain_grad = g_gains[:hd_local, 2]
    key_gain_grad = g_gains[:hd_local, 3]

    g_query = g_qkv[:, :q_cols]
    g_key = g_qkv[:, q_cols : q_cols + kv_cols]
    g_gate = jnp.concatenate([mlp_grads[h][0][:, :ff_half] for h in range(2)], axis=1)
    g_up = jnp.concatenate([mlp_grads[h][0][:, ff_half:] for h in range(2)], axis=1)
    g_down = jnp.concatenate([mlp_grads[h][1] for h in range(2)], axis=1).T
    output = (resid + narrow_scatter(down_partial, relative)).astype(jnp.bfloat16)
    return (
        output,
        d_tokens,
        attn_gain_grad,
        g_query,
        g_key,
        g_value,
        query_gain_grad,
        key_gain_grad,
        g_out_t.T,
        mlp_gain_grad,
        g_gate,
        g_up,
        g_down,
    )


def solution(mesh):
    in_specs = (
        P(("wide", "narrow"), None),
        P("wide", None),
        P(("wide", "narrow"), None),
        P("wide"),
        P("wide", "narrow"),
        P("wide", "narrow"),
        P("wide", "narrow"),
        P("wide"),
        P("wide"),
        P("narrow", "wide"),
        P("wide"),
        P("wide", "narrow"),
        P("wide", "narrow"),
        P("narrow", "wide"),
    )
    out_specs = (
        P(("wide", "narrow"), None),
        P(("wide", "narrow"), None),
        P("wide"),
        P("wide", "narrow"),
        P("wide", "narrow"),
        P("wide", "narrow"),
        P("wide"),
        P("wide"),
        P("narrow", "wide"),
        P("wide"),
        P("wide", "narrow"),
        P("wide", "narrow"),
        P("narrow", "wide"),
    )
    return jax.shard_map(shards_body, mesh=mesh, in_specs=in_specs, out_specs=out_specs, check_vma=False)
```
